256 devices in a mesh: ctx: 32 (over z, y), head: 8 (over x, core).
Axes of the slice: x: 4, y: 4, z: 8, core: 2. Of those that a mesh axis runs over, the one named last changes fastest.
Arguments:
- query_input: bfloat16 [16384, 4096], P(('ctx', 'head')), may hold values from -6 to 6
- key_input: bfloat16 [16384, 4096], P(('ctx', 'head')), may hold values from -6 to 6
- value_input: bfloat16 [16384, 4096], P(('ctx', 'head')), may hold values from -6 to 6
- cotangent: bfloat16 [16384, 4096], P(('ctx', 'head')), may hold values from -6 to 6
- level_codes: int32 [32, 15, 16384], P('head', None, 'ctx'), may hold values from 0 to 15
Outputs:
- attended: bfloat16 [16384, 4096], P(('ctx', 'head'))
- grad_queries: bfloat16 [16384, 4096], P(('ctx', 'head'))
- grad_keys: bfloat16 [16384, 4096], P(('ctx', 'head'))
- grad_values: bfloat16 [16384, 4096], P(('ctx', 'head'))
The draws below stay inside these ranges and needn't reach their ends.
All inputs are finite; a program needn't handle non-finite values.
Results may differ from the reference program's by a relative error of at most 0.0074.
Values may be sent and summed in bfloat16 or wider, within the bound.
A program may use at most 128 MiB of HBM per device.

```python
import jax
import jax.numpy as jnp
from jax import lax

H = 32
DH = 128
TOK_DEV = 512
TOKENS = 16384
TOK_BITS = 9
CTX_BITS = 5
NLEV = 15
N_CTX = 32


def set_ends(drawn, own_key, least, largest):
    place = [jax.random.randint(jax.random.fold_in(own_key, axis), (), 0, length) for axis, length in enumerate(drawn.shape)]
    longest = drawn.shape.index(max(drawn.shape))
    next_to = place[:longest] + [(place[longest] + 1) % drawn.shape[longest]] + place[longest + 1:]
    return drawn.at[tuple(place)].set(least).at[tuple(next_to)].set(largest)


def steps_of(key, dims, pieces, low, top_value):
    level, own = 1.0, jax.random.fold_in(key, 6)
    for axis_at, blocks in pieces:
        heights = jnp.exp(jax.random.uniform(jax.random.fold_in(own, axis_at), (blocks,), jnp.float32, low / len(pieces), top_value / len(pieces)))
        level = level * jnp.repeat(heights, dims[axis_at] // blocks).reshape([-1 if axis == axis_at else 1 for axis in range(len(dims))])
    return level


def centred(key, dims, scale, limit, cuts=(), kind=jnp.bfloat16):
    values = scale * jax.random.normal(key, dims, jnp.float32)
    if cuts:
        values = values * steps_of(key, dims, cuts, -0.22, 0.18)
    return jnp.clip(values, -limit, limit).astype(kind)


def setup_inputs(seed: int = 0) -> dict:
    key_list = jax.random.split(jax.random.key(seed), 6)
    return {
        "query_input": centred(key_list[0], (TOKENS, H * DH), 1.0, 6.0, ((0, 256),)),
        "key_input": centred(key_list[1], (TOKENS, H * DH), 1.0, 6.0, ((0, 256),)),
        "value_input": centred(key_list[2], (TOKENS, H * DH), 1.0, 6.0, ((0, 256),)),
        "cotangent": centred(key_list[3], (TOKENS, H * DH), 1.0, 6.0, ((0, 256),)),
        "level_codes": set_ends(jax.random.randint(key_list[4], (H, NLEV, TOKENS), 0, 16), jax.random.fold_in(key_list[4], 1), 0, 15).astype(jnp.int32),
    }


def level_gain(level):
    if level == 0:
        return 1.0
    return 2.0 ** (-(level - 1) / 2.0)


def member_of(owner_block, member_block, bit_index):
    bit_span = 2 ** bit_index
    owner_set = (owner_block // bit_span) % 2 == 1
    member_clear = (member_block // bit_span) % 2 == 0
    same_parent = owner_block // (2 * bit_span) == member_block // (2 * bit_span)
    return jnp.where(owner_set & member_clear & same_parent, 1.0, 0.0).astype(jnp.float32)


def by_block(array):
    return array.reshape(N_CTX, TOK_DEV, H, DH).transpose(0, 2, 1, 3)


def reference(query_input, key_input, value_input, cotangent, level_codes):
    score_scale = DH ** -0.5
    code_blocks = (level_codes.astype(jnp.float32) / 8.0).reshape(H, NLEV, N_CTX, TOK_DEV).transpose(2, 0, 1, 3)
    block_ids = jnp.arange(N_CTX, dtype=jnp.int32)
    query_blocks = by_block(query_input)
    key_blocks = by_block(key_input)
    value_blocks = by_block(value_input)
    cot_blocks = by_block(cotangent)

    def cross_scale(block_index, code_weights):
        return jnp.stack([code_weights[:, TOK_BITS + 1 + bit_index, :] * (score_scale * level_gain(TOK_BITS + 1 + bit_index)) * ((block_index // 2 ** bit_index) % 2).astype(jnp.float32) for bit_index in range(CTX_BITS)])

    def first_pass(inputs):
        block_index, query_heads, key_heads, value_heads, cot_heads, code_weights = inputs
        query_wide = query_heads.astype(jnp.float32)
        state = jnp.einsum("htd,hte->hde", key_heads.astype(jnp.float32), value_heads.astype(jnp.float32))
        row_scale = cross_scale(block_index, code_weights)
        scaled_cot = (row_scale[..., None] * cot_heads.astype(jnp.float32)[None]).astype(jnp.bfloat16)
        grad_state = jnp.einsum("htd,bhte->bhde", query_wide, scaled_cot.astype(jnp.float32))
        return state, grad_state

    states, grad_states = lax.map(first_pass, (block_ids, query_blocks, key_blocks, value_blocks, cot_blocks, code_blocks))
    places = jnp.arange(TOK_DEV, dtype=jnp.int32)
    levels = jnp.zeros((TOK_DEV, TOK_DEV), jnp.int32)
    for bit_index in range(TOK_BITS):
        levels = levels + (places[:, None] // 2 ** bit_index != places[None, :] // 2 ** bit_index).astype(jnp.int32)
    causal = places[None, :] <= places[:, None]

    def second_pass(inputs):
        block_index, query_heads, key_heads, value_heads, cot_heads, code_weights = inputs
        query_wide = query_heads.astype(jnp.float32)
        key_wide = key_heads.astype(jnp.float32)
        value_wide = value_heads.astype(jnp.float32)
        cot_wide = cot_heads.astype(jnp.float32)
        lower_pick = jnp.stack([member_of(block_index, block_ids, bit_index) for bit_index in range(CTX_BITS)])
        bucket = jnp.einsum("be,ehij->bhij", lower_pick, states, precision=lax.Precision.HIGHEST).astype(jnp.bfloat16)
        upper_pick = jnp.stack([member_of(block_ids, block_index, bit_index) for bit_index in range(CTX_BITS)])
        pulled = jnp.einsum("bc,cbhij->hij", upper_pick, grad_states, precision=lax.Precision.HIGHEST).astype(jnp.bfloat16)
        bucket_wide = bucket.astype(jnp.float32)
        pulled_wide = pulled.astype(jnp.float32)
        weight = jnp.zeros((H, TOK_DEV, TOK_DEV), jnp.float32)
        for level_index in range(TOK_BITS + 1):
            weight = jnp.where((levels == level_index)[None], code_weights[:, level_index, :, None] * level_gain(level_index), weight)
        weight = jnp.where(causal[None], weight, 0.0)
        row_scale = cross_scale(block_index, code_weights)
        scores = jnp.einsum("hpd,hsd->hps", query_wide, key_wide)
        attention = (score_scale * weight * scores).astype(jnp.bfloat16).astype(jnp.float32)
        local_out = jnp.einsum("hps,hse->hpe", attention, value_wide)
        cross_out = jnp.sum(row_scale[..., None] * jnp.einsum("hpd,bhde->bhpe", query_wide, bucket_wide), axis=0)
        attended = (local_out + cross_out).astype(jnp.bfloat16)
        dots = jnp.einsum("hpe,hse->hps", cot_wide, value_wide)
        score_grads = (score_scale * weight * dots).astype(jnp.bfloat16).astype(jnp.float32)
        cross_qgrad = jnp.sum(row_scale[..., None] * jnp.einsum("hpe,bhde->bhpd", cot_wide, bucket_wide), axis=0)
        grad_query = (jnp.einsum("hps,hsd->hpd", score_grads, key_wide) + cross_qgrad).astype(jnp.bfloat16)
        grad_key = (jnp.einsum("hps,hpd->hsd", score_grads, query_wide) + jnp.einsum("hse,hde->hsd", value_wide, pulled_wide)).astype(jnp.bfloat16)
        grad_value = (jnp.einsum("hps,hpe->hse", attention, cot_wide) + jnp.einsum("hsd,hde->hse", key_wide, pulled_wide)).astype(jnp.bfloat16)
        return attended, grad_query, grad_key, grad_value

    results = lax.map(second_pass, (block_ids, query_blocks, key_blocks, value_blocks, cot_blocks, code_blocks))

    def unblock(array):
        return array.transpose(0, 2, 1, 3).reshape(TOKENS, H * DH)

    return unblock(results[0]), unblock(results[1]), unblock(results[2]), unblock(results[3])
```

```python
import functools

import jax
import jax.numpy as jnp
from jax import lax
from jax.experimental import pallas as pl
from jax.experimental.pallas import tpu as pltpu
from jax.sharding import PartitionSpec as P

MESH = pl.DeviceIdType.MESH
KEY, VALUE, QUERY, COT = range(4)
TILE = 128


def level_gain(level):
    if level == 0:
        return 1.0
    return 2.0 ** (-(level - 1) / 2.0)


def dot_nn(a, b):
    return lax.dot_general(a, b, (((1,), (0,)), ((), ())), preferred_element_type=jnp.float32)


def dot_nt(a, b):
    return lax.dot_general(a, b, (((1,), (1,)), ((), ())), preferred_element_type=jnp.float32)


def dot_tn(a, b):
    return lax.dot_general(a, b, (((0,), (0,)), ((), ())), preferred_element_type=jnp.float32)


def kernel(
    n_ctx,
    n_head,
    ctx_bits,
    tok_bits,
    query_ref,
    key_ref,
    value_ref,
    cot_ref,
    codes_ref,
    out_ref,
    gq_ref,
    gk_ref,
    gv_ref,
    rows_in,
    codes,
    code_rows,
    code_cols,
    levels,
    local,
    rows_out,
    state_send,
    state_parts,
    bucket_send,
    bucket,
    grad_send,
    grad_parts,
    pulled_send,
    pulled,
    in_send,
    in_recv,
    own_sem,
    state_sems,
    bucket_send_sem,
    bucket_recv,
    grad_send_sem,
    grad_recv,
    pulled_sems,
    out_send,
    out_recv,
):
    my_ctx = lax.axis_index("ctx")
    my_head = lax.axis_index("head")
    inputs = (key_ref, value_ref, query_ref, cot_ref)
    outputs = (out_ref, gq_ref, gk_ref, gv_ref)
    share = query_ref.shape[0]
    length = share * n_head
    width = query_ref.shape[1] // n_head
    n_local = width // TILE
    state_rows = n_local * TILE
    part = state_rows // n_ctx
    tiles = length // TILE
    scale = TILE ** (-0.5)

    def bit_set(block, bit_index):
        return block // 2**bit_index % 2 == 1

    def own_bit(bit_index):
        return bit_set(my_ctx, bit_index)

    def ctx_peer(step):
        return lax.rem(my_ctx + step, n_ctx)

    def head_columns(head):
        return pl.ds(pl.multiple_of(head * TILE, TILE), TILE)

    def part_rows(owner):
        return pl.ds(pl.multiple_of(owner * part, part), part)

    def share_rows(owner):
        return pl.ds(pl.multiple_of(owner * share, share), share)

    def width_columns(owner):
        return pl.ds(pl.multiple_of(owner * width, width), width)

    barrier = pltpu.get_barrier_semaphore()
    for step in range(1, n_head):
        pl.semaphore_signal(
            barrier, inc=1, device_id={"head": lax.rem(my_head + step, n_head)}, device_id_type=MESH
        )

    @pl.loop(1, n_ctx)
    def _(step):
        pl.semaphore_signal(barrier, inc=1, device_id={"ctx": ctx_peer(step)}, device_id_type=MESH)

    codes_copy = pltpu.make_async_copy(codes_ref, codes, own_sem.at[8])
    codes_copy.start()
    for slot, array in enumerate(inputs):
        pltpu.make_async_copy(
            array.at[:, width_columns(my_head)],
            rows_in.at[slot, share_rows(my_head), :],
            own_sem.at[slot],
        ).start()
    pl.semaphore_wait(barrier, n_head - 1 + n_ctx - 1)

    for slot, array in enumerate(inputs):
        for step in range(1, n_head):
            peer = lax.rem(my_head + step, n_head)
            pltpu.make_async_remote_copy(
                src_ref=array.at[:, width_columns(peer)],
                dst_ref=rows_in.at[slot, share_rows(my_head), :],
                send_sem=in_send.at[slot],
                recv_sem=in_recv.at[slot],
                device_id={"head": peer},
                device_id_type=MESH,
            ).start()

    codes_copy.wait()
    for head in range(n_local):
        code_rows[...] = jnp.zeros_like(code_rows)
        code_rows[0 : codes.shape[1], :] = codes[head].astype(jnp.float32)
        code_cols[head] = code_rows[...].T
    place = lax.broadcasted_iota(jnp.int32, (TILE, TILE), 0)
    other = lax.broadcasted_iota(jnp.int32, (TILE, TILE), 1)
    differ = place ^ other
    level = jnp.zeros((TILE, TILE), jnp.int32)
    for bit_index in range(7):
        level = level + (differ >= 2**bit_index).astype(jnp.int32)
    levels[...] = jnp.where(other <= place, level, -1)
    for bit_index in range(ctx_bits):

        @pl.when(jnp.logical_not(own_bit(bit_index)))
        def _():
            bucket[bit_index] = jnp.zeros((state_rows, TILE), jnp.bfloat16)

    def arrived(slot):
        pltpu.make_async_copy(
            inputs[slot].at[:, width_columns(my_head)],
            rows_in.at[slot, share_rows(my_head), :],
            own_sem.at[slot],
        ).wait()
        others = rows_in.at[slot, 0 : length - share, :]
        pltpu.make_async_copy(others, others, in_recv.at[slot]).wait()

    def code_column(head, level_index, rows):
        return code_cols[head, rows, level_index : level_index + 1] * (
            level_gain(level_index) * scale / 8.0
        )

    arrived(KEY)
    arrived(VALUE)

    @pl.loop(0, n_local)
    def _(head):
        columns = head_columns(head)
        state = dot_tn(rows_in[KEY, :, columns], rows_in[VALUE, :, columns])
        state_send[columns, :] = state.astype(jnp.bfloat16)

    @pl.loop(1, n_ctx)
    def _(step):
        peer = ctx_peer(step)
        pltpu.make_async_remote_copy(
            src_ref=state_send.at[part_rows(peer), :],
            dst_ref=state_parts.at[my_ctx],
            send_sem=state_sems.at[0],
            recv_sem=state_sems.at[1],
            device_id={"ctx": peer},
            device_id_type=MESH,
        ).start()

    state_parts[my_ctx] = state_send[part_rows(my_ctx), :]
    state_others = state_parts.at[0 : n_ctx - 1]
    pltpu.make_async_copy(state_others, state_others, state_sems.at[1]).wait()

    node = state_parts[...].astype(jnp.float32)
    first_node = []
    count = 0
    for bit_index in range(ctx_bits):
        pairs = node.reshape(node.shape[0] // 2, 2, part, TILE)
        first_node.append(count)
        bucket_send[count : count + pairs.shape[0]] = pairs[:, 0].astype(jnp.bfloat16)
        count += pairs.shape[0]
        node = pairs[:, 0] + pairs[:, 1]

    @pl.loop(1, n_ctx)
    def _(step):
        peer = ctx_peer(step)
        for bit_index in range(ctx_bits):

            @pl.when(bit_set(peer, bit_index))
            def _():
                pltpu.make_async_remote_copy(
                    src_ref=bucket_send.at[first_node[bit_index] + peer // 2 ** (bit_index + 1)],
                    dst_ref=bucket.at[bit_index, part_rows(my_ctx), :],
                    send_sem=bucket_send_sem.at[bit_index],
                    recv_sem=bucket_recv.at[bit_index],
                    device_id={"ctx": peer},
                    device_id_type=MESH,
                ).start()

    for bit_index in range(ctx_bits):

        @pl.when(own_bit(bit_index))
        def _():
            bucket[bit_index, part_rows(my_ctx), :] = bucket_send[
                first_node[bit_index] + my_ctx // 2 ** (bit_index + 1)
            ]

    arrived(QUERY)
    arrived(COT)

    @pl.loop(0, n_local)
    def _(head):
        columns = head_columns(head)
        query = rows_in[QUERY, :, columns]
        cot = rows_in[COT, :, columns].astype(jnp.float32)
        for bit_index in range(ctx_bits):
            row_scale = code_column(head, tok_bits + 1 + bit_index, slice(None))
            scaled = (row_scale * cot).astype(jnp.bfloat16)
            grad_send[bit_index, columns, :] = dot_tn(query, scaled).astype(jnp.bfloat16)

    def grad_slot(block, bit_index):
        return block // 2 ** (bit_index + 1) * 2**bit_index + block % 2**bit_index

    @pl.loop(1, n_ctx)
    def _(step):
        peer = ctx_peer(step)
        for bit_index in range(ctx_bits):

            @pl.when(own_bit(bit_index))
            def _():
                pltpu.make_async_remote_copy(
                    src_ref=grad_send.at[bit_index, part_rows(peer), :],
                    dst_ref=grad_parts.at[bit_index, grad_slot(my_ctx, bit_index)],
                    send_sem=grad_send_sem.at[bit_index],
                    recv_sem=grad_recv.at[bit_index],
                    device_id={"ctx": peer},
                    device_id_type=MESH,
                ).start()

    for bit_index in range(ctx_bits):

        @pl.when(own_bit(bit_index))
        def _():
            grad_parts[bit_index, grad_slot(my_ctx, bit_index)] = grad_send[
                bit_index, part_rows(my_ctx), :
            ]

    @pl.loop(0, n_local)
    def _(head):
        columns = head_columns(head)
        for row in range(tiles):
            rows = slice(row * TILE, (row + 1) * TILE)
            reach = (row + 1) * TILE
            query = rows_in[QUERY, rows, columns]
            cot = rows_in[COT, rows, columns]
            keys = rows_in[KEY, 0:reach, columns]
            values = rows_in[VALUE, 0:reach, columns]
            scores = dot_nt(query, keys)
            dots = dot_nt(cot, values)
            probs, score_grads = [], []
            for column in range(row + 1):
                if column == row:
                    weight = jnp.zeros((TILE, TILE), jnp.float32)
                    for level_index in range(8):
                        weight = jnp.where(
                            levels[...] == level_index,
                            code_column(head, level_index, rows),
                            weight,
                        )
                else:
                    weight = code_column(head, 7 + (row ^ column).bit_length(), rows)
                at = slice(column * TILE, (column + 1) * TILE)
                probs.append((weight * scores[:, at]).astype(jnp.bfloat16))
                score_grads.append((weight * dots[:, at]).astype(jnp.bfloat16))
            probs = jnp.concatenate(probs, axis=1)
            score_grads = jnp.concatenate(score_grads, axis=1)
            local[0, rows, columns] = dot_nn(probs, values)
            local[1, rows, columns] = dot_nn(score_grads, keys)
            key_grad = dot_tn(score_grads, query)
            value_grad = dot_tn(probs, cot)
            if row:
                local[2, 0 : row * TILE, columns] += key_grad[: row * TILE]
                local[3, 0 : row * TILE, columns] += value_grad[: row * TILE]
            local[2, rows, columns] = key_grad[row * TILE :]
            local[3, rows, columns] = value_grad[row * TILE :]

    def send_out(slot):
        for step in range(1, n_head):
            peer = lax.rem(my_head + step, n_head)
            pltpu.make_async_remote_copy(
                src_ref=rows_out.at[slot, share_rows(peer), :],
                dst_ref=outputs[slot].at[:, width_columns(my_head)],
                send_sem=out_send.at[slot],
                recv_sem=out_recv.at[slot],
                device_id={"head": peer},
                device_id_type=MESH,
            ).start()
        pltpu.make_async_copy(
            rows_out.at[slot, share_rows(my_head), :],
            outputs[slot].at[:, width_columns(my_head)],
            own_sem.at[4 + slot],
        ).start()

    for bit_index in range(ctx_bits):
        half = n_ctx // 2

        @pl.when(own_bit(bit_index))
        def _():
            others = grad_parts.at[bit_index, 0 : half - 1]
            pltpu.make_async_copy(others, others, grad_recv.at[bit_index]).wait()

        @pl.when(jnp.logical_not(own_bit(bit_index)))
        def _():
            others = grad_parts.at[bit_index]
            pltpu.make_async_copy(others, others, grad_recv.at[bit_index]).wait()

    upper = []
    for bit_index in range(ctx_bits):
        terms = grad_parts[bit_index].astype(jnp.float32)
        upper.append(
            jnp.sum(terms.reshape(n_ctx // 2 ** (bit_index + 1), 2**bit_index, part, TILE), axis=1)
        )
    for block in range(n_ctx):
        total = jnp.zeros((part, TILE), jnp.float32)
        for bit_index in range(ctx_bits):
            if not block >> bit_index & 1:
                total = total + upper[bit_index][block >> (bit_index + 1)]
        pulled_send[block] = total.astype(jnp.bfloat16)

    @pl.loop(1, n_ctx)
    def _(step):
        peer = ctx_peer(step)
        pltpu.make_async_remote_copy(
            src_ref=pulled_send.at[peer],
            dst_ref=pulled.at[part_rows(my_ctx), :],
            send_sem=pulled_sems.at[0],
            recv_sem=pulled_sems.at[1],
            device_id={"ctx": peer},
            device_id_type=MESH,
        ).start()

    pulled[part_rows(my_ctx), :] = pulled_send[my_ctx]

    for bit_index in range(ctx_bits):

        @pl.when(own_bit(bit_index))
        def _():
            others = bucket.at[bit_index, 0 : state_rows - part, :]
            pltpu.make_async_copy(others, others, bucket_recv.at[bit_index]).wait()

    @pl.loop(0, n_local)
    def _(head):
        columns = head_columns(head)
        for row in range(tiles):
            rows = slice(row * TILE, (row + 1) * TILE)
            query = rows_in[QUERY, rows, columns]
            cot = rows_in[COT, rows, columns]
            attended = local[0, rows, columns]
            grad_query = local[1, rows, columns]
            for bit_index in range(ctx_bits):
                row_scale = code_column(head, tok_bits + 1 + bit_index, rows)
                states = bucket[bit_index, columns, :]
                attended = attended + row_scale * dot_nn(query, states)
                grad_query = grad_query + row_scale * dot_nt(cot, states)
            rows_out[0, rows, columns] = attended.astype(jnp.bfloat16)
            rows_out[1, rows, columns] = grad_query.astype(jnp.bfloat16)

    send_out(0)
    send_out(1)

    pulled_others = pulled.at[0 : state_rows - part, :]
    pltpu.make_async_copy(pulled_others, pulled_others, pulled_sems.at[1]).wait()

    @pl.loop(0, n_local)
    def _(head):
        columns = head_columns(head)
        states = pulled[columns, :]
        grad_key = local[2, :, columns] + dot_nt(rows_in[VALUE, :, columns], states)
        rows_out[2, :, columns] = grad_key.astype(jnp.bfloat16)
        grad_value = local[3, :, columns] + dot_nn(rows_in[KEY, :, columns], states)
        rows_out[3, :, columns] = grad_value.astype(jnp.bfloat16)

    send_out(2)
    send_out(3)

    for slot in range(4):
        sent = rows_in.at[slot, 0 : length - share, :]
        pltpu.make_async_copy(sent, sent, in_send.at[slot]).wait()
    pltpu.make_async_copy(state_others, state_others, state_sems.at[0]).wait()
    pltpu.make_async_copy(pulled_others, pulled_others, pulled_sems.at[0]).wait()
    for bit_index in range(ctx_bits):
        half = n_ctx // 2
        rest = grad_parts.at[bit_index, 0 : half - 1]

        @pl.when(own_bit(bit_index))
        def _():
            pltpu.make_async_copy(rest, rest, bucket_send_sem.at[bit_index]).wait()
            sent = grad_send.at[bit_index, 0 : state_rows - part, :]
            pltpu.make_async_copy(sent, sent, grad_send_sem.at[bit_index]).wait()

        @pl.when(jnp.logical_not(own_bit(bit_index)))
        def _():
            sent = grad_parts.at[bit_index]
            pltpu.make_async_copy(sent, sent, bucket_send_sem.at[bit_index]).wait()

    for slot in range(4):
        sent = rows_out.at[slot, 0 : length - share, :]
        pltpu.make_async_copy(sent, sent, out_send.at[slot]).wait()
        pltpu.make_async_copy(sent, sent, out_recv.at[slot]).wait()
        pltpu.make_async_copy(
            rows_out.at[slot, share_rows(my_head), :],
            outputs[slot].at[:, width_columns(my_head)],
            own_sem.at[4 + slot],
        ).wait()


def on_device(n_ctx, n_head, query_input, key_input, value_input, cotangent, level_codes):
    share, features = query_input.shape
    n_local, n_levels, length = level_codes.shape
    width = features // n_head
    tok_bits = length.bit_length() - 1
    ctx_bits = n_levels - tok_bits - 1
    state_rows = n_local * TILE
    part = state_rows // n_ctx
    half = jnp.bfloat16
    result = jax.ShapeDtypeStruct((share, features), half)
    dma = pltpu.SemaphoreType.DMA
    return pl.pallas_call(
        functools.partial(kernel, n_ctx, n_head, ctx_bits, tok_bits),
        out_shape=(result,) * 4,
        in_specs=[pl.BlockSpec(memory_space=pl.ANY)] * 5,
        out_specs=(pl.BlockSpec(memory_space=pl.ANY),) * 4,
        scratch_shapes=[
            pltpu.VMEM((4, length, width), half),
            pltpu.VMEM(level_codes.shape, jnp.int32),
            pltpu.VMEM((TILE, length), jnp.float32),
            pltpu.VMEM((n_local, length, TILE), jnp.float32),
            pltpu.VMEM((TILE, TILE), jnp.int32),
            pltpu.VMEM((4, length, width), jnp.float32),
            pltpu.VMEM((4, length, width), half),
            pltpu.VMEM((state_rows, TILE), half),
            pltpu.VMEM((n_ctx, part, TILE), half),
            pltpu.VMEM((n_ctx, part, TILE), half),
            pltpu.VMEM((ctx_bits, state_rows, TILE), half),
            pltpu.VMEM((ctx_bits, state_rows, TILE), half),
            pltpu.VMEM((ctx_bits, n_ctx // 2, part, TILE), half),
            pltpu.VMEM((n_ctx, part, TILE), half),
            pltpu.VMEM((state_rows, TILE), half),
            dma((4,)),
            dma((4,)),
            dma((9,)),
            dma((2,)),
            dma((ctx_bits,)),
            dma((ctx_bits,)),
            dma((ctx_bits,)),
            dma((ctx_bits,)),
            dma((2,)),
            dma((4,)),
            dma((4,)),
        ],
        compiler_params=pltpu.CompilerParams(collective_id=0, has_side_effects=True),
        name="layer",
    )(query_input, key_input, value_input, cotangent, level_codes)


def solution(mesh):
    rows = P(("ctx", "head"), None)
    return jax.shard_map(
        functools.partial(on_device, mesh.shape["ctx"], mesh.shape["head"]),
        mesh=mesh,
        in_specs=(rows, rows, rows, rows, P("head", None, "ctx")),
        out_specs=(rows, rows, rows, rows),
        check_vma=False,
    )
```

```python
import functools

import jax
import jax.numpy as jnp
from jax import lax
from jax.experimental import pallas as pl
from jax.experimental.pallas import tpu as pltpu
from jax.sharding import PartitionSpec as P

MESH = pl.DeviceIdType.MESH
KEY, VALUE, QUERY, COT = range(4)
TILE = 128


def level_gain(level):
    if level == 0:
        return 1.0
    return 2.0 ** (-(level - 1) / 2.0)


def dot_nn(a, b):
    return lax.dot_general(a, b, (((1,), (0,)), ((), ())), preferred_element_type=jnp.float32)


def dot_nt(a, b):
    return lax.dot_general(a, b, (((1,), (1,)), ((), ())), preferred_element_type=jnp.float32)


def dot_tn(a, b):
    return lax.dot_general(a, b, (((0,), (0,)), ((), ())), preferred_element_type=jnp.float32)


def kernel(
    n_ctx,
    n_head,
    ctx_bits,
    tok_bits,
    query_ref,
    key_ref,
    value_ref,
    cot_ref,
    codes_ref,
    out_ref,
    gq_ref,
    gk_ref,
    gv_ref,
    staged,
    rows_in,
    codes,
    code_rows,
    code_cols,
    levels,
    probs,
    score_grads,
    local,
    rows_out,
    state_send,
    state_parts,
    bucket_send,
    bucket,
    grad_send,
    grad_parts,
    pulled_send,
    pulled,
    stage_sem,
    in_send,
    in_recv,
    own_sem,
    state_sems,
    bucket_send_sem,
    bucket_recv,
    grad_send_sem,
    grad_recv,
    pulled_sems,
    out_send,
    out_recv,
):
    my_ctx = lax.axis_index("ctx")
    my_head = lax.axis_index("head")
    inputs = (key_ref, value_ref, query_ref, cot_ref)
    outputs = (out_ref, gq_ref, gk_ref, gv_ref)
    share = query_ref.shape[0]
    length = share * n_head
    width = query_ref.shape[1] // n_head
    n_local = width // TILE
    state_rows = n_local * TILE
    part = state_rows // n_ctx
    tiles = length // TILE
    scale = TILE ** (-0.5)

    def bit_set(block, bit_index):
        return block // 2**bit_index % 2 == 1

    def own_bit(bit_index):
        return bit_set(my_ctx, bit_index)

    def ctx_peer(step):
        return lax.rem(my_ctx + step, n_ctx)

    def head_columns(head):
        return pl.ds(pl.multiple_of(head * TILE, TILE), TILE)

    def part_rows(owner):
        return pl.ds(pl.multiple_of(owner * part, part), part)

    def share_rows(owner):
        return pl.ds(pl.multiple_of(owner * share, share), share)

    def width_columns(owner):
        return pl.ds(pl.multiple_of(owner * width, width), width)

    barrier = pltpu.get_barrier_semaphore()
    for step in range(1, n_head):
        pl.semaphore_signal(
            barrier, inc=1, device_id={"head": lax.rem(my_head + step, n_head)}, device_id_type=MESH
        )

    @pl.loop(1, n_ctx)
    def _(step):
        pl.semaphore_signal(barrier, inc=1, device_id={"ctx": ctx_peer(step)}, device_id_type=MESH)

    codes_copy = pltpu.make_async_copy(codes_ref, codes, own_sem.at[4])
    codes_copy.start()
    for slot, array in enumerate(inputs):
        pltpu.make_async_copy(
            array.at[:, width_columns(my_head)],
            rows_in.at[slot, share_rows(my_head), :],
            own_sem.at[slot],
        ).start()
        pltpu.make_async_copy(array, staged.at[slot], stage_sem.at[slot]).start()
    pl.semaphore_wait(barrier, n_head - 1 + n_ctx - 1)

    for slot, array in enumerate(inputs):
        pltpu.make_async_copy(array, staged.at[slot], stage_sem.at[slot]).wait()
        for step in range(1, n_head):
            peer = lax.rem(my_head + step, n_head)
            pltpu.make_async_remote_copy(
                src_ref=staged.at[slot, :, width_columns(peer)],
                dst_ref=rows_in.at[slot, share_rows(my_head), :],
                send_sem=in_send.at[slot],
                recv_sem=in_recv.at[slot],
                device_id={"head": peer},
                device_id_type=MESH,
            ).start()

    codes_copy.wait()
    for head in range(n_local):
        code_rows[...] = jnp.zeros_like(code_rows)
        code_rows[0 : codes.shape[0], :] = codes[:, head, :].astype(jnp.float32)
        code_cols[head] = code_rows[...].T
    place = lax.broadcasted_iota(jnp.int32, (TILE, TILE), 0)
    other = lax.broadcasted_iota(jnp.int32, (TILE, TILE), 1)
    differ = place ^ other
    level = jnp.zeros((TILE, TILE), jnp.int32)
    for bit_index in range(7):
        level = level + (differ >= 2**bit_index).astype(jnp.int32)
    levels[...] = jnp.where(other <= place, level, -1)
    for bit_index in range(ctx_bits):

        @pl.when(jnp.logical_not(own_bit(bit_index)))
        def _():
            bucket[bit_index] = jnp.zeros((state_rows, TILE), jnp.bfloat16)

    def arrived(slot):
        pltpu.make_async_copy(
            inputs[slot].at[:, width_columns(my_head)],
            rows_in.at[slot, share_rows(my_head), :],
            own_sem.at[slot],
        ).wait()
        others = rows_in.at[slot, 0 : length - share, :]
        pltpu.make_async_copy(others, others, in_recv.at[slot]).wait()

    def code_column(head, level_index, rows):
        return code_cols[head, rows, level_index : level_index + 1] * (
            level_gain(level_index) * scale / 8.0
        )

    def weighted(head, row, products):
        rows = slice(row * TILE, (row + 1) * TILE)
        pieces = []
        for column in range(row + 1):
            if column == row:
                weight = jnp.zeros((TILE, TILE), jnp.float32)
                for level_index in range(8):
                    weight = jnp.where(
                        levels[...] == level_index, code_column(head, level_index, rows), weight
                    )
            else:
                weight = code_column(head, 7 + (row ^ column).bit_length(), rows)
            at = slice(column * TILE, (column + 1) * TILE)
            pieces.append((weight * products[:, at]).astype(jnp.bfloat16))
        return jnp.concatenate(pieces, axis=1)

    def attend(head):
        columns = head_columns(head)
        for row in range(tiles):
            rows, reach = slice(row * TILE, (row + 1) * TILE), (row + 1) * TILE
            scores = dot_nt(rows_in[QUERY, rows, columns], rows_in[KEY, 0:reach, columns])
            pairs = weighted(head, row, scores)
            probs[head, rows, 0:reach] = pairs
            local[0, rows, columns] = dot_nn(pairs, rows_in[VALUE, 0:reach, columns])

    def attend_back(head):
        columns = head_columns(head)
        for row in range(tiles):
            rows, reach = slice(row * TILE, (row + 1) * TILE), (row + 1) * TILE
            dots = dot_nt(rows_in[COT, rows, columns], rows_in[VALUE, 0:reach, columns])
            pairs = weighted(head, row, dots)
            score_grads[head, rows, 0:reach] = pairs
            local[1, rows, columns] = dot_nn(pairs, rows_in[KEY, 0:reach, columns])

    def sum_back(head):
        columns = head_columns(head)
        for column in range(tiles):
            at, below = slice(column * TILE, (column + 1) * TILE), slice(column * TILE, length)
            local[2, at, columns] = dot_tn(
                score_grads[head, below, at], rows_in[QUERY, below, columns]
            )
            local[3, at, columns] = dot_tn(probs[head, below, at], rows_in[COT, below, columns])

    arrived(KEY)
    arrived(VALUE)

    @pl.loop(0, n_local)
    def _(head):
        columns = head_columns(head)
        state = dot_tn(rows_in[KEY, :, columns], rows_in[VALUE, :, columns])
        state_send[columns, :] = state.astype(jnp.bfloat16)

    @pl.loop(1, n_ctx)
    def _(step):
        peer = ctx_peer(step)
        pltpu.make_async_remote_copy(
            src_ref=state_send.at[part_rows(peer), :],
            dst_ref=state_parts.at[my_ctx],
            send_sem=state_sems.at[0],
            recv_sem=state_sems.at[1],
            device_id={"ctx": peer},
            device_id_type=MESH,
        ).start()

    state_parts[my_ctx] = state_send[part_rows(my_ctx), :]
    arrived(QUERY)
    pl.loop(0, n_local // 2)(attend)
    state_others = state_parts.at[0 : n_ctx - 1]
    pltpu.make_async_copy(state_others, state_others, state_sems.at[1]).wait()

    node = state_parts[...].astype(jnp.float32)
    first_node = []
    count = 0
    for bit_index in range(ctx_bits):
        pairs = node.reshape(node.shape[0] // 2, 2, part, TILE)
        first_node.append(count)
        bucket_send[count : count + pairs.shape[0]] = pairs[:, 0].astype(jnp.bfloat16)
        count += pairs.shape[0]
        node = pairs[:, 0] + pairs[:, 1]

    @pl.loop(1, n_ctx)
    def _(step):
        peer = ctx_peer(step)
        for bit_index in range(ctx_bits):

            @pl.when(bit_set(peer, bit_index))
            def _():
                pltpu.make_async_remote_copy(
                    src_ref=bucket_send.at[first_node[bit_index] + peer // 2 ** (bit_index + 1)],
                    dst_ref=bucket.at[bit_index, part_rows(my_ctx), :],
                    send_sem=bucket_send_sem.at[bit_index],
                    recv_sem=bucket_recv.at[bit_index],
                    device_id={"ctx": peer},
                    device_id_type=MESH,
                ).start()

    for bit_index in range(ctx_bits):

        @pl.when(own_bit(bit_index))
        def _():
            bucket[bit_index, part_rows(my_ctx), :] = bucket_send[
                first_node[bit_index] + my_ctx // 2 ** (bit_index + 1)
            ]

    pl.loop(n_local // 2, n_local)(attend)
    arrived(COT)

    @pl.loop(0, n_local)
    def _(head):
        columns = head_columns(head)
        cot = rows_in[COT, :, columns].astype(jnp.float32)
        scaled = [
            (code_column(head, tok_bits + 1 + bit_index, slice(None)) * cot).astype(jnp.bfloat16)
            for bit_index in range(ctx_bits)
        ]
        grads = dot_tn(rows_in[QUERY, :, columns], jnp.concatenate(scaled, axis=1))
        for bit_index in range(ctx_bits):
            grad_send[bit_index, columns, :] = grads[
                :, bit_index * TILE : (bit_index + 1) * TILE
            ].astype(jnp.bfloat16)

    def grad_slot(block, bit_index):
        return block // 2 ** (bit_index + 1) * 2**bit_index + block % 2**bit_index

    @pl.loop(1, n_ctx)
    def _(step):
        peer = ctx_peer(step)
        for bit_index in range(ctx_bits):

            @pl.when(own_bit(bit_index))
            def _():
                pltpu.make_async_remote_copy(
                    src_ref=grad_send.at[bit_index, part_rows(peer), :],
                    dst_ref=grad_parts.at[bit_index, grad_slot(my_ctx, bit_index)],
                    send_sem=grad_send_sem.at[bit_index],
                    recv_sem=grad_recv.at[bit_index],
                    device_id={"ctx": peer},
                    device_id_type=MESH,
                ).start()

    for bit_index in range(ctx_bits):

        @pl.when(own_bit(bit_index))
        def _():
            grad_parts[bit_index, grad_slot(my_ctx, bit_index)] = grad_send[
                bit_index, part_rows(my_ctx), :
            ]

    pl.loop(0, n_local)(attend_back)
    pl.loop(0, n_local)(sum_back)

    def send_out(slot, columns_of, columns):
        for step in range(1, n_head):
            peer = lax.rem(my_head + step, n_head)
            pltpu.make_async_remote_copy(
                src_ref=rows_out.at[slot, share_rows(peer), columns],
                dst_ref=outputs[slot].at[:, columns_of],
                send_sem=out_send.at[slot],
                recv_sem=out_recv.at[slot],
                device_id={"head": peer},
                device_id_type=MESH,
            ).start()
        outputs[slot][:, columns_of] = rows_out[slot, share_rows(my_head), columns]

    def out_columns(head):
        return pl.ds(pl.multiple_of(my_head * width + head * TILE, TILE), TILE)

    for bit_index in range(ctx_bits):

        @pl.when(own_bit(bit_index))
        def _():
            others = bucket.at[bit_index, 0 : state_rows - part, :]
            pltpu.make_async_copy(others, others, bucket_recv.at[bit_index]).wait()

    @pl.loop(0, n_local)
    def _(head):
        columns = head_columns(head)
        states = [bucket[bit_index, columns, :] for bit_index in range(ctx_bits)]
        wide, tall = jnp.concatenate(states, axis=1), jnp.concatenate(states, axis=0)
        for row in range(tiles):
            rows = slice(row * TILE, (row + 1) * TILE)
            attended, grad_query = local[0, rows, columns], local[1, rows, columns]
            reads = dot_nn(rows_in[QUERY, rows, columns], wide)
            cot_reads = dot_nt(rows_in[COT, rows, columns], tall)
            for bit_index in range(ctx_bits):
                row_scale = code_column(head, tok_bits + 1 + bit_index, rows)
                at = slice(bit_index * TILE, (bit_index + 1) * TILE)
                attended = attended + row_scale * reads[:, at]
                grad_query = grad_query + row_scale * cot_reads[:, at]
            rows_out[0, rows, columns] = attended.astype(jnp.bfloat16)
            rows_out[1, rows, columns] = grad_query.astype(jnp.bfloat16)
        send_out(0, out_columns(head), columns)
        send_out(1, out_columns(head), columns)

    for bit_index in range(ctx_bits):
        half = n_ctx // 2

        @pl.when(own_bit(bit_index))
        def _():
            others = grad_parts.at[bit_index, 0 : half - 1]
            pltpu.make_async_copy(others, others, grad_recv.at[bit_index]).wait()

        @pl.when(jnp.logical_not(own_bit(bit_index)))
        def _():
            others = grad_parts.at[bit_index]
            pltpu.make_async_copy(others, others, grad_recv.at[bit_index]).wait()

    upper = []
    for bit_index in range(ctx_bits):
        terms = grad_parts[bit_index].astype(jnp.float32)
        upper.append(
            jnp.sum(terms.reshape(n_ctx // 2 ** (bit_index + 1), 2**bit_index, part, TILE), axis=1)
        )
    for block in range(n_ctx):
        total = jnp.zeros((part, TILE), jnp.float32)
        for bit_index in range(ctx_bits):
            if not block >> bit_index & 1:
                total = total + upper[bit_index][block >> (bit_index + 1)]
        pulled_send[block] = total.astype(jnp.bfloat16)

    @pl.loop(1, n_ctx)
    def _(step):
        peer = ctx_peer(step)
        pltpu.make_async_remote_copy(
            src_ref=pulled_send.at[peer],
            dst_ref=pulled.at[part_rows(my_ctx), :],
            send_sem=pulled_sems.at[0],
            recv_sem=pulled_sems.at[1],
            device_id={"ctx": peer},
            device_id_type=MESH,
        ).start()

    pulled[part_rows(my_ctx), :] = pulled_send[my_ctx]

    pulled_others = pulled.at[0 : state_rows - part, :]
    pltpu.make_async_copy(pulled_others, pulled_others, pulled_sems.at[1]).wait()

    @pl.loop(0, n_local)
    def _(head):
        columns = head_columns(head)
        states = pulled[columns, :]
        grad_key = local[2, :, columns] + dot_nt(rows_in[VALUE, :, columns], states)
        rows_out[2, :, columns] = grad_key.astype(jnp.bfloat16)
        grad_value = local[3, :, columns] + dot_nn(rows_in[KEY, :, columns], states)
        rows_out[3, :, columns] = grad_value.astype(jnp.bfloat16)
        send_out(2, out_columns(head), columns)
        send_out(3, out_columns(head), columns)

    for slot in range(4):
        sent = rows_in.at[slot, 0 : length - share, :]
        pltpu.make_async_copy(sent, sent, in_send.at[slot]).wait()
    pltpu.make_async_copy(state_others, state_others, state_sems.at[0]).wait()
    pltpu.make_async_copy(pulled_others, pulled_others, pulled_sems.at[0]).wait()
    for bit_index in range(ctx_bits):
        half = n_ctx // 2
        rest = grad_parts.at[bit_index, 0 : half - 1]

        @pl.when(own_bit(bit_index))
        def _():
            pltpu.make_async_copy(rest, rest, bucket_send_sem.at[bit_index]).wait()
            sent = grad_send.at[bit_index, 0 : state_rows - part, :]
            pltpu.make_async_copy(sent, sent, grad_send_sem.at[bit_index]).wait()

        @pl.when(jnp.logical_not(own_bit(bit_index)))
        def _():
            sent = grad_parts.at[bit_index]
            pltpu.make_async_copy(sent, sent, bucket_send_sem.at[bit_index]).wait()

    for slot in range(4):
        sent = rows_out.at[slot, 0 : length - share, :]
        pltpu.make_async_copy(sent, sent, out_send.at[slot]).wait()
        pltpu.make_async_copy(sent, sent, out_recv.at[slot]).wait()


def put_out_kernel(*refs):
    held, results, sems = refs[:4], refs[4:8], refs[8]
    copies = [pltpu.make_async_copy(held[i], results[i], sems.at[i]) for i in range(4)]
    for copy in copies:
        copy.start()
    for copy in copies:
        copy.wait()


def put_out(held):
    return pl.pallas_call(
        put_out_kernel,
        out_shape=tuple(jax.ShapeDtypeStruct(array.shape, array.dtype) for array in held),
        in_specs=[pl.BlockSpec(memory_space=pltpu.VMEM)] * 4,
        out_specs=(pl.BlockSpec(memory_space=pl.ANY),) * 4,
        scratch_shapes=[pltpu.SemaphoreType.DMA((4,))],
        name="put_out",
    )(*held)


def on_device(n_ctx, n_head, query_input, key_input, value_input, cotangent, level_codes):
    share, features = query_input.shape
    n_local, n_levels, length = level_codes.shape
    width = features // n_head
    tok_bits = length.bit_length() - 1
    ctx_bits = n_levels - tok_bits - 1
    state_rows = n_local * TILE
    part = state_rows // n_ctx
    half = jnp.bfloat16
    dma = pltpu.SemaphoreType.DMA
    held = pl.pallas_call(
        functools.partial(kernel, n_ctx, n_head, ctx_bits, tok_bits),
        out_shape=(pltpu.VMEM(query_input.shape, half),) * 4,
        in_specs=[pl.BlockSpec(memory_space=pl.ANY)] * 5,
        out_specs=(pl.BlockSpec(memory_space=pltpu.VMEM),) * 4,
        scratch_shapes=[
            pltpu.VMEM((4, share, features), half),
            pltpu.VMEM((4, length, width), half),
            pltpu.VMEM((n_levels, n_local, length), jnp.int32),
            pltpu.VMEM((TILE, length), jnp.float32),
            pltpu.VMEM((n_local, length, TILE), jnp.float32),
            pltpu.VMEM((TILE, TILE), jnp.int32),
            pltpu.VMEM((n_local, length, length), half),
            pltpu.VMEM((n_local, length, length), half),
            pltpu.VMEM((4, length, width), jnp.float32),
            pltpu.VMEM((4, length, width), half),
            pltpu.VMEM((state_rows, TILE), half),
            pltpu.VMEM((n_ctx, part, TILE), half),
            pltpu.VMEM((n_ctx, part, TILE), half),
            pltpu.VMEM((ctx_bits, state_rows, TILE), half),
            pltpu.VMEM((ctx_bits, state_rows, TILE), half),
            pltpu.VMEM((ctx_bits, n_ctx // 2, part, TILE), half),
            pltpu.VMEM((n_ctx, part, TILE), half),
            pltpu.VMEM((state_rows, TILE), half),
            dma((4,)),
            dma((4,)),
            dma((4,)),
            dma((5,)),
            dma((2,)),
            dma((ctx_bits,)),
            dma((ctx_bits,)),
            dma((ctx_bits,)),
            dma((ctx_bits,)),
            dma((2,)),
            dma((4,)),
            dma((4,)),
        ],
        compiler_params=pltpu.CompilerParams(collective_id=0, has_side_effects=True),
        name="layer",
    )(query_input, key_input, value_input, cotangent, jnp.transpose(level_codes, (1, 0, 2)))
    return put_out([pltpu.with_memory_space_constraint(array, pltpu.VMEM) for array in held])


def solution(mesh):
    rows = P(("ctx", "head"), None)
    return jax.shard_map(
        functools.partial(on_device, mesh.shape["ctx"], mesh.shape["head"]),
        mesh=mesh,
        in_specs=(rows, rows, rows, rows, P("head", None, "ctx")),
        out_specs=(rows, rows, rows, rows),
        check_vma=False,
    )
```

```python
import functools

import jax
import jax.numpy as jnp
from jax import lax
from jax.experimental import pallas as pl
from jax.experimental.pallas import tpu as pltpu
from jax.sharding import PartitionSpec as P

MESH = pl.DeviceIdType.MESH
KEY, VALUE, QUERY, COT = range(4)
TILE = 128
UNITS = 2
Y_SIZE, Y_BITS = 4, 2


def level_gain(level):
    if level == 0:
        return 1.0
    return 2.0 ** (-(level - 1) / 2.0)


def dot_nn(a, b):
    return lax.dot_general(a, b, (((1,), (0,)), ((), ())), preferred_element_type=jnp.float32)


def dot_nt(a, b):
    return lax.dot_general(a, b, (((1,), (1,)), ((), ())), preferred_element_type=jnp.float32)


def dot_tn(a, b):
    return lax.dot_general(a, b, (((0,), (0,)), ((), ())), preferred_element_type=jnp.float32)


def kernel(
    n_ctx,
    n_head,
    ctx_bits,
    tok_bits,
    query_ref,
    key_ref,
    value_ref,
    cot_ref,
    codes_ref,
    out_ref,
    gq_ref,
    gk_ref,
    gv_ref,
    staged,
    rows_in,
    codes,
    code_rows,
    code_cols,
    levels,
    probs,
    score_grads,
    local,
    rows_out,
    state_send,
    state_parts,
    pair_send,
    plane_parts,
    above_send,
    bucket,
    grad_send,
    grad_parts,
    plane_grad_send,
    plane_grad_parts,
    pulled_send,
    pulled_half,
    pulled,
    next_grad,
    stage_sem,
    own_sem,
    in_send,
    in_recv,
    state_send_sem,
    state_recv,
    plane_send_sem,
    plane_recv,
    bucket_send_sem,
    bucket_recv,
    grad_send_sem,
    grad_recv,
    plane_grad_send_sem,
    plane_grad_recv,
    pulled_send_sem,
    pulled_recv,
    next_send_sem,
    next_recv,
    out_send,
    out_recv,
):
    my_ctx = lax.axis_index("ctx")
    my_head = lax.axis_index("head")
    my_y = lax.rem(my_ctx, Y_SIZE)
    my_z = my_ctx // Y_SIZE
    n_z = n_ctx // Y_SIZE
    z_bits = ctx_bits - Y_BITS
    inputs = (key_ref, value_ref, query_ref, cot_ref)
    outputs = (out_ref, gq_ref, gk_ref, gv_ref)
    share = query_ref.shape[0]
    length = share * n_head
    width = query_ref.shape[1] // n_head
    n_local = width // TILE
    unit_heads = n_local // UNITS
    unit_width = width // UNITS
    unit_rows = unit_heads * TILE
    part = unit_rows // Y_SIZE
    tiles = length // TILE
    scale = TILE ** (-0.5)
    f32, half = jnp.float32, jnp.bfloat16

    def z_bit(bit_index):
        return my_z // 2**bit_index % 2 == 1

    def group_start(bit_index):
        return my_z // 2 ** (bit_index + 1) * 2 ** (bit_index + 1)

    def y_peer(step):
        return lax.rem(my_y + step, Y_SIZE)

    def at_y(y):
        return {"ctx": my_z * Y_SIZE + y}

    def at_z(z):
        return {"ctx": z * Y_SIZE + my_y}

    def head_columns(head):
        return pl.ds(pl.multiple_of(head * TILE, TILE), TILE)

    def unit_range(unit):
        return slice(unit * unit_rows, (unit + 1) * unit_rows)

    def part_rows(unit, owner):
        return pl.ds(pl.multiple_of(unit * unit_rows + owner * part, part), part)

    def share_rows(owner):
        return pl.ds(pl.multiple_of(owner * share, share), share)

    def unit_columns(owner, unit):
        return pl.ds(pl.multiple_of(owner * width + unit * unit_width, unit_width), unit_width)

    def send(src, dst, send_sem, recv_sem, device):
        pltpu.make_async_remote_copy(
            src_ref=src,
            dst_ref=dst,
            send_sem=send_sem,
            recv_sem=recv_sem,
            device_id=device,
            device_id_type=MESH,
        ).start()

    def wait(bytes_of, sem):
        pltpu.make_async_copy(bytes_of, bytes_of, sem).wait()

    barrier = pltpu.get_barrier_semaphore()

    def greet(device):
        pl.semaphore_signal(barrier, inc=1, device_id=device, device_id_type=MESH)

    for step in range(1, n_z):
        greet(at_z(lax.rem(my_z + step, n_z)))
    for step in range(1, Y_SIZE):
        greet(at_y(y_peer(step)))
    for step in range(1, n_head):
        greet({"head": lax.rem(my_head + step, n_head)})
    for slot, array in enumerate(inputs):
        pltpu.make_async_copy(array, staged.at[slot], stage_sem.at[slot]).start()
    codes_copy = pltpu.make_async_copy(codes_ref, codes, own_sem.at[0])
    codes_copy.start()
    with jax.named_scope("s_barrier"):
        pl.semaphore_wait(barrier, n_head - 1 + n_z - 1 + Y_SIZE - 1)

    for slot, array in enumerate(inputs):
        pltpu.make_async_copy(array, staged.at[slot], stage_sem.at[slot]).wait()
    for unit in range(UNITS):
        for slot in range(4):
            for step in range(1, n_head):
                peer = lax.rem(my_head + step, n_head)
                send(
                    staged.at[slot, :, unit_columns(peer, unit)],
                    rows_in.at[slot, share_rows(my_head), unit_columns(0, unit)],
                    in_send.at[slot, unit],
                    in_recv.at[slot, unit],
                    {"head": peer},
                )

    for slot in range(4):
        rows_in[slot, share_rows(my_head), :] = staged[
            slot, :, pl.ds(pl.multiple_of(my_head * width, width), width)
        ]
    codes_copy.wait()
    for head in range(n_local):
        code_rows[...] = jnp.zeros_like(code_rows)
        code_rows[0 : codes.shape[0], :] = codes[:, head, :].astype(f32)
        code_cols[head] = code_rows[...].T
    place = lax.broadcasted_iota(jnp.int32, (TILE, TILE), 0)
    other = lax.broadcasted_iota(jnp.int32, (TILE, TILE), 1)
    differ = place ^ other
    level = jnp.zeros((TILE, TILE), jnp.int32)
    for bit_index in range(7):
        level = level + (differ >= 2**bit_index).astype(jnp.int32)
    levels[...] = jnp.where(other <= place, level, -1)

    def is_clear(bit_index):
        return my_ctx // 2**bit_index % 2 == 0

    for bit_index in range(ctx_bits):

        @pl.when(is_clear(bit_index))
        def _():
            bucket[bit_index] = jnp.zeros((n_local * TILE, TILE), half)

    @pl.when(my_y % 2 == 1)
    def _():
        next_grad[...] = jnp.zeros_like(next_grad)

    def arrived(slot, unit):
        others = rows_in.at[slot, 0 : length - share, unit_columns(0, unit)]
        with jax.named_scope("s_in"):
            wait(others, in_recv.at[slot, unit])

    def code_column(head, level_index, rows):
        return code_cols[head, rows, level_index : level_index + 1] * (
            level_gain(level_index) * scale / 8.0
        )

    def weighted(head, row, products):
        rows = slice(row * TILE, (row + 1) * TILE)
        pieces = []
        for column in range(row + 1):
            if column == row:
                weight = jnp.zeros((TILE, TILE), f32)
                for level_index in range(8):
                    weight = jnp.where(
                        levels[...] == level_index, code_column(head, level_index, rows), weight
                    )
            else:
                weight = code_column(head, 7 + (row ^ column).bit_length(), rows)
            at = slice(column * TILE, (column + 1) * TILE)
            pieces.append((weight * products[:, at]).astype(half))
        return jnp.concatenate(pieces, axis=1)

    def each_head(unit, body):
        with jax.named_scope("c_" + body.__name__):
            pl.loop(unit * unit_heads, (unit + 1) * unit_heads)(body)

    def attend(head):
        columns = head_columns(head)
        for row in range(tiles):
            rows, reach = slice(row * TILE, (row + 1) * TILE), (row + 1) * TILE
            scores = dot_nt(rows_in[QUERY, rows, columns], rows_in[KEY, 0:reach, columns])
            pairs = weighted(head, row, scores)
            probs[head, rows, 0:reach] = pairs
            local[0, rows, columns] = dot_nn(pairs, rows_in[VALUE, 0:reach, columns])

    def attend_back(head):
        columns = head_columns(head)
        for row in range(tiles):
            rows, reach = slice(row * TILE, (row + 1) * TILE), (row + 1) * TILE
            dots = dot_nt(rows_in[COT, rows, columns], rows_in[VALUE, 0:reach, columns])
            pairs = weighted(head, row, dots)
            score_grads[head, rows, 0:reach] = pairs
            local[1, rows, columns] = dot_nn(pairs, rows_in[KEY, 0:reach, columns])

    def sum_back(head):
        columns = head_columns(head)
        for column in range(tiles):
            at, below = slice(column * TILE, (column + 1) * TILE), slice(column * TILE, length)
            local[2, at, columns] = dot_tn(
                score_grads[head, below, at], rows_in[QUERY, below, columns]
            )
            local[3, at, columns] = dot_tn(probs[head, below, at], rows_in[COT, below, columns])

    def state_of(head):
        columns = head_columns(head)
        state = dot_tn(rows_in[KEY, :, columns], rows_in[VALUE, :, columns])
        state_send[columns, :] = state.astype(half)

    def send_state(unit):
        each_head(unit, state_of)
        for step in range(1, Y_SIZE):
            peer = y_peer(step)
            send(
                state_send.at[part_rows(unit, peer), :],
                state_parts.at[unit, my_y],
                state_send_sem.at[unit],
                state_recv.at[unit],
                at_y(peer),
            )

        @pl.when(my_y % 2 == 0)
        def _():
            send(
                state_send.at[unit_range(unit), :],
                bucket.at[0, unit_range(unit), :],
                bucket_send_sem.at[unit, 0],
                bucket_recv.at[unit, 0],
                at_y(my_y + 1),
            )

        state_parts[unit, my_y] = state_send[part_rows(unit, my_y), :]

    def send_plane(unit):
        with jax.named_scope("s_state"):
            wait(state_parts.at[unit, 0 : Y_SIZE - 1], state_recv.at[unit])
        lower = state_parts[unit, 0].astype(f32) + state_parts[unit, 1].astype(f32)
        upper = state_parts[unit, 2].astype(f32) + state_parts[unit, 3].astype(f32)
        pair_send[unit, 0] = (lower + upper).astype(half)
        pair_send[unit, 1] = lower.astype(half)
        for step in range(1, n_z):

            @pl.when(my_z + step < n_z)
            def _():
                send(
                    pair_send.at[unit, 0],
                    plane_parts.at[unit, my_z],
                    plane_send_sem.at[unit, step],
                    plane_recv.at[unit, my_z],
                    at_z(my_z + step),
                )

        for y in (2, 3):

            @pl.when(my_y != y)
            def _():
                send(
                    pair_send.at[unit, 1],
                    bucket.at[1, part_rows(unit, my_y), :],
                    bucket_send_sem.at[unit, 1],
                    bucket_recv.at[unit, 1],
                    at_y(y),
                )

            @pl.when(my_y == y)
            def _():
                bucket[1, part_rows(unit, my_y), :] = pair_send[unit, 1]

    def send_above(unit):
        for z in range(n_z - 1):

            @pl.when(z < my_z)
            def _():
                with jax.named_scope("s_plane"):
                    wait(plane_parts.at[unit, z], plane_recv.at[unit, z])

        for bit_index in range(z_bits):

            @pl.when(z_bit(bit_index))
            def _():
                total = jnp.zeros((part, TILE), f32)
                for block in range(2**bit_index):
                    total = total + plane_parts[unit, group_start(bit_index) + block].astype(f32)
                above_send[unit, bit_index] = total.astype(half)
                for step in range(1, Y_SIZE):
                    send(
                        above_send.at[unit, bit_index],
                        bucket.at[Y_BITS + bit_index, part_rows(unit, my_y), :],
                        bucket_send_sem.at[unit, Y_BITS + bit_index],
                        bucket_recv.at[unit, Y_BITS + bit_index],
                        at_y(y_peer(step)),
                    )
                bucket[Y_BITS + bit_index, part_rows(unit, my_y), :] = above_send[unit, bit_index]

    def grad_of(head):
        columns = head_columns(head)
        cot = rows_in[COT, :, columns].astype(f32)
        scaled = [
            (code_column(head, tok_bits + 1 + bit_index, slice(None)) * cot).astype(half)
            for bit_index in range(ctx_bits)
        ]
        grads = dot_tn(rows_in[QUERY, :, columns], jnp.concatenate(scaled, axis=1))
        for bit_index in range(ctx_bits):
            grad_send[bit_index, columns, :] = grads[
                :, bit_index * TILE : (bit_index + 1) * TILE
            ].astype(half)

    def send_grad(unit):
        each_head(unit, grad_of)

        def parts(bit_index):
            for step in range(1, Y_SIZE):
                peer = y_peer(step)
                send(
                    grad_send.at[bit_index, part_rows(unit, peer), :],
                    grad_parts.at[unit, bit_index - 1, my_y],
                    grad_send_sem.at[unit, bit_index - 1],
                    grad_recv.at[unit, bit_index - 1],
                    at_y(peer),
                )
            grad_parts[unit, bit_index - 1, my_y] = grad_send[bit_index, part_rows(unit, my_y), :]

        for bit_index in range(z_bits):

            @pl.when(z_bit(bit_index))
            def _():
                parts(Y_BITS + bit_index)

        @pl.when(my_y >= 2)
        def _():
            parts(1)

        @pl.when(my_y % 2 == 1)
        def _():
            send(
                grad_send.at[0, unit_range(unit), :],
                next_grad.at[unit_range(unit), :],
                next_send_sem.at[unit],
                next_recv.at[unit],
                at_y(my_y - 1),
            )

    def send_plane_grad(unit):
        for bit_index in range(z_bits):

            @pl.when(z_bit(bit_index))
            def _():
                with jax.named_scope("s_grad"):
                    wait(
                        grad_parts.at[unit, 1 + bit_index, 0 : Y_SIZE - 1],
                        grad_recv.at[unit, 1 + bit_index],
                    )
                total = jnp.zeros((part, TILE), f32)
                for y in range(Y_SIZE):
                    total = total + grad_parts[unit, 1 + bit_index, y].astype(f32)
                plane_grad_send[unit, bit_index] = total.astype(half)
                for block in range(2**bit_index):
                    send(
                        plane_grad_send.at[unit, bit_index],
                        plane_grad_parts.at[unit, my_z],
                        plane_grad_send_sem.at[unit, 2**bit_index - 1 + block],
                        plane_grad_recv.at[unit, my_z],
                        at_z(group_start(bit_index) + block),
                    )

    def send_pulled(unit):
        @pl.when(my_y >= 2)
        def _():
            wait(grad_parts.at[unit, 0, 0:1], grad_recv.at[unit, 0])

        @pl.when(my_y < 2)
        def _():
            wait(grad_parts.at[unit, 0, 0:2], grad_recv.at[unit, 0])

        pulled_send[unit, 1] = jnp.zeros((part, TILE), f32)
        for z in range(1, n_z):

            @pl.when(z > my_z)
            def _():
                with jax.named_scope("s_planeg"):
                    wait(plane_grad_parts.at[unit, z], plane_grad_recv.at[unit, z])
                pulled_send[unit, 1] += plane_grad_parts[unit, z].astype(f32)

        later = pulled_send[unit, 1]
        upper = grad_parts[unit, 0, 2].astype(f32) + grad_parts[unit, 0, 3].astype(f32)
        pulled_half[unit, 0] = (later + upper).astype(half)
        pulled_half[unit, 1] = later.astype(half)
        for step in range(1, Y_SIZE):
            peer = y_peer(step)
            send(
                pulled_half.at[unit, peer // 2],
                pulled.at[part_rows(unit, my_y), :],
                pulled_send_sem.at[unit],
                pulled_recv.at[unit],
                at_y(peer),
            )
        pulled[part_rows(unit, my_y), :] = pulled_half[unit, my_y // 2]

    def send_out(slot, head):
        columns = head_columns(head)
        there = pl.ds(pl.multiple_of(my_head * width + head * TILE, TILE), TILE)
        for step in range(1, n_head):
            peer = lax.rem(my_head + step, n_head)
            send(
                rows_out.at[slot, share_rows(peer), columns],
                outputs[slot].at[:, there],
                out_send.at[slot],
                out_recv.at[slot],
                {"head": peer},
            )
        outputs[slot][:, there] = rows_out[slot, share_rows(my_head), columns]

    def cross(head):
        columns = head_columns(head)
        states = [bucket[bit_index, columns, :] for bit_index in range(ctx_bits)]
        wide, tall = jnp.concatenate(states, axis=1), jnp.concatenate(states, axis=0)
        for row in range(tiles):
            rows = slice(row * TILE, (row + 1) * TILE)
            attended, grad_query = local[0, rows, columns], local[1, rows, columns]
            reads = dot_nn(rows_in[QUERY, rows, columns], wide)
            cot_reads = dot_nt(rows_in[COT, rows, columns], tall)
            for bit_index in range(ctx_bits):
                row_scale = code_column(head, tok_bits + 1 + bit_index, rows)
                at = slice(bit_index * TILE, (bit_index + 1) * TILE)
                attended = attended + row_scale * reads[:, at]
                grad_query = grad_query + row_scale * cot_reads[:, at]
            rows_out[0, rows, columns] = attended.astype(half)
            rows_out[1, rows, columns] = grad_query.astype(half)
        send_out(0, head)
        send_out(1, head)

    def read_buckets(unit):
        for bit_index in range(ctx_bits):
            if bit_index == 0:
                whole = bucket.at[0, unit_range(unit), :]
            elif bit_index == 1:
                whole = bucket.at[1, 0 : 3 * part, :]
            else:
                whole = bucket.at[bit_index, 0 : (Y_SIZE - 1) * part, :]

            @pl.when(jnp.logical_not(is_clear(bit_index)))
            def _():
                with jax.named_scope("s_bucket"):
                    wait(whole, bucket_recv.at[unit, bit_index])

        each_head(unit, cross)

    def pull(head):
        columns = head_columns(head)
        states = (pulled[columns, :].astype(f32) + next_grad[columns, :].astype(f32)).astype(half)
        grad_key = local[2, :, columns] + dot_nt(rows_in[VALUE, :, columns], states)
        rows_out[2, :, columns] = grad_key.astype(half)
        grad_value = local[3, :, columns] + dot_nn(rows_in[KEY, :, columns], states)
        rows_out[3, :, columns] = grad_value.astype(half)
        send_out(2, head)
        send_out(3, head)

    def read_pulled(unit):
        @pl.when(my_y % 2 == 0)
        def _():
            wait(next_grad.at[unit_range(unit), :], next_recv.at[unit])

        with jax.named_scope("s_pulled"):
            wait(pulled.at[0 : (Y_SIZE - 1) * part, :], pulled_recv.at[unit])
        each_head(unit, pull)

    arrived(KEY, 0)
    arrived(VALUE, 0)
    send_state(0)
    arrived(QUERY, 0)
    pl.loop(0, 1)(attend)
    send_plane(0)
    arrived(COT, 0)
    send_grad(0)
    pl.loop(1, 2)(attend)
    send_above(0)
    arrived(KEY, 1)
    arrived(VALUE, 1)
    send_state(1)
    send_plane_grad(0)
    each_head(0, attend_back)
    arrived(QUERY, 1)
    pl.loop(2, 3)(attend)
    send_plane(1)
    arrived(COT, 1)
    send_grad(1)
    read_buckets(0)
    send_pulled(0)
    each_head(0, sum_back)
    pl.loop(3, 4)(attend)
    send_above(1)
    send_plane_grad(1)
    read_pulled(0)
    each_head(1, attend_back)
    read_buckets(1)
    send_pulled(1)
    each_head(1, sum_back)
    read_pulled(1)

    for unit in range(UNITS):
        for slot in range(4):
            wait(
                rows_in.at[slot, 0 : length - share, unit_columns(0, unit)],
                in_send.at[slot, unit],
            )
        wait(state_parts.at[unit, 0 : Y_SIZE - 1], state_send_sem.at[unit])
        for step in range(1, n_z):

            @pl.when(my_z + step < n_z)
            def _():
                wait(pair_send.at[unit, 0], plane_send_sem.at[unit, step])

        @pl.when(my_y % 2 == 0)
        def _():
            wait(bucket.at[0, unit_range(unit), :], bucket_send_sem.at[unit, 0])

        @pl.when(my_y % 2 == 1)
        def _():
            wait(next_grad.at[unit_range(unit), :], next_send_sem.at[unit])

        @pl.when(my_y < 2)
        def _():
            wait(bucket.at[1, 0 : 2 * part, :], bucket_send_sem.at[unit, 1])

        @pl.when(my_y >= 2)
        def _():
            wait(bucket.at[1, 0:part, :], bucket_send_sem.at[unit, 1])
            wait(grad_parts.at[unit, 0, 0 : Y_SIZE - 1], grad_send_sem.at[unit, 0])

        for bit_index in range(z_bits):

            @pl.when(z_bit(bit_index))
            def _():
                three = bucket.at[0, 0 : (Y_SIZE - 1) * part, :]
                wait(three, bucket_send_sem.at[unit, Y_BITS + bit_index])
                wait(three, grad_send_sem.at[unit, 1 + bit_index])
                for block in range(2**bit_index):
                    wait(
                        plane_grad_send.at[unit, bit_index],
                        plane_grad_send_sem.at[unit, 2**bit_index - 1 + block],
                    )

        wait(pulled.at[0 : (Y_SIZE - 1) * part, :], pulled_send_sem.at[unit])

    for slot in range(4):
        sent = rows_out.at[slot, 0 : length - share, :]
        wait(sent, out_send.at[slot])
        with jax.named_scope("s_out"):
            wait(sent, out_recv.at[slot])


def put_out_kernel(*refs):
    held, results, sems = refs[:4], refs[4:8], refs[8]
    copies = [pltpu.make_async_copy(held[i], results[i], sems.at[i]) for i in range(4)]
    for copy in copies:
        copy.start()
    for copy in copies:
        copy.wait()


def put_out(held):
    return pl.pallas_call(
        put_out_kernel,
        out_shape=tuple(jax.ShapeDtypeStruct(array.shape, array.dtype) for array in held),
        in_specs=[pl.BlockSpec(memory_space=pltpu.VMEM)] * 4,
        out_specs=(pl.BlockSpec(memory_space=pl.ANY),) * 4,
        scratch_shapes=[pltpu.SemaphoreType.DMA((4,))],
        name="put_out",
    )(*held)


def on_device(n_ctx, n_head, query_input, key_input, value_input, cotangent, level_codes):
    share, features = query_input.shape
    n_local, n_levels, length = level_codes.shape
    width = features // n_head
    tok_bits = length.bit_length() - 1
    ctx_bits = n_levels - tok_bits - 1
    state_rows = n_local * TILE
    part = state_rows // UNITS // Y_SIZE
    n_z = n_ctx // Y_SIZE
    z_bits = ctx_bits - Y_BITS
    half = jnp.bfloat16
    dma = pltpu.SemaphoreType.DMA
    held = pl.pallas_call(
        functools.partial(kernel, n_ctx, n_head, ctx_bits, tok_bits),
        out_shape=(pltpu.VMEM(query_input.shape, half),) * 4,
        in_specs=[pl.BlockSpec(memory_space=pl.ANY)] * 5,
        out_specs=(pl.BlockSpec(memory_space=pltpu.VMEM),) * 4,
        scratch_shapes=[
            pltpu.VMEM((4, share, features), half),
            pltpu.VMEM((4, length, width), half),
            pltpu.VMEM((n_levels, n_local, length), jnp.int32),
            pltpu.VMEM((TILE, length), jnp.float32),
            pltpu.VMEM((n_local, length, TILE), jnp.float32),
            pltpu.VMEM((TILE, TILE), jnp.int32),
            pltpu.VMEM((n_local, length, length), half),
            pltpu.VMEM((n_local, length, length), half),
            pltpu.VMEM((4, length, width), jnp.float32),
            pltpu.VMEM((4, length, width), half),
            pltpu.VMEM((state_rows, TILE), half),
            pltpu.VMEM((UNITS, Y_SIZE, part, TILE), half),
            pltpu.VMEM((UNITS, 2, part, TILE), half),
            pltpu.VMEM((UNITS, n_z, part, TILE), half),
            pltpu.VMEM((UNITS, z_bits, part, TILE), half),
            pltpu.VMEM((ctx_bits, state_rows, TILE), half),
            pltpu.VMEM((ctx_bits, state_rows, TILE), half),
            pltpu.VMEM((UNITS, ctx_bits - 1, Y_SIZE, part, TILE), half),
            pltpu.VMEM((UNITS, z_bits, part, TILE), half),
            pltpu.VMEM((UNITS, n_z, part, TILE), half),
            pltpu.VMEM((UNITS, 2, part, TILE), jnp.float32),
            pltpu.VMEM((UNITS, 2, part, TILE), half),
            pltpu.VMEM((state_rows, TILE), half),
            pltpu.VMEM((state_rows, TILE), half),
            dma((4,)),
            dma((1,)),
            dma((4, UNITS)),
            dma((4, UNITS)),
            dma((UNITS,)),
            dma((UNITS,)),
            dma((UNITS, n_z)),
            dma((UNITS, n_z)),
            dma((UNITS, ctx_bits)),
            dma((UNITS, ctx_bits)),
            dma((UNITS, ctx_bits - 1)),
            dma((UNITS, ctx_bits - 1)),
            dma((UNITS, n_z)),
            dma((UNITS, n_z)),
            dma((UNITS,)),
            dma((UNITS,)),
            dma((UNITS,)),
            dma((UNITS,)),
            dma((4,)),
            dma((4,)),
        ],
        compiler_params=pltpu.CompilerParams(collective_id=0, has_side_effects=True),
        name="layer",
    )(query_input, key_input, value_input, cotangent, jnp.transpose(level_codes, (1, 0, 2)))
    return put_out([pltpu.with_memory_space_constraint(array, pltpu.VMEM) for array in held])


def solution(mesh):
    rows = P(("ctx", "head"), None)
    return jax.shard_map(
        functools.partial(on_device, mesh.shape["ctx"], mesh.shape["head"]),
        mesh=mesh,
        in_specs=(rows, rows, rows, rows, P("head", None, "ctx")),
        out_specs=(rows, rows, rows, rows),
        check_vma=False,
    )
```

```python
import functools

import jax
import jax.numpy as jnp
from jax import lax
from jax.experimental import pallas as pl
from jax.experimental.pallas import tpu as pltpu
from jax.sharding import PartitionSpec as P

MESH = pl.DeviceIdType.MESH
KEY, VALUE, QUERY, COT = range(4)
TILE = 128
UNITS = 2
Y_SIZE, Y_BITS = 4, 2


def level_gain(level):
    if level == 0:
        return 1.0
    return 2.0 ** (-(level - 1) / 2.0)


def dot_nn(a, b):
    return lax.dot_general(a, b, (((1,), (0,)), ((), ())), preferred_element_type=jnp.float32)


def dot_nt(a, b):
    return lax.dot_general(a, b, (((1,), (1,)), ((), ())), preferred_element_type=jnp.float32)


def dot_tn(a, b):
    return lax.dot_general(a, b, (((0,), (0,)), ((), ())), preferred_element_type=jnp.float32)


def kernel(
    n_ctx,
    n_head,
    ctx_bits,
    tok_bits,
    query_ref,
    key_ref,
    value_ref,
    cot_ref,
    codes_ref,
    out_ref,
    gq_ref,
    gk_ref,
    gv_ref,
    staged,
    rows_in,
    codes,
    code_rows,
    code_cols,
    levels,
    probs,
    score_grads,
    local,
    rows_out,
    state_send,
    state_parts,
    pair_send,
    plane_parts,
    above_send,
    bucket,
    grad_send,
    grad_parts,
    plane_grad_send,
    plane_grad_parts,
    pulled_send,
    pulled_half,
    pulled,
    next_grad,
    answer,
    stage_sem,
    own_sem,
    in_send,
    in_recv,
    state_send_sem,
    state_recv,
    plane_send_sem,
    plane_recv,
    bucket_send_sem,
    bucket_recv,
    grad_send_sem,
    grad_recv,
    plane_grad_send_sem,
    plane_grad_recv,
    pulled_send_sem,
    pulled_recv,
    next_send_sem,
    next_recv,
    out_send,
    out_recv,
):
    my_ctx = lax.axis_index("ctx")
    my_head = lax.axis_index("head")
    my_y = lax.rem(my_ctx, Y_SIZE)
    my_z = my_ctx // Y_SIZE
    n_z = n_ctx // Y_SIZE
    z_bits = ctx_bits - Y_BITS
    inputs = (key_ref, value_ref, query_ref, cot_ref)
    outputs = (out_ref, gq_ref, gk_ref, gv_ref)
    share = query_ref.shape[0]
    length = share * n_head
    width = query_ref.shape[1] // n_head
    n_local = width // TILE
    unit_heads = n_local // UNITS
    unit_width = width // UNITS
    unit_rows = unit_heads * TILE
    part = unit_rows // Y_SIZE
    tiles = length // TILE
    scale = TILE ** (-0.5)
    byte_count = grad_send.reshape(ctx_bits * n_local * TILE, TILE)
    f32, half = jnp.float32, jnp.bfloat16

    def z_bit(bit_index):
        return my_z // 2**bit_index % 2 == 1

    z_count = sum(my_z // 2**bit_index % 2 for bit_index in range(z_bits))

    def group_start(bit_index):
        return my_z // 2 ** (bit_index + 1) * 2 ** (bit_index + 1)

    def y_peer(step):
        return lax.rem(my_y + step, Y_SIZE)

    def at_y(y):
        return {"ctx": my_z * Y_SIZE + y}

    def at_z(z):
        return {"ctx": z * Y_SIZE + my_y}

    def head_columns(head):
        return pl.ds(pl.multiple_of(head * TILE, TILE), TILE)

    def unit_range(unit):
        return slice(unit * unit_rows, (unit + 1) * unit_rows)

    def part_rows(unit, owner):
        return pl.ds(pl.multiple_of(unit * unit_rows + owner * part, part), part)

    def share_rows(owner):
        return pl.ds(pl.multiple_of(owner * share, share), share)

    def unit_columns(owner, unit):
        return pl.ds(pl.multiple_of(owner * width + unit * unit_width, unit_width), unit_width)

    def send(src, dst, send_sem, recv_sem, device):
        pltpu.make_async_remote_copy(
            src_ref=src,
            dst_ref=dst,
            send_sem=send_sem,
            recv_sem=recv_sem,
            device_id=device,
            device_id_type=MESH,
        ).start()

    def wait(bytes_of, sem):
        pltpu.make_async_copy(bytes_of, bytes_of, sem).wait()

    barrier = pltpu.get_barrier_semaphore()

    def greet(device):
        pl.semaphore_signal(barrier, inc=1, device_id=device, device_id_type=MESH)

    for z in range(1, n_z):

        @pl.when(z > my_z)
        def _():
            greet(at_z(z))

    for step in range(1, Y_SIZE):
        greet(at_y(y_peer(step)))
    for step in range(1, n_head):
        greet({"head": lax.rem(my_head + step, n_head)})
    for slot, array in enumerate(inputs):
        pltpu.make_async_copy(array, staged.at[slot], stage_sem.at[slot]).start()
    codes_copy = pltpu.make_async_copy(codes_ref, codes, own_sem.at[0])
    codes_copy.start()
    with jax.named_scope("s_barrier"):
        pl.semaphore_wait(barrier, n_head - 1 + Y_SIZE - 1 + my_z)

    for z in range(n_z):

        @pl.when(z < my_z)
        def _():
            pl.semaphore_signal(answer, inc=1, device_id=at_z(z), device_id_type=MESH)


    for slot, array in enumerate(inputs):
        pltpu.make_async_copy(array, staged.at[slot], stage_sem.at[slot]).wait()
    for unit in range(UNITS):
        for slot in range(4):
            for step in range(1, n_head):
                peer = lax.rem(my_head + step, n_head)
                send(
                    staged.at[slot, :, unit_columns(peer, unit)],
                    rows_in.at[slot, share_rows(my_head), unit_columns(0, unit)],
                    in_send,
                    in_recv.at[slot, unit],
                    {"head": peer},
                )

    for slot in range(4):
        rows_in[slot, share_rows(my_head), :] = staged[
            slot, :, pl.ds(pl.multiple_of(my_head * width, width), width)
        ]
    codes_copy.wait()
    for head in range(n_local):
        code_rows[...] = jnp.zeros_like(code_rows)
        code_rows[0 : codes.shape[0], :] = codes[:, head, :].astype(f32)
        code_cols[head] = code_rows[...].T
    place = lax.broadcasted_iota(jnp.int32, (TILE, TILE), 0)
    other = lax.broadcasted_iota(jnp.int32, (TILE, TILE), 1)
    differ = place ^ other
    level = jnp.zeros((TILE, TILE), jnp.int32)
    for bit_index in range(7):
        level = level + (differ >= 2**bit_index).astype(jnp.int32)
    levels[...] = jnp.where(other <= place, level, -1)

    def is_clear(bit_index):
        return my_ctx // 2**bit_index % 2 == 0

    for bit_index in range(ctx_bits):

        @pl.when(is_clear(bit_index))
        def _():
            bucket[bit_index] = jnp.zeros((n_local * TILE, TILE), half)

    @pl.when(my_y % 2 == 1)
    def _():
        next_grad[...] = jnp.zeros_like(next_grad)

    def arrived(slot, unit):
        others = rows_in.at[slot, 0 : length - share, unit_columns(0, unit)]
        with jax.named_scope("s_in"):
            wait(others, in_recv.at[slot, unit])

    def code_column(head, level_index, rows):
        return code_cols[head, rows, level_index : level_index + 1] * (
            level_gain(level_index) * scale / 8.0
        )

    def weighted(head, row, products):
        rows = slice(row * TILE, (row + 1) * TILE)
        pieces = []
        for column in range(row + 1):
            if column == row:
                weight = jnp.zeros((TILE, TILE), f32)
                for level_index in range(8):
                    weight = jnp.where(
                        levels[...] == level_index, code_column(head, level_index, rows), weight
                    )
            else:
                weight = code_column(head, 7 + (row ^ column).bit_length(), rows)
            at = slice(column * TILE, (column + 1) * TILE)
            pieces.append((weight * products[:, at]).astype(half))
        return jnp.concatenate(pieces, axis=1)

    def each_head(unit, body):
        with jax.named_scope("c_" + body.__name__):
            pl.loop(unit * unit_heads, (unit + 1) * unit_heads)(body)

    def attend(head):
        columns = head_columns(head)
        for row in range(tiles):
            rows, reach = slice(row * TILE, (row + 1) * TILE), (row + 1) * TILE
            scores = dot_nt(rows_in[QUERY, rows, columns], rows_in[KEY, 0:reach, columns])
            pairs = weighted(head, row, scores)
            probs[head, rows, 0:reach] = pairs
            local[0, rows, columns] = dot_nn(pairs, rows_in[VALUE, 0:reach, columns])

    def attend_back(head):
        columns = head_columns(head)
        for row in range(tiles):
            rows, reach = slice(row * TILE, (row + 1) * TILE), (row + 1) * TILE
            dots = dot_nt(rows_in[COT, rows, columns], rows_in[VALUE, 0:reach, columns])
            pairs = weighted(head, row, dots)
            score_grads[head, rows, 0:reach] = pairs
            local[1, rows, columns] = dot_nn(pairs, rows_in[KEY, 0:reach, columns])

    def sum_back(head):
        columns = head_columns(head)
        for column in range(tiles):
            at, below = slice(column * TILE, (column + 1) * TILE), slice(column * TILE, length)
            local[2, at, columns] = dot_tn(
                score_grads[head, below, at], rows_in[QUERY, below, columns]
            )
            local[3, at, columns] = dot_tn(probs[head, below, at], rows_in[COT, below, columns])

    def state_of(head):
        columns = head_columns(head)
        state = dot_tn(rows_in[KEY, :, columns], rows_in[VALUE, :, columns])
        state_send[columns, :] = state.astype(half)

    def send_state(unit):
        each_head(unit, state_of)
        for step in range(1, Y_SIZE):
            peer = y_peer(step)
            send(
                state_send.at[part_rows(unit, peer), :],
                state_parts.at[unit, my_y],
                state_send_sem,
                state_recv.at[unit],
                at_y(peer),
            )

        @pl.when(my_y % 2 == 0)
        def _():
            send(
                state_send.at[unit_range(unit), :],
                bucket.at[0, unit_range(unit), :],
                bucket_send_sem.at[0],
                bucket_recv.at[unit, 0],
                at_y(my_y + 1),
            )

        state_parts[unit, my_y] = state_send[part_rows(unit, my_y), :]

    def send_plane(unit):
        with jax.named_scope("s_state"):
            wait(state_parts.at[unit, 0 : Y_SIZE - 1], state_recv.at[unit])
        lower = state_parts[unit, 0].astype(f32) + state_parts[unit, 1].astype(f32)
        upper = state_parts[unit, 2].astype(f32) + state_parts[unit, 3].astype(f32)
        pair_send[unit, 0] = (lower + upper).astype(half)
        pair_send[unit, 1] = lower.astype(half)
        if unit == 0:


            @pl.when(my_z < n_z - 1)
            def _():
                with jax.named_scope("s_answer"):
                    pl.semaphore_wait(answer, n_z - 1 - my_z)

        for step in range(1, n_z):

            @pl.when(my_z + step < n_z)
            def _():
                send(
                    pair_send.at[unit, 0],
                    plane_parts.at[unit, my_z],
                    plane_send_sem,
                    plane_recv.at[unit],
                    at_z(my_z + step),
                )

        for y in (2, 3):

            @pl.when(my_y != y)
            def _():
                send(
                    pair_send.at[unit, 1],
                    bucket.at[1, part_rows(unit, my_y), :],
                    bucket_send_sem.at[1],
                    bucket_recv.at[unit, 0],
                    at_y(y),
                )

            @pl.when(my_y == y)
            def _():
                bucket[1, part_rows(unit, my_y), :] = pair_send[unit, 1]

    def send_above(unit):
        for count in range(1, n_z):

            @pl.when(my_z == count)
            def _():
                with jax.named_scope("s_plane"):
                    wait(plane_parts.at[unit, 0:count], plane_recv.at[unit])

        for bit_index in range(z_bits):

            @pl.when(z_bit(bit_index))
            def _():
                total = jnp.zeros((part, TILE), f32)
                for block in range(2**bit_index):
                    total = total + plane_parts[unit, group_start(bit_index) + block].astype(f32)
                above_send[unit, bit_index] = total.astype(half)
                for step in range(1, Y_SIZE):
                    send(
                        above_send.at[unit, bit_index],
                        bucket.at[Y_BITS + bit_index, part_rows(unit, my_y), :],
                        bucket_send_sem.at[2],
                        bucket_recv.at[unit, 1],
                        at_y(y_peer(step)),
                    )
                bucket[Y_BITS + bit_index, part_rows(unit, my_y), :] = above_send[unit, bit_index]

    def grad_of(head):
        columns = head_columns(head)
        cot = rows_in[COT, :, columns].astype(f32)
        scaled = [
            (code_column(head, tok_bits + 1 + bit_index, slice(None)) * cot).astype(half)
            for bit_index in range(ctx_bits)
        ]
        grads = dot_tn(rows_in[QUERY, :, columns], jnp.concatenate(scaled, axis=1))
        for bit_index in range(ctx_bits):
            grad_send[bit_index, columns, :] = grads[
                :, bit_index * TILE : (bit_index + 1) * TILE
            ].astype(half)

    def send_grad(unit):
        each_head(unit, grad_of)

        def parts(bit_index, kind):
            for step in range(1, Y_SIZE):
                peer = y_peer(step)
                send(
                    grad_send.at[bit_index, part_rows(unit, peer), :],
                    grad_parts.at[unit, bit_index - 1, my_y],
                    grad_send_sem.at[kind],
                    grad_recv.at[unit, kind],
                    at_y(peer),
                )
            grad_parts[unit, bit_index - 1, my_y] = grad_send[bit_index, part_rows(unit, my_y), :]

        for bit_index in range(z_bits):

            @pl.when(z_bit(bit_index))
            def _():
                parts(Y_BITS + bit_index, 1)

        @pl.when(my_y >= 2)
        def _():
            parts(1, 0)

        @pl.when(my_y % 2 == 1)
        def _():
            send(
                grad_send.at[0, unit_range(unit), :],
                next_grad.at[unit_range(unit), :],
                next_send_sem,
                next_recv.at[unit],
                at_y(my_y - 1),
            )

    def send_plane_grad(unit):
        for count in range(1, z_bits + 1):

            @pl.when(z_count == count)
            def _():
                with jax.named_scope("s_grad"):
                    wait(grad_parts.at[unit, 0:count, 0 : Y_SIZE - 1], grad_recv.at[unit, 1])

        for bit_index in range(z_bits):

            @pl.when(z_bit(bit_index))
            def _():
                total = jnp.zeros((part, TILE), f32)
                for y in range(Y_SIZE):
                    total = total + grad_parts[unit, 1 + bit_index, y].astype(f32)
                plane_grad_send[unit, bit_index] = total.astype(half)
                for block in range(2**bit_index):
                    send(
                        plane_grad_send.at[unit, bit_index],
                        plane_grad_parts.at[unit, my_z],
                        plane_grad_send_sem,
                        plane_grad_recv.at[unit],
                        at_z(group_start(bit_index) + block),
                    )

    def send_pulled(unit):
        @pl.when(my_y >= 2)
        def _():
            wait(grad_parts.at[unit, 0, 0:1], grad_recv.at[unit, 0])

        @pl.when(my_y < 2)
        def _():
            wait(grad_parts.at[unit, 0, 0:2], grad_recv.at[unit, 0])

        for count in range(1, n_z):

            @pl.when(n_z - 1 - my_z == count)
            def _():
                with jax.named_scope("s_planeg"):
                    wait(plane_grad_parts.at[unit, 0:count], plane_grad_recv.at[unit])

        pulled_send[...] = jnp.zeros_like(pulled_send)
        for z in range(1, n_z):

            @pl.when(z > my_z)
            def _():
                pulled_send[...] += plane_grad_parts[unit, z].astype(f32)

        later = pulled_send[...]
        upper = grad_parts[unit, 0, 2].astype(f32) + grad_parts[unit, 0, 3].astype(f32)
        pulled_half[unit, 0] = (later + upper).astype(half)
        pulled_half[unit, 1] = later.astype(half)
        for step in range(1, Y_SIZE):
            peer = y_peer(step)
            send(
                pulled_half.at[unit, peer // 2],
                pulled.at[part_rows(unit, my_y), :],
                pulled_send_sem,
                pulled_recv.at[unit],
                at_y(peer),
            )
        pulled[part_rows(unit, my_y), :] = pulled_half[unit, my_y // 2]

    def send_out(slot, head):
        columns = head_columns(head)
        there = pl.ds(pl.multiple_of(my_head * width + head * TILE, TILE), TILE)
        for step in range(1, n_head):
            peer = lax.rem(my_head + step, n_head)
            send(
                rows_out.at[slot, share_rows(peer), columns],
                outputs[slot].at[:, there],
                out_send,
                out_recv,
                {"head": peer},
            )
        outputs[slot][:, there] = rows_out[slot, share_rows(my_head), columns]

    def cross(head):
        columns = head_columns(head)
        states = [bucket[bit_index, columns, :] for bit_index in range(ctx_bits)]
        wide, tall = jnp.concatenate(states, axis=1), jnp.concatenate(states, axis=0)
        for row in range(tiles):
            rows = slice(row * TILE, (row + 1) * TILE)
            attended, grad_query = local[0, rows, columns], local[1, rows, columns]
            reads = dot_nn(rows_in[QUERY, rows, columns], wide)
            cot_reads = dot_nt(rows_in[COT, rows, columns], tall)
            for bit_index in range(ctx_bits):
                row_scale = code_column(head, tok_bits + 1 + bit_index, rows)
                at = slice(bit_index * TILE, (bit_index + 1) * TILE)
                attended = attended + row_scale * reads[:, at]
                grad_query = grad_query + row_scale * cot_reads[:, at]
            rows_out[0, rows, columns] = attended.astype(half)
            rows_out[1, rows, columns] = grad_query.astype(half)
        send_out(0, head)
        send_out(1, head)

    def read_buckets(unit):
        for y, count in ((1, Y_SIZE), (2, Y_SIZE - 1), (3, 2 * Y_SIZE - 1)):

            @pl.when(my_y == y)
            def _():
                with jax.named_scope("s_bucket"):
                    wait(byte_count.at[0 : count * part, :], bucket_recv.at[unit, 0])

        for count in range(1, z_bits + 1):

            @pl.when(z_count == count)
            def _():
                with jax.named_scope("s_bucketz"):
                    wait(
                        byte_count.at[0 : count * (Y_SIZE - 1) * part, :], bucket_recv.at[unit, 1]
                    )

        each_head(unit, cross)

    def pull(head):
        columns = head_columns(head)
        states = (pulled[columns, :].astype(f32) + next_grad[columns, :].astype(f32)).astype(half)
        grad_key = local[2, :, columns] + dot_nt(rows_in[VALUE, :, columns], states)
        rows_out[2, :, columns] = grad_key.astype(half)
        grad_value = local[3, :, columns] + dot_nn(rows_in[KEY, :, columns], states)
        rows_out[3, :, columns] = grad_value.astype(half)
        send_out(2, head)
        send_out(3, head)

    def read_pulled(unit):
        @pl.when(my_y % 2 == 0)
        def _():
            wait(next_grad.at[unit_range(unit), :], next_recv.at[unit])

        with jax.named_scope("s_pulled"):
            wait(pulled.at[0 : (Y_SIZE - 1) * part, :], pulled_recv.at[unit])
        each_head(unit, pull)

    arrived(KEY, 0)
    arrived(VALUE, 0)
    send_state(0)
    arrived(QUERY, 0)
    pl.loop(0, 1)(attend)
    send_plane(0)
    arrived(COT, 0)
    send_grad(0)
    pl.loop(1, 2)(attend)
    send_above(0)
    each_head(0, attend_back)
    arrived(KEY, 1)
    arrived(VALUE, 1)
    send_state(1)
    send_plane_grad(0)
    read_buckets(0)
    arrived(QUERY, 1)
    pl.loop(2, 3)(attend)
    send_plane(1)
    arrived(COT, 1)
    send_grad(1)
    send_pulled(0)
    each_head(0, sum_back)
    pl.loop(3, 4)(attend)
    send_above(1)
    send_plane_grad(1)
    read_pulled(0)
    each_head(1, attend_back)
    read_buckets(1)
    send_pulled(1)
    each_head(1, sum_back)
    read_pulled(1)

    def sent(count, sem):
        wait(byte_count.at[0 : count * UNITS * part, :], sem)

    wait(rows_in.at[:, 0 : length - share, :], in_send)
    sent(Y_SIZE - 1, state_send_sem)
    sent(Y_SIZE - 1, pulled_send_sem)

    @pl.when(my_y % 2 == 0)
    def _():
        sent(Y_SIZE, bucket_send_sem.at[0])

    @pl.when(my_y % 2 == 1)
    def _():
        sent(Y_SIZE, next_send_sem)

    @pl.when(my_y < 2)
    def _():
        sent(2, bucket_send_sem.at[1])

    @pl.when(my_y >= 2)
    def _():
        sent(1, bucket_send_sem.at[1])
        sent(Y_SIZE - 1, grad_send_sem.at[0])

    for count in range(1, z_bits + 1):

        @pl.when(z_count == count)
        def _():
            sent(count * (Y_SIZE - 1), bucket_send_sem.at[2])
            sent(count * (Y_SIZE - 1), grad_send_sem.at[1])

    for count in range(1, n_z):

        @pl.when(my_z == count)
        def _():
            sent(count, plane_grad_send_sem)

        @pl.when(n_z - 1 - my_z == count)
        def _():
            sent(count, plane_send_sem)

    wait(rows_out.at[:, 0 : length - share, :], out_send)
    with jax.named_scope("s_out"):
        wait(rows_out.at[:, 0 : length - share, :], out_recv)


def put_out_kernel(*refs):
    held, results, sems = refs[:4], refs[4:8], refs[8]
    copies = [pltpu.make_async_copy(held[i], results[i], sems.at[i]) for i in range(4)]
    for copy in copies:
        copy.start()
    for copy in copies:
        copy.wait()


def put_out(held):
    return pl.pallas_call(
        put_out_kernel,
        out_shape=tuple(jax.ShapeDtypeStruct(array.shape, array.dtype) for array in held),
        in_specs=[pl.BlockSpec(memory_space=pltpu.VMEM)] * 4,
        out_specs=(pl.BlockSpec(memory_space=pl.ANY),) * 4,
        scratch_shapes=[pltpu.SemaphoreType.DMA((4,))],
        name="put_out",
    )(*held)


def on_device(n_ctx, n_head, query_input, key_input, value_input, cotangent, level_codes):
    share, features = query_input.shape
    n_local, n_levels, length = level_codes.shape
    width = features // n_head
    tok_bits = length.bit_length() - 1
    ctx_bits = n_levels - tok_bits - 1
    state_rows = n_local * TILE
    part = state_rows // UNITS // Y_SIZE
    n_z = n_ctx // Y_SIZE
    z_bits = ctx_bits - Y_BITS
    half = jnp.bfloat16
    dma = pltpu.SemaphoreType.DMA
    held = pl.pallas_call(
        functools.partial(kernel, n_ctx, n_head, ctx_bits, tok_bits),
        out_shape=(pltpu.VMEM(query_input.shape, half),) * 4,
        in_specs=[pl.BlockSpec(memory_space=pl.ANY)] * 5,
        out_specs=(pl.BlockSpec(memory_space=pltpu.VMEM),) * 4,
        scratch_shapes=[
            pltpu.VMEM((4, share, features), half),
            pltpu.VMEM((4, length, width), half),
            pltpu.VMEM((n_levels, n_local, length), jnp.int32),
            pltpu.VMEM((TILE, length), jnp.float32),
            pltpu.VMEM((n_local, length, TILE), jnp.float32),
            pltpu.VMEM((TILE, TILE), jnp.int32),
            pltpu.VMEM((n_local, length, length), half),
            pltpu.VMEM((n_local, length, length), half),
            pltpu.VMEM((4, length, width), jnp.float32),
            pltpu.VMEM((4, length, width), half),
            pltpu.VMEM((state_rows, TILE), half),
            pltpu.VMEM((UNITS, Y_SIZE, part, TILE), half),
            pltpu.VMEM((UNITS, 2, part, TILE), half),
            pltpu.VMEM((UNITS, n_z, part, TILE), half),
            pltpu.VMEM((UNITS, z_bits, part, TILE), half),
            pltpu.VMEM((ctx_bits, state_rows, TILE), half),
            pltpu.VMEM((ctx_bits, state_rows, TILE), half),
            pltpu.VMEM((UNITS, ctx_bits - 1, Y_SIZE, part, TILE), half),
            pltpu.VMEM((UNITS, z_bits, part, TILE), half),
            pltpu.VMEM((UNITS, n_z, part, TILE), half),
            pltpu.VMEM((part, TILE), jnp.float32),
            pltpu.VMEM((UNITS, 2, part, TILE), half),
            pltpu.VMEM((state_rows, TILE), half),
            pltpu.VMEM((state_rows, TILE), half),
            pltpu.SemaphoreType.REGULAR,
            dma((4,)),
            dma((1,)),
            dma,
            dma((4, UNITS)),
            dma,
            dma((UNITS,)),
            dma,
            dma((UNITS,)),
            dma((3,)),
            dma((UNITS, 2)),
            dma((2,)),
            dma((UNITS, 2)),
            dma,
            dma((UNITS,)),
            dma,
            dma((UNITS,)),
            dma,
            dma((UNITS,)),
            dma,
            dma,
        ],
        compiler_params=pltpu.CompilerParams(collective_id=0, has_side_effects=True),
        name="layer",
    )(query_input, key_input, value_input, cotangent, jnp.transpose(level_codes, (1, 0, 2)))
    return put_out([pltpu.with_memory_space_constraint(array, pltpu.VMEM) for array in held])


def solution(mesh):
    rows = P(("ctx", "head"), None)
    return jax.shard_map(
        functools.partial(on_device, mesh.shape["ctx"], mesh.shape["head"]),
        mesh=mesh,
        in_specs=(rows, rows, rows, rows, P("head", None, "ctx")),
        out_specs=(rows, rows, rows, rows),
        check_vma=False,
    )
```

```python
import functools

import jax
import jax.numpy as jnp
from jax import lax
from jax.experimental import pallas as pl
from jax.experimental.pallas import tpu as pltpu
from jax.sharding import PartitionSpec as P

MESH = pl.DeviceIdType.MESH
KEY, VALUE, QUERY, COT = range(4)
TILE = 128
UNITS = 4
Y_SIZE, Y_BITS = 4, 2


def level_gain(level):
    if level == 0:
        return 1.0
    return 2.0 ** (-(level - 1) / 2.0)


def dot_nn(a, b):
    return lax.dot_general(a, b, (((1,), (0,)), ((), ())), preferred_element_type=jnp.float32)


def dot_nt(a, b):
    return lax.dot_general(a, b, (((1,), (1,)), ((), ())), preferred_element_type=jnp.float32)


def dot_tn(a, b):
    return lax.dot_general(a, b, (((0,), (0,)), ((), ())), preferred_element_type=jnp.float32)


def kernel(
    n_ctx,
    n_head,
    ctx_bits,
    tok_bits,
    query_ref,
    key_ref,
    value_ref,
    cot_ref,
    codes_ref,
    out_ref,
    gq_ref,
    gk_ref,
    gv_ref,
    staged,
    rows_in,
    codes,
    code_rows,
    code_cols,
    levels,
    probs,
    score_grads,
    local,
    rows_out,
    state_send,
    state_parts,
    pair_send,
    plane_parts,
    above_send,
    bucket,
    grad_send,
    grad_parts,
    plane_grad_send,
    plane_grad_parts,
    pulled_send,
    pulled_half,
    pulled,
    next_grad,
    answer,
    stage_sem,
    own_sem,
    in_send,
    in_recv,
    state_send_sem,
    state_recv,
    plane_send_sem,
    plane_recv,
    bucket_send_sem,
    bucket_recv,
    grad_send_sem,
    grad_recv,
    plane_grad_send_sem,
    plane_grad_recv,
    pulled_send_sem,
    pulled_recv,
    next_send_sem,
    next_recv,
    out_send,
    out_recv,
):
    my_ctx = lax.axis_index("ctx")
    my_head = lax.axis_index("head")
    my_y = lax.rem(my_ctx, Y_SIZE)
    my_z = my_ctx // Y_SIZE
    n_z = n_ctx // Y_SIZE
    z_bits = ctx_bits - Y_BITS
    inputs = (key_ref, value_ref, query_ref, cot_ref)
    outputs = (out_ref, gq_ref, gk_ref, gv_ref)
    share = query_ref.shape[0]
    length = share * n_head
    width = query_ref.shape[1] // n_head
    n_local = width // TILE
    unit_heads = n_local // UNITS
    unit_width = width // UNITS
    unit_rows = unit_heads * TILE
    part = unit_rows // Y_SIZE
    tiles = length // TILE
    scale = TILE ** (-0.5)
    byte_count = grad_send.reshape(ctx_bits * n_local * TILE, TILE)
    f32, half = jnp.float32, jnp.bfloat16

    def z_bit(bit_index):
        return my_z // 2**bit_index % 2 == 1

    z_count = sum(my_z // 2**bit_index % 2 for bit_index in range(z_bits))

    def group_start(bit_index):
        return my_z // 2 ** (bit_index + 1) * 2 ** (bit_index + 1)

    def y_peer(step):
        return lax.rem(my_y + step, Y_SIZE)

    def at_y(y):
        return {"ctx": my_z * Y_SIZE + y}

    def at_z(z):
        return {"ctx": z * Y_SIZE + my_y}

    def head_columns(head):
        return pl.ds(pl.multiple_of(head * TILE, TILE), TILE)

    def unit_range(unit):
        return slice(unit * unit_rows, (unit + 1) * unit_rows)

    def part_rows(unit, owner):
        return pl.ds(pl.multiple_of(unit * unit_rows + owner * part, part), part)

    def share_rows(owner):
        return pl.ds(pl.multiple_of(owner * share, share), share)

    def unit_columns(owner, unit):
        return pl.ds(pl.multiple_of(owner * width + unit * unit_width, unit_width), unit_width)

    def send(src, dst, send_sem, recv_sem, device):
        pltpu.make_async_remote_copy(
            src_ref=src,
            dst_ref=dst,
            send_sem=send_sem,
            recv_sem=recv_sem,
            device_id=device,
            device_id_type=MESH,
        ).start()

    def wait(bytes_of, sem):
        pltpu.make_async_copy(bytes_of, bytes_of, sem).wait()

    barrier = pltpu.get_barrier_semaphore()

    def greet(device):
        pl.semaphore_signal(barrier, inc=1, device_id=device, device_id_type=MESH)

    for z in range(1, n_z):

        @pl.when(z > my_z)
        def _():
            greet(at_z(z))

    for step in range(1, Y_SIZE):
        greet(at_y(y_peer(step)))
    for step in range(1, n_head):
        greet({"head": lax.rem(my_head + step, n_head)})
    for slot, array in enumerate(inputs):
        pltpu.make_async_copy(array, staged.at[slot], stage_sem.at[slot]).start()
    codes_copy = pltpu.make_async_copy(codes_ref, codes, own_sem.at[0])
    codes_copy.start()
    with jax.named_scope("s_barrier"):
        pl.semaphore_wait(barrier, n_head - 1 + Y_SIZE - 1 + my_z)

    for z in range(n_z):

        @pl.when(z < my_z)
        def _():
            pl.semaphore_signal(answer, inc=1, device_id=at_z(z), device_id_type=MESH)


    for slot, array in enumerate(inputs):
        pltpu.make_async_copy(array, staged.at[slot], stage_sem.at[slot]).wait()
    for unit in range(UNITS):
        for slot in range(4):
            for step in range(1, n_head):
                peer = lax.rem(my_head + step, n_head)
                send(
                    staged.at[slot, :, unit_columns(peer, unit)],
                    rows_in.at[slot, share_rows(my_head), unit_columns(0, unit)],
                    in_send,
                    in_recv.at[slot, unit],
                    {"head": peer},
                )

    for slot in range(4):
        rows_in[slot, share_rows(my_head), :] = staged[
            slot, :, pl.ds(pl.multiple_of(my_head * width, width), width)
        ]
    codes_copy.wait()
    for head in range(n_local):
        code_rows[...] = jnp.zeros_like(code_rows)
        code_rows[0 : codes.shape[0], :] = codes[:, head, :].astype(f32)
        code_cols[head] = code_rows[...].T
    place = lax.broadcasted_iota(jnp.int32, (TILE, TILE), 0)
    other = lax.broadcasted_iota(jnp.int32, (TILE, TILE), 1)
    differ = place ^ other
    level = jnp.zeros((TILE, TILE), jnp.int32)
    for bit_index in range(7):
        level = level + (differ >= 2**bit_index).astype(jnp.int32)
    levels[...] = jnp.where(other <= place, level, -1)

    def is_clear(bit_index):
        return my_ctx // 2**bit_index % 2 == 0

    for bit_index in range(ctx_bits):

        @pl.when(is_clear(bit_index))
        def _():
            bucket[bit_index] = jnp.zeros((n_local * TILE, TILE), half)

    @pl.when(my_y % 2 == 1)
    def _():
        next_grad[...] = jnp.zeros_like(next_grad)

    def arrived(slot, unit):
        others = rows_in.at[slot, 0 : length - share, unit_columns(0, unit)]
        with jax.named_scope("s_in"):
            wait(others, in_recv.at[slot, unit])

    def code_column(head, level_index, rows):
        return code_cols[head, rows, level_index : level_index + 1] * (
            level_gain(level_index) * scale / 8.0
        )

    def weighted(head, row, products):
        rows = slice(row * TILE, (row + 1) * TILE)
        pieces = []
        for column in range(row + 1):
            if column == row:
                weight = jnp.zeros((TILE, TILE), f32)
                for level_index in range(8):
                    weight = jnp.where(
                        levels[...] == level_index, code_column(head, level_index, rows), weight
                    )
            else:
                weight = code_column(head, 7 + (row ^ column).bit_length(), rows)
            at = slice(column * TILE, (column + 1) * TILE)
            pieces.append((weight * products[:, at]).astype(half))
        return jnp.concatenate(pieces, axis=1)

    def each_head(unit, body):
        with jax.named_scope("c_" + body.__name__):
            pl.loop(unit * unit_heads, (unit + 1) * unit_heads)(body)

    def attend(head):
        columns = head_columns(head)
        for row in range(tiles):
            rows, reach = slice(row * TILE, (row + 1) * TILE), (row + 1) * TILE
            scores = dot_nt(rows_in[QUERY, rows, columns], rows_in[KEY, 0:reach, columns])
            pairs = weighted(head, row, scores)
            probs[head, rows, 0:reach] = pairs
            local[0, rows, columns] = dot_nn(pairs, rows_in[VALUE, 0:reach, columns])

    def attend_back(head):
        columns = head_columns(head)
        for row in range(tiles):
            rows, reach = slice(row * TILE, (row + 1) * TILE), (row + 1) * TILE
            dots = dot_nt(rows_in[COT, rows, columns], rows_in[VALUE, 0:reach, columns])
            pairs = weighted(head, row, dots)
            score_grads[head, rows, 0:reach] = pairs
            local[1, rows, columns] = dot_nn(pairs, rows_in[KEY, 0:reach, columns])

    def sum_back(head):
        columns = head_columns(head)
        for column in range(tiles):
            at, below = slice(column * TILE, (column + 1) * TILE), slice(column * TILE, length)
            local[2, at, columns] = dot_tn(
                score_grads[head, below, at], rows_in[QUERY, below, columns]
            )
            local[3, at, columns] = dot_tn(probs[head, below, at], rows_in[COT, below, columns])

    def state_of(head):
        columns = head_columns(head)
        state = dot_tn(rows_in[KEY, :, columns], rows_in[VALUE, :, columns])
        state_send[columns, :] = state.astype(half)

    def send_state(unit):
        each_head(unit, state_of)
        for step in range(1, Y_SIZE):
            peer = y_peer(step)
            send(
                state_send.at[part_rows(unit, peer), :],
                state_parts.at[unit, my_y],
                state_send_sem,
                state_recv.at[unit],
                at_y(peer),
            )

        @pl.when(my_y % 2 == 0)
        def _():
            send(
                state_send.at[unit_range(unit), :],
                bucket.at[0, unit_range(unit), :],
                bucket_send_sem.at[0],
                bucket_recv.at[unit, 0],
                at_y(my_y + 1),
            )

        state_parts[unit, my_y] = state_send[part_rows(unit, my_y), :]

    def send_plane(unit):
        with jax.named_scope("s_state"):
            wait(state_parts.at[unit, 0 : Y_SIZE - 1], state_recv.at[unit])
        lower = state_parts[unit, 0].astype(f32) + state_parts[unit, 1].astype(f32)
        upper = state_parts[unit, 2].astype(f32) + state_parts[unit, 3].astype(f32)
        pair_send[unit, 0] = (lower + upper).astype(half)
        pair_send[unit, 1] = lower.astype(half)
        if unit == 0:


            @pl.when(my_z < n_z - 1)
            def _():
                with jax.named_scope("s_answer"):
                    pl.semaphore_wait(answer, n_z - 1 - my_z)

        for step in range(1, n_z):

            @pl.when(my_z + step < n_z)
            def _():
                send(
                    pair_send.at[unit, 0],
                    plane_parts.at[unit, my_z],
                    plane_send_sem,
                    plane_recv.at[unit],
                    at_z(my_z + step),
                )

        for y in (2, 3):

            @pl.when(my_y != y)
            def _():
                send(
                    pair_send.at[unit, 1],
                    bucket.at[1, part_rows(unit, my_y), :],
                    bucket_send_sem.at[1],
                    bucket_recv.at[unit, 0],
                    at_y(y),
                )

            @pl.when(my_y == y)
            def _():
                bucket[1, part_rows(unit, my_y), :] = pair_send[unit, 1]

    def send_above(unit):
        for count in range(1, n_z):

            @pl.when(my_z == count)
            def _():
                with jax.named_scope("s_plane"):
                    wait(plane_parts.at[unit, 0:count], plane_recv.at[unit])

        for bit_index in range(z_bits):

            @pl.when(z_bit(bit_index))
            def _():
                total = jnp.zeros((part, TILE), f32)
                for block in range(2**bit_index):
                    total = total + plane_parts[unit, group_start(bit_index) + block].astype(f32)
                above_send[unit, bit_index] = total.astype(half)
                for step in range(1, Y_SIZE):
                    send(
                        above_send.at[unit, bit_index],
                        bucket.at[Y_BITS + bit_index, part_rows(unit, my_y), :],
                        bucket_send_sem.at[2],
                        bucket_recv.at[unit, 1],
                        at_y(y_peer(step)),
                    )
                bucket[Y_BITS + bit_index, part_rows(unit, my_y), :] = above_send[unit, bit_index]

    def grad_of(head):
        columns = head_columns(head)
        cot = rows_in[COT, :, columns].astype(f32)
        scaled = [
            (code_column(head, tok_bits + 1 + bit_index, slice(None)) * cot).astype(half)
            for bit_index in range(ctx_bits)
        ]
        grads = dot_tn(rows_in[QUERY, :, columns], jnp.concatenate(scaled, axis=1))
        for bit_index in range(ctx_bits):
            grad_send[bit_index, columns, :] = grads[
                :, bit_index * TILE : (bit_index + 1) * TILE
            ].astype(half)

    def send_grad(unit):
        each_head(unit, grad_of)

        def parts(bit_index, kind):
            for step in range(1, Y_SIZE):
                peer = y_peer(step)
                send(
                    grad_send.at[bit_index, part_rows(unit, peer), :],
                    grad_parts.at[unit, bit_index - 1, my_y],
                    grad_send_sem.at[kind],
                    grad_recv.at[unit, kind],
                    at_y(peer),
                )
            grad_parts[unit, bit_index - 1, my_y] = grad_send[bit_index, part_rows(unit, my_y), :]

        for bit_index in range(z_bits):

            @pl.when(z_bit(bit_index))
            def _():
                parts(Y_BITS + bit_index, 1)

        @pl.when(my_y >= 2)
        def _():
            parts(1, 0)

        @pl.when(my_y % 2 == 1)
        def _():
            send(
                grad_send.at[0, unit_range(unit), :],
                next_grad.at[unit_range(unit), :],
                next_send_sem,
                next_recv.at[unit],
                at_y(my_y - 1),
            )

    def send_plane_grad(unit):
        for count in range(1, z_bits + 1):

            @pl.when(z_count == count)
            def _():
                with jax.named_scope("s_grad"):
                    wait(grad_parts.at[unit, 0:count, 0 : Y_SIZE - 1], grad_recv.at[unit, 1])

        for bit_index in range(z_bits):

            @pl.when(z_bit(bit_index))
            def _():
                total = jnp.zeros((part, TILE), f32)
                for y in range(Y_SIZE):
                    total = total + grad_parts[unit, 1 + bit_index, y].astype(f32)
                plane_grad_send[unit, bit_index] = total.astype(half)
                for block in range(2**bit_index):
                    send(
                        plane_grad_send.at[unit, bit_index],
                        plane_grad_parts.at[unit, my_z],
                        plane_grad_send_sem,
                        plane_grad_recv.at[unit],
                        at_z(group_start(bit_index) + block),
                    )

    def send_pulled(unit):
        @pl.when(my_y >= 2)
        def _():
            wait(grad_parts.at[unit, 0, 0:1], grad_recv.at[unit, 0])

        @pl.when(my_y < 2)
        def _():
            wait(grad_parts.at[unit, 0, 0:2], grad_recv.at[unit, 0])

        for count in range(1, n_z):

            @pl.when(n_z - 1 - my_z == count)
            def _():
                with jax.named_scope("s_planeg"):
                    wait(plane_grad_parts.at[unit, 0:count], plane_grad_recv.at[unit])

        pulled_send[...] = jnp.zeros_like(pulled_send)
        for z in range(1, n_z):

            @pl.when(z > my_z)
            def _():
                pulled_send[...] += plane_grad_parts[unit, z].astype(f32)

        later = pulled_send[...]
        upper = grad_parts[unit, 0, 2].astype(f32) + grad_parts[unit, 0, 3].astype(f32)
        pulled_half[unit, 0] = (later + upper).astype(half)
        pulled_half[unit, 1] = later.astype(half)
        for step in range(1, Y_SIZE):
            peer = y_peer(step)
            send(
                pulled_half.at[unit, peer // 2],
                pulled.at[part_rows(unit, my_y), :],
                pulled_send_sem,
                pulled_recv.at[unit],
                at_y(peer),
            )
        pulled[part_rows(unit, my_y), :] = pulled_half[unit, my_y // 2]

    def send_out(slot, head):
        columns = head_columns(head)
        there = pl.ds(pl.multiple_of(my_head * width + head * TILE, TILE), TILE)
        for step in range(1, n_head):
            peer = lax.rem(my_head + step, n_head)
            send(
                rows_out.at[slot, share_rows(peer), columns],
                outputs[slot].at[:, there],
                out_send,
                out_recv,
                {"head": peer},
            )
        outputs[slot][:, there] = rows_out[slot, share_rows(my_head), columns]

    def cross(head):
        columns = head_columns(head)
        states = [bucket[bit_index, columns, :] for bit_index in range(ctx_bits)]
        wide, tall = jnp.concatenate(states, axis=1), jnp.concatenate(states, axis=0)
        for row in range(tiles):
            rows = slice(row * TILE, (row + 1) * TILE)
            attended, grad_query = local[0, rows, columns], local[1, rows, columns]
            reads = dot_nn(rows_in[QUERY, rows, columns], wide)
            cot_reads = dot_nt(rows_in[COT, rows, columns], tall)
            for bit_index in range(ctx_bits):
                row_scale = code_column(head, tok_bits + 1 + bit_index, rows)
                at = slice(bit_index * TILE, (bit_index + 1) * TILE)
                attended = attended + row_scale * reads[:, at]
                grad_query = grad_query + row_scale * cot_reads[:, at]
            rows_out[0, rows, columns] = attended.astype(half)
            rows_out[1, rows, columns] = grad_query.astype(half)
        send_out(0, head)
        send_out(1, head)

    def read_buckets(unit):
        for y, count in ((1, Y_SIZE), (2, Y_SIZE - 1), (3, 2 * Y_SIZE - 1)):

            @pl.when(my_y == y)
            def _():
                with jax.named_scope("s_bucket"):
                    wait(byte_count.at[0 : count * part, :], bucket_recv.at[unit, 0])

        for count in range(1, z_bits + 1):

            @pl.when(z_count == count)
            def _():
                with jax.named_scope("s_bucketz"):
                    wait(
                        byte_count.at[0 : count * (Y_SIZE - 1) * part, :], bucket_recv.at[unit, 1]
                    )

        each_head(unit, cross)

    def pull(head):
        columns = head_columns(head)
        states = (pulled[columns, :].astype(f32) + next_grad[columns, :].astype(f32)).astype(half)
        grad_key = local[2, :, columns] + dot_nt(rows_in[VALUE, :, columns], states)
        rows_out[2, :, columns] = grad_key.astype(half)
        grad_value = local[3, :, columns] + dot_nn(rows_in[KEY, :, columns], states)
        rows_out[3, :, columns] = grad_value.astype(half)
        send_out(2, head)
        send_out(3, head)

    def read_pulled(unit):
        @pl.when(my_y % 2 == 0)
        def _():
            wait(next_grad.at[unit_range(unit), :], next_recv.at[unit])

        with jax.named_scope("s_pulled"):
            wait(pulled.at[0 : (Y_SIZE - 1) * part, :], pulled_recv.at[unit])
        each_head(unit, pull)

    def step_in(unit):
        arrived(KEY, unit)
        arrived(VALUE, unit)
        send_state(unit)
        if unit >= 2:
            read_buckets(unit - 2)
        arrived(QUERY, unit)
        each_head(unit, attend)
        if unit >= 1:
            send_plane_grad(unit - 1)
            send_above(unit - 1)
        if unit >= 3:
            read_pulled(unit - 3)
        arrived(COT, unit)
        send_grad(unit)
        send_plane(unit)
        if unit >= 2:
            send_pulled(unit - 2)
        each_head(unit, attend_back)
        if unit >= 1:
            each_head(unit - 1, sum_back)

    for unit in range(UNITS):
        step_in(unit)
    last = UNITS - 1
    read_buckets(last - 1)
    send_plane_grad(last)
    send_above(last)
    read_pulled(last - 2)
    send_pulled(last - 1)
    each_head(last, sum_back)
    read_buckets(last)
    read_pulled(last - 1)
    send_pulled(last)
    read_pulled(last)

    def sent(count, sem):
        wait(byte_count.at[0 : count * UNITS * part, :], sem)

    wait(rows_in.at[:, 0 : length - share, :], in_send)
    sent(Y_SIZE - 1, state_send_sem)
    sent(Y_SIZE - 1, pulled_send_sem)

    @pl.when(my_y % 2 == 0)
    def _():
        sent(Y_SIZE, bucket_send_sem.at[0])

    @pl.when(my_y % 2 == 1)
    def _():
        sent(Y_SIZE, next_send_sem)

    @pl.when(my_y < 2)
    def _():
        sent(2, bucket_send_sem.at[1])

    @pl.when(my_y >= 2)
    def _():
        sent(1, bucket_send_sem.at[1])
        sent(Y_SIZE - 1, grad_send_sem.at[0])

    for count in range(1, z_bits + 1):

        @pl.when(z_count == count)
        def _():
            sent(count * (Y_SIZE - 1), bucket_send_sem.at[2])
            sent(count * (Y_SIZE - 1), grad_send_sem.at[1])

    for count in range(1, n_z):

        @pl.when(my_z == count)
        def _():
            sent(count, plane_grad_send_sem)

        @pl.when(n_z - 1 - my_z == count)
        def _():
            sent(count, plane_send_sem)

    wait(rows_out.at[:, 0 : length - share, :], out_send)
    with jax.named_scope("s_out"):
        wait(rows_out.at[:, 0 : length - share, :], out_recv)


def put_out_kernel(*refs):
    held, results, sems = refs[:4], refs[4:8], refs[8]
    copies = [pltpu.make_async_copy(held[i], results[i], sems.at[i]) for i in range(4)]
    for copy in copies:
        copy.start()
    for copy in copies:
        copy.wait()


def put_out(held):
    return pl.pallas_call(
        put_out_kernel,
        out_shape=tuple(jax.ShapeDtypeStruct(array.shape, array.dtype) for array in held),
        in_specs=[pl.BlockSpec(memory_space=pltpu.VMEM)] * 4,
        out_specs=(pl.BlockSpec(memory_space=pl.ANY),) * 4,
        scratch_shapes=[pltpu.SemaphoreType.DMA((4,))],
        name="put_out",
    )(*held)


def on_device(n_ctx, n_head, query_input, key_input, value_input, cotangent, level_codes):
    share, features = query_input.shape
    n_local, n_levels, length = level_codes.shape
    width = features // n_head
    tok_bits = length.bit_length() - 1
    ctx_bits = n_levels - tok_bits - 1
    state_rows = n_local * TILE
    part = state_rows // UNITS // Y_SIZE
    n_z = n_ctx // Y_SIZE
    z_bits = ctx_bits - Y_BITS
    half = jnp.bfloat16
    dma = pltpu.SemaphoreType.DMA
    held = pl.pallas_call(
        functools.partial(kernel, n_ctx, n_head, ctx_bits, tok_bits),
        out_shape=(pltpu.VMEM(query_input.shape, half),) * 4,
        in_specs=[pl.BlockSpec(memory_space=pl.ANY)] * 5,
        out_specs=(pl.BlockSpec(memory_space=pltpu.VMEM),) * 4,
        scratch_shapes=[
            pltpu.VMEM((4, share, features), half),
            pltpu.VMEM((4, length, width), half),
            pltpu.VMEM((n_levels, n_local, length), jnp.int32),
            pltpu.VMEM((TILE, length), jnp.float32),
            pltpu.VMEM((n_local, length, TILE), jnp.float32),
            pltpu.VMEM((TILE, TILE), jnp.int32),
            pltpu.VMEM((n_local, length, length), half),
            pltpu.VMEM((n_local, length, length), half),
            pltpu.VMEM((4, length, width), jnp.float32),
            pltpu.VMEM((4, length, width), half),
            pltpu.VMEM((state_rows, TILE), half),
            pltpu.VMEM((UNITS, Y_SIZE, part, TILE), half),
            pltpu.VMEM((UNITS, 2, part, TILE), half),
            pltpu.VMEM((UNITS, n_z, part, TILE), half),
            pltpu.VMEM((UNITS, z_bits, part, TILE), half),
            pltpu.VMEM((ctx_bits, state_rows, TILE), half),
            pltpu.VMEM((ctx_bits, state_rows, TILE), half),
            pltpu.VMEM((UNITS, ctx_bits - 1, Y_SIZE, part, TILE), half),
            pltpu.VMEM((UNITS, z_bits, part, TILE), half),
            pltpu.VMEM((UNITS, n_z, part, TILE), half),
            pltpu.VMEM((part, TILE), jnp.float32),
            pltpu.VMEM((UNITS, 2, part, TILE), half),
            pltpu.VMEM((state_rows, TILE), half),
            pltpu.VMEM((state_rows, TILE), half),
            pltpu.SemaphoreType.REGULAR,
            dma((4,)),
            dma((1,)),
            dma,
            dma((4, UNITS)),
            dma,
            dma((UNITS,)),
            dma,
            dma((UNITS,)),
            dma((3,)),
            dma((UNITS, 2)),
            dma((2,)),
            dma((UNITS, 2)),
            dma,
            dma((UNITS,)),
            dma,
            dma((UNITS,)),
            dma,
            dma((UNITS,)),
            dma,
            dma,
        ],
        compiler_params=pltpu.CompilerParams(collective_id=0, has_side_effects=True),
        name="layer",
    )(query_input, key_input, value_input, cotangent, jnp.transpose(level_codes, (1, 0, 2)))
    return put_out([pltpu.with_memory_space_constraint(array, pltpu.VMEM) for array in held])


def solution(mesh):
    rows = P(("ctx", "head"), None)
    return jax.shard_map(
        functools.partial(on_device, mesh.shape["ctx"], mesh.shape["head"]),
        mesh=mesh,
        in_specs=(rows, rows, rows, rows, P("head", None, "ctx")),
        out_specs=(rows, rows, rows, rows),
        check_vma=False,
    )
```

```python
import functools

import jax
import jax.numpy as jnp
from jax import lax
from jax.experimental import pallas as pl
from jax.experimental.pallas import tpu as pltpu
from jax.sharding import PartitionSpec as P

MESH = pl.DeviceIdType.MESH
KEY, VALUE, QUERY, COT = range(4)
TILE = 128
UNITS = 4
Y_SIZE, Y_BITS = 4, 2


def level_gain(level):
    if level == 0:
        return 1.0
    return 2.0 ** (-(level - 1) / 2.0)


def dot_nn(a, b):
    return lax.dot_general(a, b, (((1,), (0,)), ((), ())), preferred_element_type=jnp.float32)


def dot_nt(a, b):
    return lax.dot_general(a, b, (((1,), (1,)), ((), ())), preferred_element_type=jnp.float32)


def dot_tn(a, b):
    return lax.dot_general(a, b, (((0,), (0,)), ((), ())), preferred_element_type=jnp.float32)


def kernel(
    n_ctx,
    n_head,
    ctx_bits,
    tok_bits,
    query_ref,
    key_ref,
    value_ref,
    cot_ref,
    codes_ref,
    out_ref,
    gq_ref,
    gk_ref,
    gv_ref,
    staged,
    rows_in,
    codes,
    code_rows,
    code_cols,
    levels,
    probs,
    score_grads,
    local,
    rows_out,
    state_send,
    state_parts,
    pair_send,
    plane_parts,
    above_send,
    bucket,
    grad_send,
    grad_parts,
    plane_grad_send,
    plane_grad_parts,
    pulled_send,
    pulled_half,
    pulled,
    next_grad,
    answer,
    stage_sem,
    own_sem,
    x_send,
    ctx_send,
    in_recv,
    state_recv,
    plane_recv,
    bucket_recv,
    grad_recv,
    plane_grad_recv,
    pulled_recv,
    next_recv,
    out_recv,
):
    my_ctx = lax.axis_index("ctx")
    my_head = lax.axis_index("head")
    my_y = lax.rem(my_ctx, Y_SIZE)
    my_z = my_ctx // Y_SIZE
    n_z = n_ctx // Y_SIZE
    z_bits = ctx_bits - Y_BITS
    inputs = (key_ref, value_ref, query_ref, cot_ref)
    outputs = (out_ref, gq_ref, gk_ref, gv_ref)
    share = query_ref.shape[0]
    length = share * n_head
    width = query_ref.shape[1] // n_head
    n_local = width // TILE
    unit_heads = n_local // UNITS
    unit_width = width // UNITS
    unit_rows = unit_heads * TILE
    part = unit_rows // Y_SIZE
    tiles = length // TILE
    scale = TILE ** (-0.5)
    byte_count = grad_send.reshape(ctx_bits * n_local * TILE, TILE)
    f32, half = jnp.float32, jnp.bfloat16

    def z_bit(bit_index):
        return my_z // 2**bit_index % 2 == 1

    z_count = sum(my_z // 2**bit_index % 2 for bit_index in range(z_bits))

    def group_start(bit_index):
        return my_z // 2 ** (bit_index + 1) * 2 ** (bit_index + 1)

    def y_peer(step):
        return lax.rem(my_y + step, Y_SIZE)

    def at_y(y):
        return {"ctx": my_z * Y_SIZE + y}

    def at_z(z):
        return {"ctx": z * Y_SIZE + my_y}

    def head_columns(head):
        return pl.ds(pl.multiple_of(head * TILE, TILE), TILE)

    def unit_range(unit):
        return slice(unit * unit_rows, (unit + 1) * unit_rows)

    def part_rows(unit, owner):
        return pl.ds(pl.multiple_of(unit * unit_rows + owner * part, part), part)

    def share_rows(owner):
        return pl.ds(pl.multiple_of(owner * share, share), share)

    def unit_columns(owner, unit):
        return pl.ds(pl.multiple_of(owner * width + unit * unit_width, unit_width), unit_width)

    def send(src, dst, send_sem, recv_sem, device):
        pltpu.make_async_remote_copy(
            src_ref=src,
            dst_ref=dst,
            send_sem=send_sem,
            recv_sem=recv_sem,
            device_id=device,
            device_id_type=MESH,
        ).start()

    def wait(bytes_of, sem):
        pltpu.make_async_copy(bytes_of, bytes_of, sem).wait()

    barrier = pltpu.get_barrier_semaphore()

    def greet(device):
        pl.semaphore_signal(barrier, inc=1, device_id=device, device_id_type=MESH)

    for z in range(1, n_z):

        @pl.when(z > my_z)
        def _():
            greet(at_z(z))

    for y in range(1, Y_SIZE):

        @pl.when(y > my_y)
        def _():
            greet(at_y(y))

    for step in range(1, n_head):
        greet({"head": lax.rem(my_head + step, n_head)})
    for slot, array in enumerate(inputs):
        pltpu.make_async_copy(array, staged.at[slot], stage_sem.at[slot]).start()
    codes_copy = pltpu.make_async_copy(codes_ref, codes, own_sem.at[0])
    codes_copy.start()
    with jax.named_scope("s_barrier"):
        pl.semaphore_wait(barrier, n_head - 1 + my_y + my_z)

    for y in range(Y_SIZE - 1):

        @pl.when(y < my_y)
        def _():
            pl.semaphore_signal(answer.at[0], inc=1, device_id=at_y(y), device_id_type=MESH)

    for z in range(n_z - 1):

        @pl.when(z < my_z)
        def _():
            pl.semaphore_signal(answer.at[1], inc=1, device_id=at_z(z), device_id_type=MESH)


    for slot, array in enumerate(inputs):
        pltpu.make_async_copy(array, staged.at[slot], stage_sem.at[slot]).wait()
    for unit in range(UNITS):
        for slot in range(4):
            for step in range(1, n_head):
                peer = lax.rem(my_head + step, n_head)
                send(
                    staged.at[slot, :, unit_columns(peer, unit)],
                    rows_in.at[slot, share_rows(my_head), unit_columns(0, unit)],
                    x_send,
                    in_recv.at[max(slot - 1, 0), unit],
                    {"head": peer},
                )

    for slot in range(4):
        rows_in[slot, share_rows(my_head), :] = staged[
            slot, :, pl.ds(pl.multiple_of(my_head * width, width), width)
        ]
    codes_copy.wait()
    for head in range(n_local):
        code_rows[...] = jnp.zeros_like(code_rows)
        code_rows[0 : codes.shape[0], :] = codes[:, head, :].astype(f32)
        code_cols[head] = code_rows[...].T
    place = lax.broadcasted_iota(jnp.int32, (TILE, TILE), 0)
    other = lax.broadcasted_iota(jnp.int32, (TILE, TILE), 1)
    differ = place ^ other
    level = jnp.zeros((TILE, TILE), jnp.int32)
    for bit_index in range(7):
        level = level + (differ >= 2**bit_index).astype(jnp.int32)
    levels[...] = jnp.where(other <= place, level, -1)

    def is_clear(bit_index):
        return my_ctx // 2**bit_index % 2 == 0

    for bit_index in range(ctx_bits):

        @pl.when(is_clear(bit_index))
        def _():
            bucket[bit_index] = jnp.zeros((n_local * TILE, TILE), half)

    @pl.when(my_y % 2 == 1)
    def _():
        next_grad[...] = jnp.zeros_like(next_grad)

    def arrived(slots, unit):
        others = rows_in.at[slots, 0 : length - share, unit_columns(0, unit)]
        with jax.named_scope("s_in"):
            wait(others, in_recv.at[max(slots.stop - 2, 0), unit])

    def code_column(head, level_index, rows):
        return code_cols[head, rows, level_index : level_index + 1] * (
            level_gain(level_index) * scale / 8.0
        )

    def weighted(head, row, products):
        rows = slice(row * TILE, (row + 1) * TILE)
        pieces = []
        for column in range(row + 1):
            if column == row:
                weight = jnp.zeros((TILE, TILE), f32)
                for level_index in range(8):
                    weight = jnp.where(
                        levels[...] == level_index, code_column(head, level_index, rows), weight
                    )
            else:
                weight = code_column(head, 7 + (row ^ column).bit_length(), rows)
            at = slice(column * TILE, (column + 1) * TILE)
            pieces.append((weight * products[:, at]).astype(half))
        return jnp.concatenate(pieces, axis=1)

    def each_head(unit, body):
        with jax.named_scope("c_" + body.__name__):
            pl.loop(unit * unit_heads, (unit + 1) * unit_heads)(body)

    def attend(head):
        columns = head_columns(head)
        for row in range(tiles):
            rows, reach = slice(row * TILE, (row + 1) * TILE), (row + 1) * TILE
            scores = dot_nt(rows_in[QUERY, rows, columns], rows_in[KEY, 0:reach, columns])
            pairs = weighted(head, row, scores)
            probs[head, rows, 0:reach] = pairs
            local[0, rows, columns] = dot_nn(pairs, rows_in[VALUE, 0:reach, columns])

    def attend_back(head):
        columns = head_columns(head)
        for row in range(tiles):
            rows, reach = slice(row * TILE, (row + 1) * TILE), (row + 1) * TILE
            dots = dot_nt(rows_in[COT, rows, columns], rows_in[VALUE, 0:reach, columns])
            pairs = weighted(head, row, dots)
            score_grads[head, rows, 0:reach] = pairs
            local[1, rows, columns] = dot_nn(pairs, rows_in[KEY, 0:reach, columns])

    def sum_back(head):
        columns = head_columns(head)
        for column in range(tiles):
            at, below = slice(column * TILE, (column + 1) * TILE), slice(column * TILE, length)
            local[2, at, columns] = dot_tn(
                score_grads[head, below, at], rows_in[QUERY, below, columns]
            )
            local[3, at, columns] = dot_tn(probs[head, below, at], rows_in[COT, below, columns])

    def state_of(head):
        columns = head_columns(head)
        state = dot_tn(rows_in[KEY, :, columns], rows_in[VALUE, :, columns])
        state_send[columns, :] = state.astype(half)

    def send_state(unit):
        each_head(unit, state_of)
        if unit == 0:

            @pl.when(my_y < Y_SIZE - 1)
            def _():
                with jax.named_scope("s_answery"):
                    pl.semaphore_wait(answer.at[0], Y_SIZE - 1 - my_y)

        for step in range(1, Y_SIZE):
            peer = y_peer(step)
            send(
                state_send.at[part_rows(unit, peer), :],
                state_parts.at[unit, my_y],
                ctx_send,
                state_recv.at[unit],
                at_y(peer),
            )

        @pl.when(my_y % 2 == 0)
        def _():
            send(
                state_send.at[unit_range(unit), :],
                bucket.at[0, unit_range(unit), :],
                ctx_send,
                bucket_recv.at[unit, 0],
                at_y(my_y + 1),
            )

        state_parts[unit, my_y] = state_send[part_rows(unit, my_y), :]

    def send_plane(unit):
        with jax.named_scope("s_state"):
            wait(state_parts.at[unit, 0 : Y_SIZE - 1], state_recv.at[unit])
        lower = state_parts[unit, 0].astype(f32) + state_parts[unit, 1].astype(f32)
        upper = state_parts[unit, 2].astype(f32) + state_parts[unit, 3].astype(f32)
        pair_send[unit, 0] = (lower + upper).astype(half)
        pair_send[unit, 1] = lower.astype(half)
        if unit == 0:


            @pl.when(my_z < n_z - 1)
            def _():
                with jax.named_scope("s_answer"):
                    pl.semaphore_wait(answer.at[1], n_z - 1 - my_z)

        for step in range(1, n_z):

            @pl.when(my_z + step < n_z)
            def _():
                send(
                    pair_send.at[unit, 0],
                    plane_parts.at[unit, my_z],
                    ctx_send,
                    plane_recv.at[unit],
                    at_z(my_z + step),
                )

        for y in (2, 3):

            @pl.when(my_y != y)
            def _():
                send(
                    pair_send.at[unit, 1],
                    bucket.at[1, part_rows(unit, my_y), :],
                    ctx_send,
                    bucket_recv.at[unit, 0],
                    at_y(y),
                )

            @pl.when(my_y == y)
            def _():
                bucket[1, part_rows(unit, my_y), :] = pair_send[unit, 1]

    def send_above(unit):
        for count in range(1, n_z):

            @pl.when(my_z == count)
            def _():
                with jax.named_scope("s_plane"):
                    wait(plane_parts.at[unit, 0:count], plane_recv.at[unit])

        for bit_index in range(z_bits):

            @pl.when(z_bit(bit_index))
            def _():
                total = jnp.zeros((part, TILE), f32)
                for block in range(2**bit_index):
                    total = total + plane_parts[unit, group_start(bit_index) + block].astype(f32)
                above_send[unit, bit_index] = total.astype(half)
                for step in range(1, Y_SIZE):
                    send(
                        above_send.at[unit, bit_index],
                        bucket.at[Y_BITS + bit_index, part_rows(unit, my_y), :],
                        ctx_send,
                        bucket_recv.at[unit, 1],
                        at_y(y_peer(step)),
                    )
                bucket[Y_BITS + bit_index, part_rows(unit, my_y), :] = above_send[unit, bit_index]

    def grad_of(head):
        columns = head_columns(head)
        cot = rows_in[COT, :, columns].astype(f32)
        scaled = [
            (code_column(head, tok_bits + 1 + bit_index, slice(None)) * cot).astype(half)
            for bit_index in range(ctx_bits)
        ]
        grads = dot_tn(rows_in[QUERY, :, columns], jnp.concatenate(scaled, axis=1))
        for bit_index in range(ctx_bits):
            grad_send[bit_index, columns, :] = grads[
                :, bit_index * TILE : (bit_index + 1) * TILE
            ].astype(half)

    def send_grad(unit):
        each_head(unit, grad_of)

        def parts(bit_index, kind):
            for step in range(1, Y_SIZE):
                peer = y_peer(step)
                send(
                    grad_send.at[bit_index, part_rows(unit, peer), :],
                    grad_parts.at[unit, bit_index - 1, my_y],
                    ctx_send,
                    grad_recv.at[unit, kind],
                    at_y(peer),
                )
            grad_parts[unit, bit_index - 1, my_y] = grad_send[bit_index, part_rows(unit, my_y), :]

        for bit_index in range(z_bits):

            @pl.when(z_bit(bit_index))
            def _():
                parts(Y_BITS + bit_index, 1)

        @pl.when(my_y >= 2)
        def _():
            parts(1, 0)

        @pl.when(my_y % 2 == 1)
        def _():
            send(
                grad_send.at[0, unit_range(unit), :],
                next_grad.at[unit_range(unit), :],
                ctx_send,
                next_recv.at[unit],
                at_y(my_y - 1),
            )

    def send_plane_grad(unit):
        for count in range(1, z_bits + 1):

            @pl.when(z_count == count)
            def _():
                with jax.named_scope("s_grad"):
                    wait(grad_parts.at[unit, 0:count, 0 : Y_SIZE - 1], grad_recv.at[unit, 1])

        for bit_index in range(z_bits):

            @pl.when(z_bit(bit_index))
            def _():
                total = jnp.zeros((part, TILE), f32)
                for y in range(Y_SIZE):
                    total = total + grad_parts[unit, 1 + bit_index, y].astype(f32)
                plane_grad_send[unit, bit_index] = total.astype(half)
                for block in range(2**bit_index):
                    send(
                        plane_grad_send.at[unit, bit_index],
                        plane_grad_parts.at[unit, my_z],
                        ctx_send,
                        plane_grad_recv.at[unit],
                        at_z(group_start(bit_index) + block),
                    )

    def send_pulled(unit):
        @pl.when(my_y >= 2)
        def _():
            wait(grad_parts.at[unit, 0, 0:1], grad_recv.at[unit, 0])

        @pl.when(my_y < 2)
        def _():
            wait(grad_parts.at[unit, 0, 0:2], grad_recv.at[unit, 0])

        for count in range(1, n_z):

            @pl.when(n_z - 1 - my_z == count)
            def _():
                with jax.named_scope("s_planeg"):
                    wait(plane_grad_parts.at[unit, 0:count], plane_grad_recv.at[unit])

        pulled_send[...] = jnp.zeros_like(pulled_send)
        for z in range(1, n_z):

            @pl.when(z > my_z)
            def _():
                pulled_send[...] += plane_grad_parts[unit, z].astype(f32)

        later = pulled_send[...]
        upper = grad_parts[unit, 0, 2].astype(f32) + grad_parts[unit, 0, 3].astype(f32)
        pulled_half[unit, 0] = (later + upper).astype(half)
        pulled_half[unit, 1] = later.astype(half)
        for step in range(1, Y_SIZE):
            peer = y_peer(step)
            send(
                pulled_half.at[unit, peer // 2],
                pulled.at[part_rows(unit, my_y), :],
                ctx_send,
                pulled_recv.at[unit],
                at_y(peer),
            )
        pulled[part_rows(unit, my_y), :] = pulled_half[unit, my_y // 2]

    def send_out(slot, head):
        columns = head_columns(head)
        there = pl.ds(pl.multiple_of(my_head * width + head * TILE, TILE), TILE)
        for step in range(1, n_head):
            peer = lax.rem(my_head + step, n_head)
            send(
                rows_out.at[slot, share_rows(peer), columns],
                outputs[slot].at[:, there],
                x_send,
                out_recv,
                {"head": peer},
            )
        outputs[slot][:, there] = rows_out[slot, share_rows(my_head), columns]

    def cross(head):
        columns = head_columns(head)
        states = [bucket[bit_index, columns, :] for bit_index in range(ctx_bits)]
        wide, tall = jnp.concatenate(states, axis=1), jnp.concatenate(states, axis=0)
        for row in range(tiles):
            rows = slice(row * TILE, (row + 1) * TILE)
            attended, grad_query = local[0, rows, columns], local[1, rows, columns]
            reads = dot_nn(rows_in[QUERY, rows, columns], wide)
            cot_reads = dot_nt(rows_in[COT, rows, columns], tall)
            for bit_index in range(ctx_bits):
                row_scale = code_column(head, tok_bits + 1 + bit_index, rows)
                at = slice(bit_index * TILE, (bit_index + 1) * TILE)
                attended = attended + row_scale * reads[:, at]
                grad_query = grad_query + row_scale * cot_reads[:, at]
            rows_out[0, rows, columns] = attended.astype(half)
            rows_out[1, rows, columns] = grad_query.astype(half)
        send_out(0, head)
        send_out(1, head)

    def read_buckets(unit):
        for y, count in ((1, Y_SIZE), (2, Y_SIZE - 1), (3, 2 * Y_SIZE - 1)):

            @pl.when(my_y == y)
            def _():
                with jax.named_scope("s_bucket"):
                    wait(byte_count.at[0 : count * part, :], bucket_recv.at[unit, 0])

        for count in range(1, z_bits + 1):

            @pl.when(z_count == count)
            def _():
                with jax.named_scope("s_bucketz"):
                    wait(
                        byte_count.at[0 : count * (Y_SIZE - 1) * part, :], bucket_recv.at[unit, 1]
                    )

        each_head(unit, cross)

    def pull(head):
        columns = head_columns(head)
        states = (pulled[columns, :].astype(f32) + next_grad[columns, :].astype(f32)).astype(half)
        grad_key = local[2, :, columns] + dot_nt(rows_in[VALUE, :, columns], states)
        rows_out[2, :, columns] = grad_key.astype(half)
        grad_value = local[3, :, columns] + dot_nn(rows_in[KEY, :, columns], states)
        rows_out[3, :, columns] = grad_value.astype(half)
        send_out(2, head)
        send_out(3, head)

    def read_pulled(unit):
        @pl.when(my_y % 2 == 0)
        def _():
            wait(next_grad.at[unit_range(unit), :], next_recv.at[unit])

        with jax.named_scope("s_pulled"):
            wait(pulled.at[0 : (Y_SIZE - 1) * part, :], pulled_recv.at[unit])
        each_head(unit, pull)

    def step_in(unit):
        arrived(slice(KEY, VALUE + 1), unit)
        send_state(unit)
        if unit >= 2:
            read_buckets(unit - 2)
        arrived(slice(QUERY, QUERY + 1), unit)
        each_head(unit, attend)
        if unit >= 1:
            send_plane_grad(unit - 1)
            send_above(unit - 1)
        if unit >= 3:
            read_pulled(unit - 3)
        arrived(slice(COT, COT + 1), unit)
        send_grad(unit)
        send_plane(unit)
        if unit >= 2:
            send_pulled(unit - 2)
        each_head(unit, attend_back)
        if unit >= 1:
            each_head(unit - 1, sum_back)

    for unit in range(UNITS):
        step_in(unit)
    last = UNITS - 1
    read_buckets(last - 1)
    send_plane_grad(last)
    send_above(last)
    read_pulled(last - 2)
    send_pulled(last - 1)
    each_head(last, sum_back)
    read_buckets(last)
    read_pulled(last - 1)
    send_pulled(last)
    read_pulled(last)

    flat = local.reshape(local.shape[0] * length, width)
    part_bytes = UNITS * part * TILE * 2 // (width * 4)
    for low in (True, False):
        for count in range(z_bits + 1):

            @pl.when(((my_y < 2) == low) & (z_count == count))
            def _():
                parts = 2 * (Y_SIZE - 1) + Y_SIZE + n_z - 1
                parts += (2 if low else 4) + 2 * (Y_SIZE - 1) * count
                wait(flat.at[0 : parts * part_bytes, :], ctx_send)

    wait(local.at[:, 0 : length - share, :], x_send)
    with jax.named_scope("s_out"):
        wait(rows_out.at[:, 0 : length - share, :], out_recv)


def put_out_kernel(*refs):
    held, results, sems = refs[:4], refs[4:8], refs[8]
    copies = [pltpu.make_async_copy(held[i], results[i], sems.at[i]) for i in range(4)]
    for copy in copies:
        copy.start()
    for copy in copies:
        copy.wait()


def put_out(held):
    return pl.pallas_call(
        put_out_kernel,
        out_shape=tuple(jax.ShapeDtypeStruct(array.shape, array.dtype) for array in held),
        in_specs=[pl.BlockSpec(memory_space=pltpu.VMEM)] * 4,
        out_specs=(pl.BlockSpec(memory_space=pl.ANY),) * 4,
        scratch_shapes=[pltpu.SemaphoreType.DMA((4,))],
        name="put_out",
    )(*held)


def on_device(n_ctx, n_head, query_input, key_input, value_input, cotangent, level_codes):
    share, features = query_input.shape
    n_local, n_levels, length = level_codes.shape
    width = features // n_head
    tok_bits = length.bit_length() - 1
    ctx_bits = n_levels - tok_bits - 1
    state_rows = n_local * TILE
    part = state_rows // UNITS // Y_SIZE
    n_z = n_ctx // Y_SIZE
    z_bits = ctx_bits - Y_BITS
    half = jnp.bfloat16
    dma = pltpu.SemaphoreType.DMA
    held = pl.pallas_call(
        functools.partial(kernel, n_ctx, n_head, ctx_bits, tok_bits),
        out_shape=(pltpu.VMEM(query_input.shape, half),) * 4,
        in_specs=[pl.BlockSpec(memory_space=pl.ANY)] * 5,
        out_specs=(pl.BlockSpec(memory_space=pltpu.VMEM),) * 4,
        scratch_shapes=[
            pltpu.VMEM((4, share, features), half),
            pltpu.VMEM((4, length, width), half),
            pltpu.VMEM((n_levels, n_local, length), jnp.int32),
            pltpu.VMEM((TILE, length), jnp.float32),
            pltpu.VMEM((n_local, length, TILE), jnp.float32),
            pltpu.VMEM((TILE, TILE), jnp.int32),
            pltpu.VMEM((n_local, length, length), half),
            pltpu.VMEM((n_local, length, length), half),
            pltpu.VMEM((4, length, width), jnp.float32),
            pltpu.VMEM((4, length, width), half),
            pltpu.VMEM((state_rows, TILE), half),
            pltpu.VMEM((UNITS, Y_SIZE, part, TILE), half),
            pltpu.VMEM((UNITS, 2, part, TILE), half),
            pltpu.VMEM((UNITS, n_z, part, TILE), half),
            pltpu.VMEM((UNITS, z_bits, part, TILE), half),
            pltpu.VMEM((ctx_bits, state_rows, TILE), half),
            pltpu.VMEM((ctx_bits, state_rows, TILE), half),
            pltpu.VMEM((UNITS, ctx_bits - 1, Y_SIZE, part, TILE), half),
            pltpu.VMEM((UNITS, z_bits, part, TILE), half),
            pltpu.VMEM((UNITS, n_z, part, TILE), half),
            pltpu.VMEM((part, TILE), jnp.float32),
            pltpu.VMEM((UNITS, 2, part, TILE), half),
            pltpu.VMEM((state_rows, TILE), half),
            pltpu.VMEM((state_rows, TILE), half),
            pltpu.SemaphoreType.REGULAR((2,)),
            dma((4,)),
            dma((1,)),
            dma,
            dma,
            dma((3, UNITS)),
            dma((UNITS,)),
            dma((UNITS,)),
            dma((UNITS, 2)),
            dma((UNITS, 2)),
            dma((UNITS,)),
            dma((UNITS,)),
            dma((UNITS,)),
            dma,
        ],
        compiler_params=pltpu.CompilerParams(collective_id=0, has_side_effects=True),
        name="layer",
    )(query_input, key_input, value_input, cotangent, jnp.transpose(level_codes, (1, 0, 2)))
    return put_out([pltpu.with_memory_space_constraint(array, pltpu.VMEM) for array in held])


def solution(mesh):
    rows = P(("ctx", "head"), None)
    return jax.shard_map(
        functools.partial(on_device, mesh.shape["ctx"], mesh.shape["head"]),
        mesh=mesh,
        in_specs=(rows, rows, rows, rows, P("head", None, "ctx")),
        out_specs=(rows, rows, rows, rows),
        check_vma=False,
    )
```

```python
import functools

import jax
import jax.numpy as jnp
from jax import lax
from jax.experimental import pallas as pl
from jax.experimental.pallas import tpu as pltpu
from jax.sharding import PartitionSpec as P

MESH = pl.DeviceIdType.MESH
KEY, VALUE, QUERY, COT = range(4)
TILE = 128
UNITS = 4
Y_SIZE, Y_BITS = 4, 2


def level_gain(level):
    if level == 0:
        return 1.0
    return 2.0 ** (-(level - 1) / 2.0)


def dot_nn(a, b):
    return lax.dot_general(a, b, (((1,), (0,)), ((), ())), preferred_element_type=jnp.float32)


def dot_nt(a, b):
    return lax.dot_general(a, b, (((1,), (1,)), ((), ())), preferred_element_type=jnp.float32)


def dot_tn(a, b):
    return lax.dot_general(a, b, (((0,), (0,)), ((), ())), preferred_element_type=jnp.float32)


def kernel(
    n_ctx,
    n_head,
    ctx_bits,
    tok_bits,
    query_ref,
    key_ref,
    value_ref,
    cot_ref,
    codes_ref,
    out_ref,
    gq_ref,
    gk_ref,
    gv_ref,
    staged,
    rows_in,
    codes,
    code_rows,
    code_cols,
    levels,
    probs,
    score_grads,
    local,
    rows_out,
    state_send,
    state_parts,
    pair_send,
    plane_parts,
    above_send,
    bucket,
    grad_send,
    grad_parts,
    plane_grad_send,
    plane_grad_parts,
    pulled_send,
    pulled_half,
    pulled,
    next_grad,
    answer,
    stage_sem,
    own_sem,
    x_send,
    ctx_send,
    in_recv,
    state_recv,
    plane_recv,
    bucket_recv,
    grad_recv,
    plane_grad_recv,
    pulled_recv,
    next_recv,
    out_recv,
):
    my_ctx = lax.axis_index("ctx")
    my_head = lax.axis_index("head")
    my_y = lax.rem(my_ctx, Y_SIZE)
    my_z = my_ctx // Y_SIZE
    n_z = n_ctx // Y_SIZE
    z_bits = ctx_bits - Y_BITS
    inputs = (key_ref, value_ref, query_ref, cot_ref)
    outputs = (out_ref, gq_ref, gk_ref, gv_ref)
    share = query_ref.shape[0]
    length = share * n_head
    width = query_ref.shape[1] // n_head
    n_local = width // TILE
    unit_heads = n_local // UNITS
    unit_width = width // UNITS
    unit_rows = unit_heads * TILE
    part = unit_rows // Y_SIZE
    tiles = length // TILE
    scale = TILE ** (-0.5)
    byte_count = grad_send.reshape(ctx_bits * n_local * TILE, TILE)
    f32, half = jnp.float32, jnp.bfloat16

    def z_bit(bit_index):
        return my_z // 2**bit_index % 2 == 1

    z_count = sum(my_z // 2**bit_index % 2 for bit_index in range(z_bits))

    def group_start(bit_index):
        return my_z // 2 ** (bit_index + 1) * 2 ** (bit_index + 1)

    def y_peer(step):
        return lax.rem(my_y + step, Y_SIZE)

    chips = n_head // 2
    far = chips // 2
    near = [step for reach in range(far - 1, 0, -1) for step in (reach, chips - reach)]
    line = [
        lax.rem(my_head // 2 + step, chips) * 2 + lax.rem(my_head + core, 2)
        for step, core in [(far, 0), (far, 1)] + [(step, core) for core in (0, 1) for step in near]
        if step
    ] + [my_head // 2 * 2 + lax.rem(my_head + 1, 2)]

    def at_y(y):
        return {"ctx": my_z * Y_SIZE + y}

    def at_z(z):
        return {"ctx": z * Y_SIZE + my_y}

    def head_columns(head):
        return pl.ds(pl.multiple_of(head * TILE, TILE), TILE)

    def unit_range(unit):
        return slice(unit * unit_rows, (unit + 1) * unit_rows)

    def part_rows(unit, owner):
        return pl.ds(pl.multiple_of(unit * unit_rows + owner * part, part), part)

    def share_rows(owner):
        return pl.ds(pl.multiple_of(owner * share, share), share)

    def unit_columns(owner, unit):
        return pl.ds(pl.multiple_of(owner * width + unit * unit_width, unit_width), unit_width)

    def send(src, dst, send_sem, recv_sem, device):
        pltpu.make_async_remote_copy(
            src_ref=src,
            dst_ref=dst,
            send_sem=send_sem,
            recv_sem=recv_sem,
            device_id=device,
            device_id_type=MESH,
        ).start()

    def wait(bytes_of, sem):
        pltpu.make_async_copy(bytes_of, bytes_of, sem).wait()

    barrier = pltpu.get_barrier_semaphore()

    def greet(device):
        pl.semaphore_signal(barrier, inc=1, device_id=device, device_id_type=MESH)

    for z in range(1, n_z):

        @pl.when(z > my_z)
        def _():
            greet(at_z(z))

    for y in range(1, Y_SIZE):

        @pl.when(y > my_y)
        def _():
            greet(at_y(y))

    for step in range(1, n_head):
        greet({"head": lax.rem(my_head + step, n_head)})
    for slot, array in enumerate(inputs):
        pltpu.make_async_copy(array, staged.at[slot], stage_sem.at[slot]).start()
    codes_copy = pltpu.make_async_copy(codes_ref, codes, own_sem.at[0])
    codes_copy.start()
    with jax.named_scope("s_barrier"):
        pl.semaphore_wait(barrier, n_head - 1 + my_y + my_z)

    for y in range(Y_SIZE - 1):

        @pl.when(y < my_y)
        def _():
            pl.semaphore_signal(answer.at[0], inc=1, device_id=at_y(y), device_id_type=MESH)

    for z in range(n_z - 1):

        @pl.when(z < my_z)
        def _():
            pl.semaphore_signal(answer.at[1], inc=1, device_id=at_z(z), device_id_type=MESH)


    for slot, array in enumerate(inputs):
        pltpu.make_async_copy(array, staged.at[slot], stage_sem.at[slot]).wait()
    for unit in range(UNITS):
        for slot in range(4):
            for peer in line:
                send(
                    staged.at[slot, :, unit_columns(peer, unit)],
                    rows_in.at[slot, share_rows(my_head), unit_columns(0, unit)],
                    x_send,
                    in_recv.at[max(slot - 1, 0), unit],
                    {"head": peer},
                )

    for slot in range(4):
        rows_in[slot, share_rows(my_head), :] = staged[
            slot, :, pl.ds(pl.multiple_of(my_head * width, width), width)
        ]
    codes_copy.wait()
    for head in range(n_local):
        code_rows[...] = jnp.zeros_like(code_rows)
        code_rows[0 : codes.shape[0], :] = codes[:, head, :].astype(f32)
        code_cols[head] = code_rows[...].T
    place = lax.broadcasted_iota(jnp.int32, (TILE, TILE), 0)
    other = lax.broadcasted_iota(jnp.int32, (TILE, TILE), 1)
    differ = place ^ other
    level = jnp.zeros((TILE, TILE), jnp.int32)
    for bit_index in range(7):
        level = level + (differ >= 2**bit_index).astype(jnp.int32)
    levels[...] = jnp.where(other <= place, level, -1)

    def is_clear(bit_index):
        return my_ctx // 2**bit_index % 2 == 0

    for bit_index in range(ctx_bits):

        @pl.when(is_clear(bit_index))
        def _():
            bucket[bit_index] = jnp.zeros((n_local * TILE, TILE), half)

    @pl.when(my_y % 2 == 1)
    def _():
        next_grad[...] = jnp.zeros_like(next_grad)

    def arrived(slots, unit):
        others = rows_in.at[slots, 0 : length - share, unit_columns(0, unit)]
        with jax.named_scope("s_in"):
            wait(others, in_recv.at[max(slots.stop - 2, 0), unit])

    def code_column(head, level_index, rows):
        return code_cols[head, rows, level_index : level_index + 1] * (
            level_gain(level_index) * scale / 8.0
        )

    def weighted(head, row, products):
        rows = slice(row * TILE, (row + 1) * TILE)
        pieces = []
        for column in range(row + 1):
            if column == row:
                weight = jnp.zeros((TILE, TILE), f32)
                for level_index in range(8):
                    weight = jnp.where(
                        levels[...] == level_index, code_column(head, level_index, rows), weight
                    )
            else:
                weight = code_column(head, 7 + (row ^ column).bit_length(), rows)
            at = slice(column * TILE, (column + 1) * TILE)
            pieces.append((weight * products[:, at]).astype(half))
        return jnp.concatenate(pieces, axis=1)

    def each_head(unit, body):
        with jax.named_scope("c_" + body.__name__):
            pl.loop(unit * unit_heads, (unit + 1) * unit_heads)(body)

    def attend(head):
        columns = head_columns(head)
        for row in range(tiles):
            rows, reach = slice(row * TILE, (row + 1) * TILE), (row + 1) * TILE
            scores = dot_nt(rows_in[QUERY, rows, columns], rows_in[KEY, 0:reach, columns])
            pairs = weighted(head, row, scores)
            probs[head, rows, 0:reach] = pairs
            local[0, rows, columns] = dot_nn(pairs, rows_in[VALUE, 0:reach, columns])

    def attend_back(head):
        columns = head_columns(head)
        for row in range(tiles):
            rows, reach = slice(row * TILE, (row + 1) * TILE), (row + 1) * TILE
            dots = dot_nt(rows_in[COT, rows, columns], rows_in[VALUE, 0:reach, columns])
            pairs = weighted(head, row, dots)
            score_grads[head, rows, 0:reach] = pairs
            local[1, rows, columns] = dot_nn(pairs, rows_in[KEY, 0:reach, columns])

    def sum_back(head):
        columns = head_columns(head)
        for column in range(tiles):
            at, below = slice(column * TILE, (column + 1) * TILE), slice(column * TILE, length)
            local[2, at, columns] = dot_tn(
                score_grads[head, below, at], rows_in[QUERY, below, columns]
            )
            local[3, at, columns] = dot_tn(probs[head, below, at], rows_in[COT, below, columns])

    def state_of(head):
        columns = head_columns(head)
        state = dot_tn(rows_in[KEY, :, columns], rows_in[VALUE, :, columns])
        state_send[columns, :] = state.astype(half)

    def send_state(unit):
        each_head(unit, state_of)
        if unit == 0:

            @pl.when(my_y < Y_SIZE - 1)
            def _():
                with jax.named_scope("s_answery"):
                    pl.semaphore_wait(answer.at[0], Y_SIZE - 1 - my_y)

        for step in range(1, Y_SIZE):
            peer = y_peer(step)
            send(
                state_send.at[part_rows(unit, peer), :],
                state_parts.at[unit, my_y],
                ctx_send,
                state_recv.at[unit],
                at_y(peer),
            )

        @pl.when(my_y % 2 == 0)
        def _():
            send(
                state_send.at[unit_range(unit), :],
                bucket.at[0, unit_range(unit), :],
                ctx_send,
                bucket_recv.at[unit, 0],
                at_y(my_y + 1),
            )

        state_parts[unit, my_y] = state_send[part_rows(unit, my_y), :]

    def send_plane(unit):
        with jax.named_scope("s_state"):
            wait(state_parts.at[unit, 0 : Y_SIZE - 1], state_recv.at[unit])
        lower = state_parts[unit, 0].astype(f32) + state_parts[unit, 1].astype(f32)
        upper = state_parts[unit, 2].astype(f32) + state_parts[unit, 3].astype(f32)
        pair_send[unit, 0] = (lower + upper).astype(half)
        pair_send[unit, 1] = lower.astype(half)
        if unit == 0:


            @pl.when(my_z < n_z - 1)
            def _():
                with jax.named_scope("s_answer"):
                    pl.semaphore_wait(answer.at[1], n_z - 1 - my_z)

        for step in range(1, n_z):

            @pl.when(my_z + step < n_z)
            def _():
                send(
                    pair_send.at[unit, 0],
                    plane_parts.at[unit, my_z],
                    ctx_send,
                    plane_recv.at[unit],
                    at_z(my_z + step),
                )

        for y in (2, 3):

            @pl.when(my_y != y)
            def _():
                send(
                    pair_send.at[unit, 1],
                    bucket.at[1, part_rows(unit, my_y), :],
                    ctx_send,
                    bucket_recv.at[unit, 0],
                    at_y(y),
                )

            @pl.when(my_y == y)
            def _():
                bucket[1, part_rows(unit, my_y), :] = pair_send[unit, 1]

    def send_above(unit):
        for count in range(1, n_z):

            @pl.when(my_z == count)
            def _():
                with jax.named_scope("s_plane"):
                    wait(plane_parts.at[unit, 0:count], plane_recv.at[unit])

        for bit_index in range(z_bits):

            @pl.when(z_bit(bit_index))
            def _():
                total = jnp.zeros((part, TILE), f32)
                for block in range(2**bit_index):
                    total = total + plane_parts[unit, group_start(bit_index) + block].astype(f32)
                above_send[unit, bit_index] = total.astype(half)
                for step in range(1, Y_SIZE):
                    send(
                        above_send.at[unit, bit_index],
                        bucket.at[Y_BITS + bit_index, part_rows(unit, my_y), :],
                        ctx_send,
                        bucket_recv.at[unit, 1],
                        at_y(y_peer(step)),
                    )
                bucket[Y_BITS + bit_index, part_rows(unit, my_y), :] = above_send[unit, bit_index]

    def grad_of(head):
        columns = head_columns(head)
        cot = rows_in[COT, :, columns].astype(f32)
        scaled = [
            (code_column(head, tok_bits + 1 + bit_index, slice(None)) * cot).astype(half)
            for bit_index in range(ctx_bits)
        ]
        grads = dot_tn(rows_in[QUERY, :, columns], jnp.concatenate(scaled, axis=1))
        for bit_index in range(ctx_bits):
            grad_send[bit_index, columns, :] = grads[
                :, bit_index * TILE : (bit_index + 1) * TILE
            ].astype(half)

    def send_grad(unit):
        each_head(unit, grad_of)

        def parts(bit_index, kind):
            for step in range(1, Y_SIZE):
                peer = y_peer(step)
                send(
                    grad_send.at[bit_index, part_rows(unit, peer), :],
                    grad_parts.at[unit, bit_index - 1, my_y],
                    ctx_send,
                    grad_recv.at[unit, kind],
                    at_y(peer),
                )
            grad_parts[unit, bit_index - 1, my_y] = grad_send[bit_index, part_rows(unit, my_y), :]

        for bit_index in range(z_bits):

            @pl.when(z_bit(bit_index))
            def _():
                parts(Y_BITS + bit_index, 1)

        @pl.when(my_y >= 2)
        def _():
            parts(1, 0)

        @pl.when(my_y % 2 == 1)
        def _():
            send(
                grad_send.at[0, unit_range(unit), :],
                next_grad.at[unit_range(unit), :],
                ctx_send,
                next_recv.at[unit],
                at_y(my_y - 1),
            )

    def send_plane_grad(unit):
        for count in range(1, z_bits + 1):

            @pl.when(z_count == count)
            def _():
                with jax.named_scope("s_grad"):
                    wait(grad_parts.at[unit, 0:count, 0 : Y_SIZE - 1], grad_recv.at[unit, 1])

        for bit_index in range(z_bits):

            @pl.when(z_bit(bit_index))
            def _():
                total = jnp.zeros((part, TILE), f32)
                for y in range(Y_SIZE):
                    total = total + grad_parts[unit, 1 + bit_index, y].astype(f32)
                plane_grad_send[unit, bit_index] = total.astype(half)
                for block in range(2**bit_index):
                    send(
                        plane_grad_send.at[unit, bit_index],
                        plane_grad_parts.at[unit, my_z],
                        ctx_send,
                        plane_grad_recv.at[unit],
                        at_z(group_start(bit_index) + block),
                    )

    def send_pulled(unit):
        @pl.when(my_y >= 2)
        def _():
            wait(grad_parts.at[unit, 0, 0:1], grad_recv.at[unit, 0])

        @pl.when(my_y < 2)
        def _():
            wait(grad_parts.at[unit, 0, 0:2], grad_recv.at[unit, 0])

        for count in range(1, n_z):

            @pl.when(n_z - 1 - my_z == count)
            def _():
                with jax.named_scope("s_planeg"):
                    wait(plane_grad_parts.at[unit, 0:count], plane_grad_recv.at[unit])

        pulled_send[...] = jnp.zeros_like(pulled_send)
        for z in range(1, n_z):

            @pl.when(z > my_z)
            def _():
                pulled_send[...] += plane_grad_parts[unit, z].astype(f32)

        later = pulled_send[...]
        upper = grad_parts[unit, 0, 2].astype(f32) + grad_parts[unit, 0, 3].astype(f32)
        pulled_half[unit, 0] = (later + upper).astype(half)
        pulled_half[unit, 1] = later.astype(half)
        for step in range(1, Y_SIZE):
            peer = y_peer(step)
            send(
                pulled_half.at[unit, peer // 2],
                pulled.at[part_rows(unit, my_y), :],
                ctx_send,
                pulled_recv.at[unit],
                at_y(peer),
            )
        pulled[part_rows(unit, my_y), :] = pulled_half[unit, my_y // 2]

    def send_out(slot, head):
        columns = head_columns(head)
        there = pl.ds(pl.multiple_of(my_head * width + head * TILE, TILE), TILE)
        for peer in line:
            send(
                rows_out.at[slot, share_rows(peer), columns],
                outputs[slot].at[:, there],
                x_send,
                out_recv,
                {"head": peer},
            )
        outputs[slot][:, there] = rows_out[slot, share_rows(my_head), columns]

    def cross(head):
        columns = head_columns(head)
        states = [bucket[bit_index, columns, :] for bit_index in range(ctx_bits)]
        wide, tall = jnp.concatenate(states, axis=1), jnp.concatenate(states, axis=0)
        for row in range(tiles):
            rows = slice(row * TILE, (row + 1) * TILE)
            attended, grad_query = local[0, rows, columns], local[1, rows, columns]
            reads = dot_nn(rows_in[QUERY, rows, columns], wide)
            cot_reads = dot_nt(rows_in[COT, rows, columns], tall)
            for bit_index in range(ctx_bits):
                row_scale = code_column(head, tok_bits + 1 + bit_index, rows)
                at = slice(bit_index * TILE, (bit_index + 1) * TILE)
                attended = attended + row_scale * reads[:, at]
                grad_query = grad_query + row_scale * cot_reads[:, at]
            rows_out[0, rows, columns] = attended.astype(half)
            rows_out[1, rows, columns] = grad_query.astype(half)
        send_out(0, head)
        send_out(1, head)

    def read_buckets(unit):
        for y, count in ((1, Y_SIZE), (2, Y_SIZE - 1), (3, 2 * Y_SIZE - 1)):

            @pl.when(my_y == y)
            def _():
                with jax.named_scope("s_bucket"):
                    wait(byte_count.at[0 : count * part, :], bucket_recv.at[unit, 0])

        for count in range(1, z_bits + 1):

            @pl.when(z_count == count)
            def _():
                with jax.named_scope("s_bucketz"):
                    wait(
                        byte_count.at[0 : count * (Y_SIZE - 1) * part, :], bucket_recv.at[unit, 1]
                    )

        each_head(unit, cross)

    def pull(head):
        columns = head_columns(head)
        states = (pulled[columns, :].astype(f32) + next_grad[columns, :].astype(f32)).astype(half)
        grad_key = local[2, :, columns] + dot_nt(rows_in[VALUE, :, columns], states)
        rows_out[2, :, columns] = grad_key.astype(half)
        grad_value = local[3, :, columns] + dot_nn(rows_in[KEY, :, columns], states)
        rows_out[3, :, columns] = grad_value.astype(half)
        send_out(2, head)
        send_out(3, head)

    def read_pulled(unit):
        @pl.when(my_y % 2 == 0)
        def _():
            wait(next_grad.at[unit_range(unit), :], next_recv.at[unit])

        with jax.named_scope("s_pulled"):
            wait(pulled.at[0 : (Y_SIZE - 1) * part, :], pulled_recv.at[unit])
        each_head(unit, pull)

    def step_in(unit):
        arrived(slice(KEY, VALUE + 1), unit)
        send_state(unit)
        if unit >= 2:
            read_buckets(unit - 2)
        arrived(slice(QUERY, QUERY + 1), unit)
        each_head(unit, attend)
        if unit >= 1:
            send_plane_grad(unit - 1)
            send_above(unit - 1)
        if unit >= 3:
            read_pulled(unit - 3)
        arrived(slice(COT, COT + 1), unit)
        send_grad(unit)
        send_plane(unit)
        if unit >= 2:
            send_pulled(unit - 2)
        each_head(unit, attend_back)
        if unit >= 1:
            each_head(unit - 1, sum_back)

    for unit in range(UNITS):
        step_in(unit)
    last = UNITS - 1
    read_buckets(last - 1)
    send_plane_grad(last)
    send_above(last)
    read_pulled(last - 2)
    send_pulled(last - 1)
    each_head(last, sum_back)
    read_buckets(last)
    read_pulled(last - 1)
    send_pulled(last)
    read_pulled(last)

    flat = local.reshape(local.shape[0] * length, width)
    part_bytes = UNITS * part * TILE * 2 // (width * 4)
    for low in (True, False):
        for count in range(z_bits + 1):

            @pl.when(((my_y < 2) == low) & (z_count == count))
            def _():
                parts = 2 * (Y_SIZE - 1) + Y_SIZE + n_z - 1
                parts += (2 if low else 4) + 2 * (Y_SIZE - 1) * count
                wait(flat.at[0 : parts * part_bytes, :], ctx_send)

    wait(local.at[:, 0 : length - share, :], x_send)
    with jax.named_scope("s_out"):
        wait(rows_out.at[:, 0 : length - share, :], out_recv)


def put_out_kernel(*refs):
    held, results, sems = refs[:4], refs[4:8], refs[8]
    copies = [pltpu.make_async_copy(held[i], results[i], sems.at[i]) for i in range(4)]
    for copy in copies:
        copy.start()
    for copy in copies:
        copy.wait()


def put_out(held):
    return pl.pallas_call(
        put_out_kernel,
        out_shape=tuple(jax.ShapeDtypeStruct(array.shape, array.dtype) for array in held),
        in_specs=[pl.BlockSpec(memory_space=pltpu.VMEM)] * 4,
        out_specs=(pl.BlockSpec(memory_space=pl.ANY),) * 4,
        scratch_shapes=[pltpu.SemaphoreType.DMA((4,))],
        name="put_out",
    )(*held)


def on_device(n_ctx, n_head, query_input, key_input, value_input, cotangent, level_codes):
    share, features = query_input.shape
    n_local, n_levels, length = level_codes.shape
    width = features // n_head
    tok_bits = length.bit_length() - 1
    ctx_bits = n_levels - tok_bits - 1
    state_rows = n_local * TILE
    part = state_rows // UNITS // Y_SIZE
    n_z = n_ctx // Y_SIZE
    z_bits = ctx_bits - Y_BITS
    half = jnp.bfloat16
    dma = pltpu.SemaphoreType.DMA
    held = pl.pallas_call(
        functools.partial(kernel, n_ctx, n_head, ctx_bits, tok_bits),
        out_shape=(pltpu.VMEM(query_input.shape, half),) * 4,
        in_specs=[pl.BlockSpec(memory_space=pl.ANY)] * 5,
        out_specs=(pl.BlockSpec(memory_space=pltpu.VMEM),) * 4,
        scratch_shapes=[
            pltpu.VMEM((4, share, features), half),
            pltpu.VMEM((4, length, width), half),
            pltpu.VMEM((n_levels, n_local, length), jnp.int32),
            pltpu.VMEM((TILE, length), jnp.float32),
            pltpu.VMEM((n_local, length, TILE), jnp.float32),
            pltpu.VMEM((TILE, TILE), jnp.int32),
            pltpu.VMEM((n_local, length, length), half),
            pltpu.VMEM((n_local, length, length), half),
            pltpu.VMEM((4, length, width), jnp.float32),
            pltpu.VMEM((4, length, width), half),
            pltpu.VMEM((state_rows, TILE), half),
            pltpu.VMEM((UNITS, Y_SIZE, part, TILE), half),
            pltpu.VMEM((UNITS, 2, part, TILE), half),
            pltpu.VMEM((UNITS, n_z, part, TILE), half),
            pltpu.VMEM((UNITS, z_bits, part, TILE), half),
            pltpu.VMEM((ctx_bits, state_rows, TILE), half),
            pltpu.VMEM((ctx_bits, state_rows, TILE), half),
            pltpu.VMEM((UNITS, ctx_bits - 1, Y_SIZE, part, TILE), half),
            pltpu.VMEM((UNITS, z_bits, part, TILE), half),
            pltpu.VMEM((UNITS, n_z, part, TILE), half),
            pltpu.VMEM((part, TILE), jnp.float32),
            pltpu.VMEM((UNITS, 2, part, TILE), half),
            pltpu.VMEM((state_rows, TILE), half),
            pltpu.VMEM((state_rows, TILE), half),
            pltpu.SemaphoreType.REGULAR((2,)),
            dma((4,)),
            dma((1,)),
            dma,
            dma,
            dma((3, UNITS)),
            dma((UNITS,)),
            dma((UNITS,)),
            dma((UNITS, 2)),
            dma((UNITS, 2)),
            dma((UNITS,)),
            dma((UNITS,)),
            dma((UNITS,)),
            dma,
        ],
        compiler_params=pltpu.CompilerParams(collective_id=0, has_side_effects=True),
        name="layer",
    )(query_input, key_input, value_input, cotangent, jnp.transpose(level_codes, (1, 0, 2)))
    return put_out([pltpu.with_memory_space_constraint(array, pltpu.VMEM) for array in held])


def solution(mesh):
    rows = P(("ctx", "head"), None)
    return jax.shard_map(
        functools.partial(on_device, mesh.shape["ctx"], mesh.shape["head"]),
        mesh=mesh,
        in_specs=(rows, rows, rows, rows, P("head", None, "ctx")),
        out_specs=(rows, rows, rows, rows),
        check_vma=False,
    )
```

```python
import functools

import jax
import jax.numpy as jnp
from jax import lax
from jax.experimental import pallas as pl
from jax.experimental.pallas import tpu as pltpu
from jax.sharding import PartitionSpec as P

MESH = pl.DeviceIdType.MESH
KEY, VALUE, QUERY, COT = range(4)
TILE = 128
UNITS = 4
Y_SIZE, Y_BITS = 4, 2


def level_gain(level):
    if level == 0:
        return 1.0
    return 2.0 ** (-(level - 1) / 2.0)


def dot_nn(a, b):
    return lax.dot_general(a, b, (((1,), (0,)), ((), ())), preferred_element_type=jnp.float32)


def dot_nt(a, b):
    return lax.dot_general(a, b, (((1,), (1,)), ((), ())), preferred_element_type=jnp.float32)


def dot_tn(a, b):
    return lax.dot_general(a, b, (((0,), (0,)), ((), ())), preferred_element_type=jnp.float32)


def kernel(
    n_ctx,
    n_head,
    ctx_bits,
    tok_bits,
    query_ref,
    key_ref,
    value_ref,
    cot_ref,
    codes_ref,
    out_ref,
    gq_ref,
    gk_ref,
    gv_ref,
    staged,
    rows_in,
    codes,
    code_rows,
    code_cols,
    levels,
    probs,
    score_grads,
    local,
    rows_out,
    state_send,
    state_parts,
    pair_send,
    plane_parts,
    above_send,
    bucket,
    grad_send,
    grad_parts,
    plane_grad_send,
    plane_grad_parts,
    pulled_send,
    pulled_half,
    pulled,
    next_grad,
    answer,
    stage_sem,
    own_sem,
    x_send,
    ctx_send,
    in_recv,
    state_recv,
    plane_recv,
    bucket_recv,
    grad_recv,
    plane_grad_recv,
    pulled_recv,
    next_recv,
    out_recv,
):
    my_ctx = lax.axis_index("ctx")
    my_head = lax.axis_index("head")
    my_y = lax.rem(my_ctx, Y_SIZE)
    my_z = my_ctx // Y_SIZE
    n_z = n_ctx // Y_SIZE
    z_bits = ctx_bits - Y_BITS
    inputs = (key_ref, value_ref, query_ref, cot_ref)
    outputs = (out_ref, gq_ref, gk_ref, gv_ref)
    share = query_ref.shape[0]
    length = share * n_head
    width = query_ref.shape[1] // n_head
    n_local = width // TILE
    unit_heads = n_local // UNITS
    unit_width = width // UNITS
    unit_rows = unit_heads * TILE
    part = unit_rows // Y_SIZE
    tiles = length // TILE
    scale = TILE ** (-0.5)
    byte_count = grad_send.reshape(ctx_bits * n_local * TILE, TILE)
    f32, half = jnp.float32, jnp.bfloat16

    def z_bit(bit_index):
        return my_z // 2**bit_index % 2 == 1

    z_count = sum(my_z // 2**bit_index % 2 for bit_index in range(z_bits))

    def group_start(bit_index):
        return my_z // 2 ** (bit_index + 1) * 2 ** (bit_index + 1)

    def y_peer(step):
        return lax.rem(my_y + (2, 1, 3)[step - 1], Y_SIZE)

    chips = n_head // 2
    far = chips // 2
    near = [step for reach in range(far - 1, 0, -1) for step in (reach, chips - reach)]
    line = [
        lax.rem(my_head // 2 + step, chips) * 2 + lax.rem(my_head + core, 2)
        for step, core in [(far, 0), (far, 1)] + [(step, core) for core in (0, 1) for step in near]
        if step
    ] + [my_head // 2 * 2 + lax.rem(my_head + 1, 2)]

    def at_y(y):
        return {"ctx": my_z * Y_SIZE + y}

    def at_z(z):
        return {"ctx": z * Y_SIZE + my_y}

    def head_columns(head):
        return pl.ds(pl.multiple_of(head * TILE, TILE), TILE)

    def unit_range(unit):
        return slice(unit * unit_rows, (unit + 1) * unit_rows)

    def part_rows(unit, owner):
        return pl.ds(pl.multiple_of(unit * unit_rows + owner * part, part), part)

    def share_rows(owner):
        return pl.ds(pl.multiple_of(owner * share, share), share)

    def unit_columns(owner, unit):
        return pl.ds(pl.multiple_of(owner * width + unit * unit_width, unit_width), unit_width)

    def send(src, dst, send_sem, recv_sem, device):
        pltpu.make_async_remote_copy(
            src_ref=src,
            dst_ref=dst,
            send_sem=send_sem,
            recv_sem=recv_sem,
            device_id=device,
            device_id_type=MESH,
        ).start()

    def wait(bytes_of, sem):
        pltpu.make_async_copy(bytes_of, bytes_of, sem).wait()

    barrier = pltpu.get_barrier_semaphore()

    def greet(device):
        pl.semaphore_signal(barrier, inc=1, device_id=device, device_id_type=MESH)

    for z in range(1, n_z):

        @pl.when(z > my_z)
        def _():
            greet(at_z(z))

    for y in range(1, Y_SIZE):

        @pl.when(y > my_y)
        def _():
            greet(at_y(y))

    for step in range(1, n_head):
        greet({"head": lax.rem(my_head + step, n_head)})
    for slot, array in enumerate(inputs):
        pltpu.make_async_copy(array, staged.at[slot], stage_sem.at[slot]).start()
    codes_copy = pltpu.make_async_copy(codes_ref, codes, own_sem.at[0])
    codes_copy.start()
    with jax.named_scope("s_barrier"):
        pl.semaphore_wait(barrier, n_head - 1 + my_y + my_z)

    for y in range(Y_SIZE - 1):

        @pl.when(y < my_y)
        def _():
            pl.semaphore_signal(answer.at[0], inc=1, device_id=at_y(y), device_id_type=MESH)

    for z in range(n_z - 1):

        @pl.when(z < my_z)
        def _():
            pl.semaphore_signal(answer.at[1], inc=1, device_id=at_z(z), device_id_type=MESH)


    for slot, array in enumerate(inputs):
        pltpu.make_async_copy(array, staged.at[slot], stage_sem.at[slot]).wait()
    for unit in range(UNITS):
        for slot in range(4):
            for peer in line:
                send(
                    staged.at[slot, :, unit_columns(peer, unit)],
                    rows_in.at[slot, share_rows(my_head), unit_columns(0, unit)],
                    x_send,
                    in_recv.at[max(slot - 1, 0), unit],
                    {"head": peer},
                )

    for slot in range(4):
        rows_in[slot, share_rows(my_head), :] = staged[
            slot, :, pl.ds(pl.multiple_of(my_head * width, width), width)
        ]
    codes_copy.wait()
    for head in range(n_local):
        code_rows[...] = jnp.zeros_like(code_rows)
        code_rows[0 : codes.shape[0], :] = codes[:, head, :].astype(f32)
        code_cols[head] = code_rows[...].T
    place = lax.broadcasted_iota(jnp.int32, (TILE, TILE), 0)
    other = lax.broadcasted_iota(jnp.int32, (TILE, TILE), 1)
    differ = place ^ other
    level = jnp.zeros((TILE, TILE), jnp.int32)
    for bit_index in range(7):
        level = level + (differ >= 2**bit_index).astype(jnp.int32)
    levels[...] = jnp.where(other <= place, level, -1)

    def is_clear(bit_index):
        return my_ctx // 2**bit_index % 2 == 0

    for bit_index in range(ctx_bits):

        @pl.when(is_clear(bit_index))
        def _():
            bucket[bit_index] = jnp.zeros((n_local * TILE, TILE), half)

    @pl.when(my_y % 2 == 1)
    def _():
        next_grad[...] = jnp.zeros_like(next_grad)

    def arrived(slots, unit):
        others = rows_in.at[slots, 0 : length - share, unit_columns(0, unit)]
        with jax.named_scope("s_in"):
            wait(others, in_recv.at[max(slots.stop - 2, 0), unit])

    def code_column(head, level_index, rows):
        return code_cols[head, rows, level_index : level_index + 1] * (
            level_gain(level_index) * scale / 8.0
        )

    def weighted(head, row, products):
        rows = slice(row * TILE, (row + 1) * TILE)
        pieces = []
        for column in range(row + 1):
            if column == row:
                weight = jnp.zeros((TILE, TILE), f32)
                for level_index in range(8):
                    weight = jnp.where(
                        levels[...] == level_index, code_column(head, level_index, rows), weight
                    )
            else:
                weight = code_column(head, 7 + (row ^ column).bit_length(), rows)
            at = slice(column * TILE, (column + 1) * TILE)
            pieces.append((weight * products[:, at]).astype(half))
        return jnp.concatenate(pieces, axis=1)

    def each_head(unit, body):
        with jax.named_scope("c_" + body.__name__):
            pl.loop(unit * unit_heads, (unit + 1) * unit_heads)(body)

    def attend(head):
        columns = head_columns(head)
        for row in range(tiles):
            rows, reach = slice(row * TILE, (row + 1) * TILE), (row + 1) * TILE
            scores = dot_nt(rows_in[QUERY, rows, columns], rows_in[KEY, 0:reach, columns])
            pairs = weighted(head, row, scores)
            probs[head, rows, 0:reach] = pairs
            local[0, rows, columns] = dot_nn(pairs, rows_in[VALUE, 0:reach, columns])

    def attend_back(head):
        columns = head_columns(head)
        for row in range(tiles):
            rows, reach = slice(row * TILE, (row + 1) * TILE), (row + 1) * TILE
            dots = dot_nt(rows_in[COT, rows, columns], rows_in[VALUE, 0:reach, columns])
            pairs = weighted(head, row, dots)
            score_grads[head, rows, 0:reach] = pairs
            local[1, rows, columns] = dot_nn(pairs, rows_in[KEY, 0:reach, columns])

    def sum_back(head):
        columns = head_columns(head)
        for column in range(tiles):
            at, below = slice(column * TILE, (column + 1) * TILE), slice(column * TILE, length)
            local[2, at, columns] = dot_tn(
                score_grads[head, below, at], rows_in[QUERY, below, columns]
            )
            local[3, at, columns] = dot_tn(probs[head, below, at], rows_in[COT, below, columns])

    def state_of(head):
        columns = head_columns(head)
        state = dot_tn(rows_in[KEY, :, columns], rows_in[VALUE, :, columns])
        state_send[columns, :] = state.astype(half)

    def send_state(unit):
        each_head(unit, state_of)
        if unit == 0:

            @pl.when(my_y < Y_SIZE - 1)
            def _():
                with jax.named_scope("s_answery"):
                    pl.semaphore_wait(answer.at[0], Y_SIZE - 1 - my_y)

        for step in range(1, Y_SIZE):
            peer = y_peer(step)
            send(
                state_send.at[part_rows(unit, peer), :],
                state_parts.at[unit, my_y],
                ctx_send,
                state_recv.at[unit],
                at_y(peer),
            )

        @pl.when(my_y % 2 == 0)
        def _():
            send(
                state_send.at[unit_range(unit), :],
                bucket.at[0, unit_range(unit), :],
                ctx_send,
                bucket_recv.at[unit, 0],
                at_y(my_y + 1),
            )

        state_parts[unit, my_y] = state_send[part_rows(unit, my_y), :]

    def send_plane(unit):
        with jax.named_scope("s_state"):
            wait(state_parts.at[unit, 0 : Y_SIZE - 1], state_recv.at[unit])
        lower = state_parts[unit, 0].astype(f32) + state_parts[unit, 1].astype(f32)
        upper = state_parts[unit, 2].astype(f32) + state_parts[unit, 3].astype(f32)
        pair_send[unit, 0] = (lower + upper).astype(half)
        pair_send[unit, 1] = lower.astype(half)
        if unit == 0:


            @pl.when(my_z < n_z - 1)
            def _():
                with jax.named_scope("s_answer"):
                    pl.semaphore_wait(answer.at[1], n_z - 1 - my_z)

        for step in range(1, n_z):

            @pl.when(my_z + step < n_z)
            def _():
                send(
                    pair_send.at[unit, 0],
                    plane_parts.at[unit, my_z],
                    ctx_send,
                    plane_recv.at[unit],
                    at_z(my_z + step),
                )

        for y in (2, 3):

            @pl.when(my_y != y)
            def _():
                send(
                    pair_send.at[unit, 1],
                    bucket.at[1, part_rows(unit, my_y), :],
                    ctx_send,
                    bucket_recv.at[unit, 0],
                    at_y(y),
                )

            @pl.when(my_y == y)
            def _():
                bucket[1, part_rows(unit, my_y), :] = pair_send[unit, 1]

    def send_above(unit):
        for count in range(1, n_z):

            @pl.when(my_z == count)
            def _():
                with jax.named_scope("s_plane"):
                    wait(plane_parts.at[unit, 0:count], plane_recv.at[unit])

        for bit_index in range(z_bits):

            @pl.when(z_bit(bit_index))
            def _():
                total = jnp.zeros((part, TILE), f32)
                for block in range(2**bit_index):
                    total = total + plane_parts[unit, group_start(bit_index) + block].astype(f32)
                above_send[unit, bit_index] = total.astype(half)
                for step in range(1, Y_SIZE):
                    send(
                        above_send.at[unit, bit_index],
                        bucket.at[Y_BITS + bit_index, part_rows(unit, my_y), :],
                        ctx_send,
                        bucket_recv.at[unit, 1],
                        at_y(y_peer(step)),
                    )
                bucket[Y_BITS + bit_index, part_rows(unit, my_y), :] = above_send[unit, bit_index]

    def grad_of(head):
        columns = head_columns(head)
        cot = rows_in[COT, :, columns].astype(f32)
        scaled = [
            (code_column(head, tok_bits + 1 + bit_index, slice(None)) * cot).astype(half)
            for bit_index in range(ctx_bits)
        ]
        grads = dot_tn(rows_in[QUERY, :, columns], jnp.concatenate(scaled, axis=1))
        for bit_index in range(ctx_bits):
            grad_send[bit_index, columns, :] = grads[
                :, bit_index * TILE : (bit_index + 1) * TILE
            ].astype(half)

    def send_grad(unit):
        each_head(unit, grad_of)

        def parts(bit_index, kind):
            for step in range(1, Y_SIZE):
                peer = y_peer(step)
                send(
                    grad_send.at[bit_index, part_rows(unit, peer), :],
                    grad_parts.at[unit, bit_index - 1, my_y],
                    ctx_send,
                    grad_recv.at[unit, kind],
                    at_y(peer),
                )
            grad_parts[unit, bit_index - 1, my_y] = grad_send[bit_index, part_rows(unit, my_y), :]

        for bit_index in range(z_bits):

            @pl.when(z_bit(bit_index))
            def _():
                parts(Y_BITS + bit_index, 1)

        @pl.when(my_y >= 2)
        def _():
            parts(1, 0)

        @pl.when(my_y % 2 == 1)
        def _():
            send(
                grad_send.at[0, unit_range(unit), :],
                next_grad.at[unit_range(unit), :],
                ctx_send,
                next_recv.at[unit],
                at_y(my_y - 1),
            )

    def send_plane_grad(unit):
        for count in range(1, z_bits + 1):

            @pl.when(z_count == count)
            def _():
                with jax.named_scope("s_grad"):
                    wait(grad_parts.at[unit, 0:count, 0 : Y_SIZE - 1], grad_recv.at[unit, 1])

        for bit_index in range(z_bits):

            @pl.when(z_bit(bit_index))
            def _():
                total = jnp.zeros((part, TILE), f32)
                for y in range(Y_SIZE):
                    total = total + grad_parts[unit, 1 + bit_index, y].astype(f32)
                plane_grad_send[unit, bit_index] = total.astype(half)
                for block in range(2**bit_index):
                    send(
                        plane_grad_send.at[unit, bit_index],
                        plane_grad_parts.at[unit, my_z],
                        ctx_send,
                        plane_grad_recv.at[unit],
                        at_z(group_start(bit_index) + block),
                    )

    def send_pulled(unit):
        @pl.when(my_y >= 2)
        def _():
            wait(grad_parts.at[unit, 0, 0:1], grad_recv.at[unit, 0])

        @pl.when(my_y < 2)
        def _():
            wait(grad_parts.at[unit, 0, 0:2], grad_recv.at[unit, 0])

        for count in range(1, n_z):

            @pl.when(n_z - 1 - my_z == count)
            def _():
                with jax.named_scope("s_planeg"):
                    wait(plane_grad_parts.at[unit, 0:count], plane_grad_recv.at[unit])

        pulled_send[...] = jnp.zeros_like(pulled_send)
        for z in range(1, n_z):

            @pl.when(z > my_z)
            def _():
                pulled_send[...] += plane_grad_parts[unit, z].astype(f32)

        later = pulled_send[...]
        upper = grad_parts[unit, 0, 2].astype(f32) + grad_parts[unit, 0, 3].astype(f32)
        pulled_half[unit, 0] = (later + upper).astype(half)
        pulled_half[unit, 1] = later.astype(half)
        for step in range(1, Y_SIZE):
            peer = y_peer(step)
            send(
                pulled_half.at[unit, peer // 2],
                pulled.at[part_rows(unit, my_y), :],
                ctx_send,
                pulled_recv.at[unit],
                at_y(peer),
            )
        pulled[part_rows(unit, my_y), :] = pulled_half[unit, my_y // 2]

    def send_out(slot, head):
        columns = head_columns(head)
        there = pl.ds(pl.multiple_of(my_head * width + head * TILE, TILE), TILE)
        for peer in line:
            send(
                rows_out.at[slot, share_rows(peer), columns],
                outputs[slot].at[:, there],
                x_send,
                out_recv,
                {"head": peer},
            )
        outputs[slot][:, there] = rows_out[slot, share_rows(my_head), columns]

    def cross(head):
        columns = head_columns(head)
        states = [bucket[bit_index, columns, :] for bit_index in range(ctx_bits)]
        wide, tall = jnp.concatenate(states, axis=1), jnp.concatenate(states, axis=0)
        for row in range(tiles):
            rows = slice(row * TILE, (row + 1) * TILE)
            attended, grad_query = local[0, rows, columns], local[1, rows, columns]
            reads = dot_nn(rows_in[QUERY, rows, columns], wide)
            cot_reads = dot_nt(rows_in[COT, rows, columns], tall)
            for bit_index in range(ctx_bits):
                row_scale = code_column(head, tok_bits + 1 + bit_index, rows)
                at = slice(bit_index * TILE, (bit_index + 1) * TILE)
                attended = attended + row_scale * reads[:, at]
                grad_query = grad_query + row_scale * cot_reads[:, at]
            rows_out[0, rows, columns] = attended.astype(half)
            rows_out[1, rows, columns] = grad_query.astype(half)
        send_out(0, head)
        send_out(1, head)

    def read_buckets(unit):
        for y, count in ((1, Y_SIZE), (2, Y_SIZE - 1), (3, 2 * Y_SIZE - 1)):

            @pl.when(my_y == y)
            def _():
                with jax.named_scope("s_bucket"):
                    wait(byte_count.at[0 : count * part, :], bucket_recv.at[unit, 0])

        for count in range(1, z_bits + 1):

            @pl.when(z_count == count)
            def _():
                with jax.named_scope("s_bucketz"):
                    wait(
                        byte_count.at[0 : count * (Y_SIZE - 1) * part, :], bucket_recv.at[unit, 1]
                    )

        each_head(unit, cross)

    def pull(head):
        columns = head_columns(head)
        states = (pulled[columns, :].astype(f32) + next_grad[columns, :].astype(f32)).astype(half)
        grad_key = local[2, :, columns] + dot_nt(rows_in[VALUE, :, columns], states)
        rows_out[2, :, columns] = grad_key.astype(half)
        grad_value = local[3, :, columns] + dot_nn(rows_in[KEY, :, columns], states)
        rows_out[3, :, columns] = grad_value.astype(half)
        send_out(2, head)
        send_out(3, head)

    def read_pulled(unit):
        @pl.when(my_y % 2 == 0)
        def _():
            wait(next_grad.at[unit_range(unit), :], next_recv.at[unit])

        with jax.named_scope("s_pulled"):
            wait(pulled.at[0 : (Y_SIZE - 1) * part, :], pulled_recv.at[unit])
        each_head(unit, pull)

    def step_in(unit):
        arrived(slice(KEY, VALUE + 1), unit)
        send_state(unit)
        if unit >= 2:
            read_buckets(unit - 2)
        arrived(slice(QUERY, QUERY + 1), unit)
        each_head(unit, attend)
        if unit >= 1:
            send_plane_grad(unit - 1)
            send_above(unit - 1)
        if unit >= 3:
            read_pulled(unit - 3)
        arrived(slice(COT, COT + 1), unit)
        send_grad(unit)
        send_plane(unit)
        if unit >= 2:
            send_pulled(unit - 2)
        each_head(unit, attend_back)
        if unit >= 1:
            each_head(unit - 1, sum_back)

    for unit in range(UNITS):
        step_in(unit)
    last = UNITS - 1
    read_buckets(last - 1)
    send_plane_grad(last)
    send_above(last)
    read_pulled(last - 2)
    send_pulled(last - 1)
    each_head(last, sum_back)
    read_buckets(last)
    read_pulled(last - 1)
    send_pulled(last)
    read_pulled(last)

    flat = local.reshape(local.shape[0] * length, width)
    part_bytes = UNITS * part * TILE * 2 // (width * 4)
    for low in (True, False):
        for count in range(z_bits + 1):

            @pl.when(((my_y < 2) == low) & (z_count == count))
            def _():
                parts = 2 * (Y_SIZE - 1) + Y_SIZE + n_z - 1
                parts += (2 if low else 4) + 2 * (Y_SIZE - 1) * count
                wait(flat.at[0 : parts * part_bytes, :], ctx_send)

    wait(local.at[:, 0 : length - share, :], x_send)
    with jax.named_scope("s_out"):
        wait(rows_out.at[:, 0 : length - share, :], out_recv)


def put_out_kernel(*refs):
    held, results, sems = refs[:4], refs[4:8], refs[8]
    copies = [pltpu.make_async_copy(held[i], results[i], sems.at[i]) for i in range(4)]
    for copy in copies:
        copy.start()
    for copy in copies:
        copy.wait()


def put_out(held):
    return pl.pallas_call(
        put_out_kernel,
        out_shape=tuple(jax.ShapeDtypeStruct(array.shape, array.dtype) for array in held),
        in_specs=[pl.BlockSpec(memory_space=pltpu.VMEM)] * 4,
        out_specs=(pl.BlockSpec(memory_space=pl.ANY),) * 4,
        scratch_shapes=[pltpu.SemaphoreType.DMA((4,))],
        name="put_out",
    )(*held)


def on_device(n_ctx, n_head, query_input, key_input, value_input, cotangent, level_codes):
    share, features = query_input.shape
    n_local, n_levels, length = level_codes.shape
    width = features // n_head
    tok_bits = length.bit_length() - 1
    ctx_bits = n_levels - tok_bits - 1
    state_rows = n_local * TILE
    part = state_rows // UNITS // Y_SIZE
    n_z = n_ctx // Y_SIZE
    z_bits = ctx_bits - Y_BITS
    half = jnp.bfloat16
    dma = pltpu.SemaphoreType.DMA
    held = pl.pallas_call(
        functools.partial(kernel, n_ctx, n_head, ctx_bits, tok_bits),
        out_shape=(pltpu.VMEM(query_input.shape, half),) * 4,
        in_specs=[pl.BlockSpec(memory_space=pl.ANY)] * 5,
        out_specs=(pl.BlockSpec(memory_space=pltpu.VMEM),) * 4,
        scratch_shapes=[
            pltpu.VMEM((4, share, features), half),
            pltpu.VMEM((4, length, width), half),
            pltpu.VMEM((n_levels, n_local, length), jnp.int32),
            pltpu.VMEM((TILE, length), jnp.float32),
            pltpu.VMEM((n_local, length, TILE), jnp.float32),
            pltpu.VMEM((TILE, TILE), jnp.int32),
            pltpu.VMEM((n_local, length, length), half),
            pltpu.VMEM((n_local, length, length), half),
            pltpu.VMEM((4, length, width), jnp.float32),
            pltpu.VMEM((4, length, width), half),
            pltpu.VMEM((state_rows, TILE), half),
            pltpu.VMEM((UNITS, Y_SIZE, part, TILE), half),
            pltpu.VMEM((UNITS, 2, part, TILE), half),
            pltpu.VMEM((UNITS, n_z, part, TILE), half),
            pltpu.VMEM((UNITS, z_bits, part, TILE), half),
            pltpu.VMEM((ctx_bits, state_rows, TILE), half),
            pltpu.VMEM((ctx_bits, state_rows, TILE), half),
            pltpu.VMEM((UNITS, ctx_bits - 1, Y_SIZE, part, TILE), half),
            pltpu.VMEM((UNITS, z_bits, part, TILE), half),
            pltpu.VMEM((UNITS, n_z, part, TILE), half),
            pltpu.VMEM((part, TILE), jnp.float32),
            pltpu.VMEM((UNITS, 2, part, TILE), half),
            pltpu.VMEM((state_rows, TILE), half),
            pltpu.VMEM((state_rows, TILE), half),
            pltpu.SemaphoreType.REGULAR((2,)),
            dma((4,)),
            dma((1,)),
            dma,
            dma,
            dma((3, UNITS)),
            dma((UNITS,)),
            dma((UNITS,)),
            dma((UNITS, 2)),
            dma((UNITS, 2)),
            dma((UNITS,)),
            dma((UNITS,)),
            dma((UNITS,)),
            dma,
        ],
        compiler_params=pltpu.CompilerParams(collective_id=0, has_side_effects=True),
        name="layer",
    )(query_input, key_input, value_input, cotangent, jnp.transpose(level_codes, (1, 0, 2)))
    return put_out([pltpu.with_memory_space_constraint(array, pltpu.VMEM) for array in held])


def solution(mesh):
    rows = P(("ctx", "head"), None)
    return jax.shard_map(
        functools.partial(on_device, mesh.shape["ctx"], mesh.shape["head"]),
        mesh=mesh,
        in_specs=(rows, rows, rows, rows, P("head", None, "ctx")),
        out_specs=(rows, rows, rows, rows),
        check_vma=False,
    )
```
